32 devices in a mesh: dp: 4 (over x, core), ctx: 4 (over z), tensor: 2 (over y).
Axes of the slice: x: 2, y: 2, z: 4, core: 2. Of those that a mesh axis runs over, the one named last changes fastest.
Arguments:
- inputs: bfloat16 [4, 1024, 2048], P('dp', 'ctx'), may hold values from -6 to 6
- segment_ids: int32 [4, 1024], P('dp', 'ctx'), may hold values from 0 to 3, as said below
- positions: int32 [4, 1024], P('dp', 'ctx'), may hold values from 0 to 383, as said below
- out_grad: bfloat16 [4, 1024, 2048], P('dp', 'ctx'), may hold values from -6 to 6
- attn_gain: bfloat16 [2048], P(('dp', 'ctx')), may hold values from 0.5 to 1.5
- w_query: bfloat16 [2048, 2048], P(('dp', 'ctx'), 'tensor'), may hold values from -0.125 to 0.125
- w_key: bfloat16 [2048, 1024], P(('dp', 'ctx'), 'tensor'), may hold values from -0.125 to 0.125
- w_value: bfloat16 [2048, 1024], P(('dp', 'ctx'), 'tensor'), may hold values from -0.125 to 0.125
- q_gain: bfloat16 [128], P(('dp', 'ctx')), may hold values from 0.5 to 7, as said below
- k_gain: bfloat16 [128], P(('dp', 'ctx')), may hold values from 0.5 to 7, as said below
- w_out: bfloat16 [2048, 2048], P('tensor', ('dp', 'ctx')), may hold values from -1.5 to 1.5
- mlp_gain: bfloat16 [2048], P(('dp', 'ctx')), may hold values from 0.5 to 1.5
- w_gate: bfloat16 [2048, 6144], P(('dp', 'ctx'), 'tensor'), may hold values from -0.125 to 0.125
- w_up: bfloat16 [2048, 6144], P(('dp', 'ctx'), 'tensor'), may hold values from -0.125 to 0.125
- w_down: bfloat16 [6144, 2048], P('tensor', ('dp', 'ctx')), may hold values from -0.3125 to 0.3125
Outputs:
- output: bfloat16 [4, 1024, 2048], P('dp', 'ctx')
- input_grad: bfloat16 [4, 1024, 2048], P('dp', 'ctx')
- attn_gain_grad: float32 [2048], P(('dp', 'ctx'))
- w_query_grad: float32 [2048, 2048], P(('dp', 'ctx'), 'tensor')
- w_key_grad: float32 [2048, 1024], P(('dp', 'ctx'), 'tensor')
- w_value_grad: float32 [2048, 1024], P(('dp', 'ctx'), 'tensor')
- q_gain_grad: float32 [128], P(('dp', 'ctx'))
- k_gain_grad: float32 [128], P(('dp', 'ctx'))
- w_out_grad: float32 [2048, 2048], P('tensor', ('dp', 'ctx'))
- mlp_gain_grad: float32 [2048], P(('dp', 'ctx'))
- w_gate_grad: float32 [2048, 6144], P(('dp', 'ctx'), 'tensor')
- w_up_grad: float32 [2048, 6144], P(('dp', 'ctx'), 'tensor')
- w_down_grad: float32 [6144, 2048], P('tensor', ('dp', 'ctx'))
The draws below stay inside these ranges and needn't reach their ends.
Inputs may be any that keep to these rules, and one draw needn't show every extreme that they name: `segment_ids`: segment numbers never fall along a sequence, start at 0, and each of 0 to 3 names one document in every sequence. `positions`: a token's position counts the tokens before it in its own document. `q_gain`: positive gains. `k_gain`: positive gains.
All inputs are finite; a program needn't handle non-finite values.
Results may differ from the reference program's by a relative error of at most 0.025.
The reference program's roundings to bfloat16 on the way count: a program that leaves them out, or rounds other values in their place, can miss the bound.
Values may be sent and summed in bfloat16 or wider, within the bound.
A program may use at most 256 MiB of HBM per device.

```python
import math
import jax
import jax.numpy as jnp
from jax import lax

D = 2048
HEADS = 16
KV_HEADS = 8
HEAD_DIM = 128
FF = 6144
DOCS = 4
SEQ_LEN = 1024
SEQS = 4


def document_layout(key):
    quarter = SEQ_LEN // (4 * DOCS)
    cut_moves = jax.random.randint(jax.random.fold_in(key, 11), (SEQS, DOCS - 1), -quarter, quarter + 1).astype(jnp.int32)
    cut_moves = cut_moves.at[0, 0].set(-quarter)
    cut_moves = cut_moves.at[0, 1].set(quarter)
    cut_points = (jnp.arange(1, DOCS, dtype=jnp.int32) * (SEQ_LEN // DOCS))[None, :] + cut_moves
    token_index = jnp.arange(SEQ_LEN, dtype=jnp.int32)
    passed = token_index[None, :, None] >= cut_points[:, None, :]
    segments = jnp.sum(passed.astype(jnp.int32), axis=-1)
    starts = jnp.max(jnp.where(passed, cut_points[:, None, :], 0), axis=-1)
    return (segments.astype(jnp.int32), (token_index[None, :] - starts).astype(jnp.int32))


def draw_segment_ids(key, part):
    return document_layout(key)[0]


def draw_positions(key, part):
    return document_layout(key)[1]


def gain_values(key, salt):
    values = jax.random.uniform(jax.random.fold_in(key, salt), (HEAD_DIM,), jnp.float32, 0.5, 2.0)
    return values.astype(jnp.bfloat16)


def draw_q_gain(key, part):
    return gain_values(key, 3)


def draw_k_gain(key, part):
    return gain_values(key, 5)


def steps_of(key, dims, split, smallest, top_value):
    loudness = 1.0
    for dim, shards_of in split:
        heights = jax.random.uniform(jax.random.fold_in(jax.random.fold_in(key, 6), dim), (shards_of,), jnp.float32, smallest / len(split), top_value / len(split))
        loudness = loudness * jnp.repeat(jnp.exp(heights), dims[dim] // shards_of).reshape((-1,) + (1,) * (len(dims) - 1 - dim))
    return loudness


def scatter_about(rng, shape, scale, bound, pieces=(), held_as=jnp.bfloat16):
    loudness = steps_of(rng, shape, pieces, -0.22, 0.18) if pieces else 1.0
    values = jax.random.normal(rng, shape, jnp.float32) * scale * loudness
    return jnp.minimum(jnp.maximum(values, -bound), bound).astype(held_as)


def setup_inputs(seed: int = 0) -> dict:
    key_of = jax.random.split(jax.random.key(seed), 16)
    return {
        "inputs": scatter_about(key_of[0], (SEQS, SEQ_LEN, D), 1.0, 6.0, ((0, 4), (1, 4))),
        "segment_ids": draw_segment_ids(jax.random.fold_in(key_of[15], 71), 0),
        "positions": draw_positions(jax.random.fold_in(key_of[15], 71), 0),
        "out_grad": scatter_about(key_of[3], (SEQS, SEQ_LEN, D), 1.0, 6.0, ((0, 4), (1, 4))),
        "attn_gain": jnp.clip(1.0 + 0.1 * jax.random.normal(key_of[4], (D,), jnp.float32), 0.5, 1.5).astype(jnp.bfloat16),
        "w_query": scatter_about(key_of[5], (D, HEADS * HEAD_DIM), D ** -0.5, 0.125, ((0, 16), (1, 2))),
        "w_key": scatter_about(key_of[6], (D, KV_HEADS * HEAD_DIM), D ** -0.5, 0.125, ((0, 16), (1, 2))),
        "w_value": scatter_about(key_of[7], (D, KV_HEADS * HEAD_DIM), D ** -0.5, 0.125, ((0, 16), (1, 2))),
        "q_gain": draw_q_gain(jax.random.fold_in(key_of[15], 71), 0),
        "k_gain": draw_k_gain(jax.random.fold_in(key_of[15], 71), 0),
        "w_out": scatter_about(key_of[10], (HEADS * HEAD_DIM, D), (HEADS * HEAD_DIM // 128) ** -0.5, 1.5, ((0, 2), (1, 16))),
        "mlp_gain": jnp.clip(1.0 + 0.1 * jax.random.normal(key_of[11], (D,), jnp.float32), 0.5, 1.5).astype(jnp.bfloat16),
        "w_gate": scatter_about(key_of[12], (D, FF), D ** -0.5, 0.125, ((0, 16), (1, 2))),
        "w_up": scatter_about(key_of[13], (D, FF), D ** -0.5, 0.125, ((0, 16), (1, 2))),
        "w_down": scatter_about(key_of[14], (FF, D), (FF // 16) ** -0.5, 0.3125, ((0, 2), (1, 16))),
    }


@jax.custom_vjp
def low(v):
    return lax.optimization_barrier(v.astype(jnp.bfloat16)).astype(jnp.float32)

@jax.custom_vjp
def low_back(v):
    return v

def low_keep(v):
    return (low(v), None)

def low_pass(kept, grad):
    return (grad,)

def back_keep(v):
    return (v, None)

def back_low(kept, grad):
    return (low(grad),)
low.defvjp(low_keep, low_pass)
low_back.defvjp(back_keep, back_low)
epsilon = 1e-06
rope_base = 1000000.0
masked_value = -1e+30

def matmul(left, right):
    return jnp.dot(left, right, precision=lax.Precision.HIGHEST, preferred_element_type=jnp.float32)

def rope_tables(positions, head_size):
    half_dim = head_size // 2
    frequency = rope_base ** (-(jnp.arange(half_dim, dtype=jnp.float32) * 2.0) / head_size)
    angles = positions.astype(jnp.float32)[..., None] * frequency
    return (jnp.cos(angles), jnp.sin(angles))

def rotate(values, cosine_table, sine_table):
    half_dim = values.shape[-1] // 2
    first_half = values[..., :half_dim]
    second_half = values[..., half_dim:]
    return jnp.concatenate([first_half * cosine_table - second_half * sine_table, second_half * cosine_table + first_half * sine_table], axis=-1)

def head_norm(raw_heads, gain_vector, cosine_table, sine_table):
    scaled = raw_heads * lax.rsqrt(lax.optimization_barrier(jnp.mean(raw_heads * raw_heads, axis=-1, keepdims=True)) + epsilon) * gain_vector
    return rotate(scaled, cosine_table, sine_table)

def rms_norm(stream, gain_vector):
    return stream * lax.rsqrt(lax.optimization_barrier(jnp.mean(stream * stream, axis=-1, keepdims=True)) + epsilon) * gain_vector

def sequence_layer(stream, seg_row, pos_row, params):
    attn_gain, w_query, w_key, w_value, q_gain, k_gain, w_out, mlp_gain, w_gate, w_up, w_down = params
    seq_len = stream.shape[0]
    head_size = q_gain.shape[0]
    kv_count = w_key.shape[1] // head_size
    group_size = w_query.shape[1] // w_key.shape[1]
    normed_low = low(rms_norm(stream, attn_gain))
    query_raw = low_back(matmul(normed_low, w_query)).reshape(seq_len, kv_count * group_size, head_size)
    key_raw = low_back(matmul(normed_low, w_key)).reshape(seq_len, kv_count, head_size)
    value_low = low(low_back(matmul(normed_low, w_value))).reshape(seq_len, kv_count, head_size)
    cosine_table, sine_table = rope_tables(pos_row, head_size)
    cosine_table = cosine_table[:, None, :]
    sine_table = sine_table[:, None, :]
    query_low = low(head_norm(query_raw, q_gain, cosine_table, sine_table)).reshape(seq_len, kv_count, group_size, head_size)
    key_low = low(head_norm(key_raw, k_gain, cosine_table, sine_table))
    block_rows = math.gcd(seq_len, 512)
    key_index = jnp.arange(seq_len, dtype=jnp.int32)
    score_scale = 1.0 / math.sqrt(head_size)

    def attend_block(block_index):
        first_row = (block_index * block_rows).astype(jnp.int32)
        query_block = lax.dynamic_slice_in_dim(query_low, first_row, block_rows, 0)
        seg_block = lax.dynamic_slice_in_dim(seg_row, first_row, block_rows, 0)
        row_index = first_row + jnp.arange(block_rows, dtype=jnp.int32)
        raw_scores = low_back(jnp.einsum('tkgd,nkd->kgtn', query_block, key_low, precision=lax.Precision.HIGHEST, preferred_element_type=jnp.float32) * score_scale)
        allowed = (key_index[None, :] <= row_index[:, None]) & (seg_row[None, :] == seg_block[:, None])
        masked = jnp.where(allowed, raw_scores, masked_value)
        probability = jax.nn.softmax(masked, axis=-1)
        return jnp.einsum('kgtn,nkd->tkgd', low(probability), value_low, precision=lax.Precision.HIGHEST, preferred_element_type=jnp.float32)
    attended = lax.map(jax.checkpoint(attend_block), jnp.arange(seq_len // block_rows, dtype=jnp.int32))
    attended_low = low(low_back(attended.reshape(seq_len, kv_count * group_size * head_size)))
    middle = stream + low_back(matmul(attended_low, w_out))
    normed_mid = low(rms_norm(middle, mlp_gain))
    gate = low_back(matmul(normed_mid, w_gate))
    upward = low_back(matmul(normed_mid, w_up))
    hidden = low(jax.nn.silu(gate) * upward)
    return middle + matmul(hidden, w_down)

def reference(inputs, segment_ids, positions, out_grad, attn_gain, w_query, w_key, w_value, q_gain, k_gain, w_out, mlp_gain, w_gate, w_up, w_down):
    initials = (inputs, attn_gain, w_query, w_key, w_value, q_gain, k_gain, w_out, mlp_gain, w_gate, w_up, w_down)
    floats = tuple((initial.astype(jnp.float32) for initial in initials))

    def forward(stream, *params):

        def one_sequence(item):
            return sequence_layer(item[0], item[1], item[2], params)
        return lax.map(jax.checkpoint(one_sequence), (stream, segment_ids, positions))
    result, pullback = jax.vjp(forward, *floats)
    gradients = pullback(out_grad.astype(jnp.float32))
    return (result.astype(jnp.bfloat16), gradients[0].astype(jnp.bfloat16), gradients[1], gradients[2], gradients[3], gradients[4], gradients[5], gradients[6], gradients[7], gradients[8], gradients[9], gradients[10], gradients[11])
```

```python
import math

import jax
import jax.numpy as jnp
from jax import lax
from jax.sharding import PartitionSpec as P

HEAD_DIM = 128
BF16 = jnp.bfloat16
F32 = jnp.float32

epsilon = 1e-06
rope_base = 1000000.0
masked_value = -1e30


def from_behind(value, axis, steps):
    count = lax.axis_size(axis)
    pairs = [(source, (source + steps) % count) for source in range(count)]
    return lax.ppermute(value, axis, pairs)


def rope_tables(positions, head_size):
    half_dim = head_size // 2
    frequency = rope_base ** (-(jnp.arange(half_dim, dtype=jnp.float32) * 2.0) / head_size)
    angles = positions.astype(jnp.float32)[..., None] * frequency
    return (jnp.cos(angles), jnp.sin(angles))


def rotate(values, cosine_table, sine_table):
    half_dim = values.shape[-1] // 2
    first_half = values[..., :half_dim]
    second_half = values[..., half_dim:]
    return jnp.concatenate(
        [
            first_half * cosine_table - second_half * sine_table,
            second_half * cosine_table + first_half * sine_table,
        ],
        axis=-1,
    )


def head_norm(raw_heads, gain_vector, cosine_table, sine_table):
    scaled = (
        raw_heads
        * lax.rsqrt(jnp.mean(raw_heads * raw_heads, axis=-1, keepdims=True) + epsilon)
        * gain_vector
    )
    return rotate(scaled, cosine_table, sine_table)


def rms_norm(stream, gain_vector):
    return (
        stream
        * lax.rsqrt(jnp.mean(stream * stream, axis=-1, keepdims=True) + epsilon)
        * gain_vector
    )


def silu_product(gate, upward):
    return jax.nn.silu(gate) * upward


def dot32(left, right, spec):
    return jnp.einsum(spec, left, right, preferred_element_type=F32)


def shift(value, axis, steps):
    count = lax.axis_size(axis)
    pairs = [(source, (source + steps) % count) for source in range(count)]
    return lax.ppermute(value, axis, pairs)


def take_ring(blocks, first):
    return lax.dynamic_slice_in_dim(jnp.concatenate([blocks, blocks]), first, blocks.shape[0], 0)


def reversed_ring(blocks):
    return jnp.concatenate([blocks[:1], blocks[:0:-1]])


def gather_behind(block):
    count = lax.axis_size("ctx")
    return jnp.stack([block] + [shift(block, "ctx", d) for d in range(1, count)])


def scatter_sum(blocks):
    total = blocks[0].astype(F32)
    for d in range(1, blocks.shape[0]):
        total = total + shift(blocks[d], "ctx", -d).astype(F32)
    return total


def swap_by_target(blocks):
    count = lax.axis_size("ctx")
    rank = lax.axis_index("ctx")
    ahead = take_ring(blocks, rank)
    got = jnp.stack([ahead[0]] + [shift(ahead[d], "ctx", d) for d in range(1, count)])
    return take_ring(reversed_ring(got), (count - rank) % count)


def swap_behind(blocks):
    count = lax.axis_size("ctx")
    rank = lax.axis_index("ctx")
    got = jnp.stack([blocks[0]] + [shift(blocks[d], "ctx", -d) for d in range(1, count)])
    return take_ring(got, (count - rank) % count)


def swap_to_behind(blocks):
    count = lax.axis_size("ctx")
    ahead = take_ring(blocks, lax.axis_index("ctx"))
    return jnp.stack([ahead[0]] + [shift(ahead[d], "ctx", d) for d in range(1, count)])


def slices_of(shard):
    count = lax.axis_size("ctx")
    rows, width = shard.shape
    mine = swap_by_target(shard.reshape(rows, count, width // count).transpose(1, 0, 2))
    mine = mine.reshape(count * rows, width // count)
    full = lax.all_gather(mine, ("tensor", "dp"), axis=0, tiled=True)
    tensors = lax.axis_size("tensor")
    return full.reshape(tensors, full.shape[0] // tensors, full.shape[1])


def shards_of(partial):
    count = lax.axis_size("ctx")
    width = partial.shape[2]
    flat = partial.astype(BF16).reshape(-1, width)
    mine = lax.psum_scatter(flat, ("tensor", "dp"), scatter_dimension=0, tiled=True)
    got = swap_by_target(mine.reshape(count, mine.shape[0] // count, width))
    return got.transpose(1, 0, 2).reshape(got.shape[1], count * width).astype(F32)


def with_twin(own):
    other = shift(own, "tensor", 1)
    first = lax.axis_index("tensor") == 0
    return jnp.concatenate([jnp.where(first, own, other), jnp.where(first, other, own)])


def on_device_sliced(
    inputs,
    segment_ids,
    positions,
    out_grad,
    attn_gain,
    w_query,
    w_key,
    w_value,
    q_gain,
    k_gain,
    w_out,
    mlp_gain,
    w_gate,
    w_up,
    w_down,
):
    _, tok_count, width = inputs.shape
    count = lax.axis_size("ctx")
    tensors = lax.axis_size("tensor")
    rank = lax.axis_index("ctx")
    half = lax.axis_index("tensor")
    own_rows = tok_count // tensors
    rows = own_rows * count
    head_rows = w_out.shape[0]
    score_scale = 1.0 / math.sqrt(HEAD_DIM)

    q_cols = w_query.shape[1] // count
    k_cols = w_key.shape[1] // count
    local_kv = k_cols // HEAD_DIM
    group = q_cols // k_cols
    in_width = q_cols + 2 * k_cols
    in_shard = jnp.concatenate(
        [
            w_query.reshape(-1, count, q_cols),
            w_key.reshape(-1, count, k_cols),
            w_value.reshape(-1, count, k_cols),
        ],
        axis=2,
    ).reshape(w_query.shape[0], count * in_width)
    in_weight = slices_of(in_shard)
    out_weight = lax.all_gather(w_out.T, ("tensor", "dp", "ctx"), axis=0, tiled=True).reshape(
        tensors, width, head_rows
    )
    gate_weight = slices_of(w_gate)
    up_weight = slices_of(w_up)
    down_weight = slices_of(w_down.T)

    gains = lax.all_gather(
        jnp.concatenate([attn_gain, mlp_gain, q_gain, k_gain]), ("dp", "ctx"), axis=0
    )
    piece = attn_gain.shape[0]
    small = q_gain.shape[0]
    attn_scale = gains[:, :piece].reshape(-1).astype(F32)
    mlp_scale = gains[:, piece : 2 * piece].reshape(-1).astype(F32)
    query_scale = gains[:, 2 * piece : 2 * piece + small].reshape(-1).astype(F32)
    key_scale = gains[:, 2 * piece + small :].reshape(-1).astype(F32)

    marks = lax.all_gather(jnp.stack([segment_ids[0], positions[0]]), "ctx", axis=0)
    marks = marks.reshape(count, 2, tensors, own_rows)
    behind = (rank - jnp.arange(count)) % count
    marks = marks[behind]
    starts = behind * tok_count
    offsets = starts[:, None] + jnp.arange(own_rows)[None, :]

    def marks_of(which):
        segs = lax.dynamic_index_in_dim(marks[:, 0], which, 1, keepdims=False).reshape(rows)
        return segs, (offsets + which * own_rows).reshape(rows)

    own_segs, own_index = marks_of(half)
    twin_segs, twin_index = marks_of(1 - half)
    own_positions = lax.dynamic_index_in_dim(marks[:, 1], half, 1, keepdims=False).reshape(rows)
    key_segs = jnp.concatenate([own_segs, twin_segs])
    key_index = jnp.concatenate([own_index, twin_index])
    allowed = (key_index[None, :] <= own_index[:, None]) & (key_segs[None, :] == own_segs[:, None])

    stream = lax.dynamic_slice_in_dim(inputs[0], half * own_rows, own_rows, 0).astype(F32)
    grad_own = lax.dynamic_slice_in_dim(out_grad[0], half * own_rows, own_rows, 0)
    normed_attn, attn_norm_pullback = jax.vjp(rms_norm, stream, attn_scale)
    normed_low = gather_behind(normed_attn.astype(BF16)).reshape(rows, width)
    raw = dot32(normed_low, in_weight, "mk,tkc->mtc")
    query_raw = raw[..., :q_cols].reshape(rows, tensors * local_kv * group, HEAD_DIM)
    key_raw = raw[..., q_cols : q_cols + k_cols].reshape(rows, tensors * local_kv, HEAD_DIM)
    kv_heads = tensors * local_kv
    value_low = raw[..., q_cols + k_cols :].astype(BF16).reshape(rows, kv_heads, HEAD_DIM)
    cosine_table, sine_table = rope_tables(own_positions, HEAD_DIM)
    cosine_table = cosine_table[:, None, :]
    sine_table = sine_table[:, None, :]

    def norm_rope(raw_heads, gain_vector):
        return head_norm(raw_heads, gain_vector, cosine_table, sine_table)

    query_rot, query_pullback = jax.vjp(norm_rope, query_raw, query_scale)
    key_rot, key_pullback = jax.vjp(norm_rope, key_raw, key_scale)
    query_low = query_rot.astype(BF16).reshape(rows, kv_heads, group, HEAD_DIM)
    key_low = key_rot.astype(BF16)
    kv_own = jnp.stack([key_low, value_low])
    kv_all = jnp.concatenate([kv_own, shift(kv_own, "tensor", 1)], axis=1)
    keys, values = kv_all[0], kv_all[1]

    scores = dot32(query_low, keys, "mkgd,nkd->kgmn") * score_scale
    masked = jnp.where(allowed, scores, masked_value)
    best = jnp.max(masked, axis=-1, keepdims=True)
    weights = jnp.where(allowed, jnp.exp(masked - best), 0.0)
    total = jnp.sum(weights, axis=-1, keepdims=True)
    prob = weights / total
    prob_low = prob.astype(BF16)
    attended = dot32(prob_low, values, "kgmn,nkd->mkgd")
    attended_heads = attended.astype(BF16).reshape(count, own_rows, tensors, q_cols)
    attended_own = swap_behind(attended_heads)
    attended_own = attended_own.transpose(1, 2, 0, 3).reshape(own_rows, tensors, head_rows)
    middle = stream + dot32(attended_own, out_weight, "mtr,tkr->mk")
    normed_mid, mlp_norm_pullback = jax.vjp(rms_norm, middle, mlp_scale)
    mid_low = gather_behind(normed_mid.astype(BF16)).reshape(rows, width)
    grad_low = gather_behind(grad_own).reshape(rows, width)

    gate = dot32(mid_low, gate_weight, "mk,tkc->tmc")
    upward = dot32(mid_low, up_weight, "mk,tkc->tmc")
    hidden, silu_pullback = jax.vjp(silu_product, gate, upward)
    hidden_low = hidden.astype(BF16)
    hidden_grad = dot32(grad_low, down_weight, "mk,tkc->tmc")
    gate_grad, upward_grad = silu_pullback(hidden_grad)
    gate_grad_low = gate_grad.astype(BF16)
    upward_grad_low = upward_grad.astype(BF16)
    mid_grad_part = dot32(gate_grad_low, gate_weight, "tmc,tkc->mk") + dot32(
        upward_grad_low, up_weight, "tmc,tkc->mk"
    )
    mid_grad = scatter_sum(mid_grad_part.astype(BF16).reshape(count, own_rows, width))
    down_part = dot32(hidden_low, down_weight, "tmc,tkc->mk")
    down_sum = scatter_sum(down_part.astype(BF16).reshape(count, own_rows, width))
    output = with_twin((middle + down_sum).astype(BF16))[None]
    down_weight_grad = shards_of(dot32(grad_low, hidden_low, "mk,tmc->tkc")).T
    gate_weight_grad = shards_of(dot32(mid_low, gate_grad_low, "mk,tmc->tkc"))
    up_weight_grad = shards_of(dot32(mid_low, upward_grad_low, "mk,tmc->tkc"))

    middle_norm_grad, mlp_gain_grad = mlp_norm_pullback(mid_grad)
    middle_grad = grad_own.astype(F32) + middle_norm_grad
    branch_grad = middle_grad.astype(BF16)
    out_weight_grad = dot32(branch_grad, attended_own, "mk,mtr->tkr").astype(BF16)
    out_weight_grad = (
        lax.psum_scatter(
            out_weight_grad.reshape(tensors * width, head_rows),
            ("tensor", "dp", "ctx"),
            scatter_dimension=0,
            tiled=True,
        )
        .astype(F32)
        .T
    )
    attended_grad = dot32(branch_grad, out_weight, "mk,tkr->mtr").astype(BF16)
    attended_grad = attended_grad.reshape(own_rows, tensors, count, q_cols).transpose(2, 0, 1, 3)
    attended_grad = swap_to_behind(attended_grad).reshape(rows, kv_heads, group, HEAD_DIM)
    prob_grad = dot32(attended_grad, values, "mkgd,nkd->kgmn")
    delta = jnp.sum(prob * prob_grad, axis=-1, keepdims=True)
    score_grad = (prob * (prob_grad - delta)).astype(BF16)
    query_grad = dot32(score_grad, keys, "kgmn,nkd->mkgd") * score_scale
    key_grad_all = dot32(score_grad, query_low, "kgmn,mkgd->nkd")
    value_grad_all = dot32(prob_low, attended_grad, "kgmn,mkgd->nkd")
    kv_grad_all = jnp.stack([key_grad_all, value_grad_all])
    kv_grad = kv_grad_all[:, :rows] + shift(
        kv_grad_all[:, rows:].astype(BF16), "tensor", 1
    ).astype(F32)
    query_raw_grad, query_gain_grad = query_pullback(query_grad.reshape(query_raw.shape))
    key_raw_grad, key_gain_grad = key_pullback(kv_grad[0] * score_scale)
    raw_grad_low = jnp.concatenate(
        [
            query_raw_grad.astype(BF16).reshape(rows, tensors, q_cols),
            key_raw_grad.astype(BF16).reshape(rows, tensors, k_cols),
            kv_grad[1].astype(BF16).reshape(rows, tensors, k_cols),
        ],
        axis=2,
    )
    normed_grad_part = dot32(raw_grad_low, in_weight, "mtc,tkc->mk")
    normed_grad = scatter_sum(normed_grad_part.astype(BF16).reshape(count, own_rows, width))
    in_weight_grad = shards_of(dot32(normed_low, raw_grad_low, "mk,mtc->tkc"))
    in_weight_grad = in_weight_grad.reshape(-1, count, in_width)
    query_weight_grad = in_weight_grad[..., :q_cols].reshape(w_query.shape)
    key_weight_grad = in_weight_grad[..., q_cols : q_cols + k_cols].reshape(w_key.shape)
    value_weight_grad = in_weight_grad[..., q_cols + k_cols :].reshape(w_value.shape)
    stream_norm_grad, attn_gain_grad = attn_norm_pullback(normed_grad)
    input_grad = with_twin((middle_grad + stream_norm_grad).astype(BF16))[None]

    gain_grads = jnp.concatenate(
        [
            attn_gain_grad.reshape(-1, piece),
            mlp_gain_grad.reshape(-1, piece),
            query_gain_grad.reshape(-1, small),
            key_gain_grad.reshape(-1, small),
        ],
        axis=1,
    )
    gain_grads = lax.psum(gain_grads, ("dp", "ctx", "tensor"))
    owner = lax.axis_index("dp") * count + rank
    gain_grads = lax.dynamic_index_in_dim(gain_grads, owner, 0, keepdims=False)
    return (
        output,
        input_grad,
        gain_grads[:piece],
        query_weight_grad,
        key_weight_grad,
        value_weight_grad,
        gain_grads[2 * piece : 2 * piece + small],
        gain_grads[2 * piece + small :],
        out_weight_grad,
        gain_grads[piece : 2 * piece],
        gate_weight_grad,
        up_weight_grad,
        down_weight_grad,
    )


def can_slice(mesh, inputs, w_key, w_gate):
    tensors, count = mesh.shape["tensor"], mesh.shape["ctx"]
    return (
        tensors == 2
        and inputs.shape[0] == mesh.shape["dp"]
        and (inputs.shape[1] // count) % (16 * tensors) == 0
        and w_key.shape[1] % (tensors * count * HEAD_DIM) == 0
        and w_gate.shape[1] % (tensors * count * 128) == 0
    )


def from_behind(value, axis, steps):
    return shift(value, axis, steps)


def on_device(
    inputs,
    segment_ids,
    positions,
    out_grad,
    attn_gain,
    w_query,
    w_key,
    w_value,
    q_gain,
    k_gain,
    w_out,
    mlp_gain,
    w_gate,
    w_up,
    w_down,
):
    seq_count, tok_count, width = inputs.shape
    row_count = seq_count * tok_count
    cycle_size = lax.axis_size("ctx")
    cycle_rank = lax.axis_index("ctx")
    gathered_attn = (
        lax.all_gather(w_query, ("dp", "ctx"), axis=0, tiled=True),
        lax.all_gather(w_key, ("dp", "ctx"), axis=0, tiled=True),
        lax.all_gather(w_value, ("dp", "ctx"), axis=0, tiled=True),
        lax.all_gather(w_out, ("dp", "ctx"), axis=1, tiled=True),
        lax.all_gather(attn_gain, ("dp", "ctx"), axis=0, tiled=True),
        lax.all_gather(q_gain, ("dp", "ctx"), axis=0, tiled=True),
        lax.all_gather(k_gain, ("dp", "ctx"), axis=0, tiled=True),
    )
    query_weight, key_weight, value_weight, out_weight, attn_scale, query_scale, key_scale = (
        gathered_attn
    )
    gathered_mlp = (
        lax.all_gather(w_gate, ("dp", "ctx"), axis=0, tiled=True),
        lax.all_gather(w_up, ("dp", "ctx"), axis=0, tiled=True),
        lax.all_gather(w_down, ("dp", "ctx"), axis=1, tiled=True),
        lax.all_gather(mlp_gain, ("dp", "ctx"), axis=0, tiled=True),
    )
    gate_weight, up_weight, down_weight, mlp_scale = gathered_mlp
    segments_all = lax.all_gather(segment_ids, "ctx", axis=1, tiled=True)
    local_heads = query_weight.shape[1] // HEAD_DIM
    local_kv = key_weight.shape[1] // HEAD_DIM
    group_size = local_heads // local_kv
    kv_width = local_kv * HEAD_DIM
    score_scale = 1.0 / math.sqrt(HEAD_DIM)
    stream = inputs.astype(jnp.float32).reshape(row_count, width)
    normed_attn, attn_norm_pullback = jax.vjp(rms_norm, stream, attn_scale.astype(jnp.float32))
    normed_low = normed_attn.astype(jnp.bfloat16)
    query_raw = jnp.dot(normed_low, query_weight, preferred_element_type=jnp.float32).reshape(
        seq_count, tok_count, local_heads, HEAD_DIM
    )
    key_raw = jnp.dot(normed_low, key_weight, preferred_element_type=jnp.float32).reshape(
        seq_count, tok_count, local_kv, HEAD_DIM
    )
    value_low = (
        jnp.dot(normed_low, value_weight, preferred_element_type=jnp.float32)
        .astype(jnp.bfloat16)
        .reshape(seq_count, tok_count, kv_width)
    )
    cosine_table, sine_table = rope_tables(positions, HEAD_DIM)
    cosine_table = cosine_table[:, :, None, :]
    sine_table = sine_table[:, :, None, :]

    def norm_rope(raw_heads, gain_vector):
        return head_norm(raw_heads, gain_vector, cosine_table, sine_table)

    query_rot, query_pullback = jax.vjp(norm_rope, query_raw, query_scale.astype(jnp.float32))
    key_rot, key_pullback = jax.vjp(norm_rope, key_raw, key_scale.astype(jnp.float32))
    query_low = query_rot.astype(jnp.bfloat16).reshape(
        seq_count, tok_count, local_kv, group_size, HEAD_DIM
    )
    key_low = key_rot.astype(jnp.bfloat16).reshape(seq_count, tok_count, kv_width)
    query_index = cycle_rank * tok_count + jnp.arange(tok_count, dtype=jnp.int32)

    def block_scores(key_block, first_row):
        key_count = key_block.shape[1]
        key_heads = key_block.reshape(seq_count, key_count, local_kv, HEAD_DIM)
        raw_scores = (
            jnp.einsum(
                "stkgd,snkd->skgtn", query_low, key_heads, preferred_element_type=jnp.float32
            )
            * score_scale
        )
        key_index = first_row + jnp.arange(key_count, dtype=jnp.int32)
        key_segments = lax.dynamic_slice_in_dim(segments_all, first_row, key_count, 1)
        allowed = (key_index[None, None, :] <= query_index[None, :, None]) & (
            key_segments[:, None, :] == segment_ids[:, :, None]
        )
        return (raw_scores, allowed[:, None, None, :, :])

    stat_shape = (seq_count, local_kv, group_size, tok_count)
    pieces = (
        lax.all_gather(key_low, "ctx", axis=1, tiled=True),
        lax.all_gather(value_low, "ctx", axis=1, tiled=True),
    )
    row_best = jnp.full(stat_shape, masked_value, jnp.float32)
    raw_scores, allowed = block_scores(pieces[0], jnp.int32(0))
    masked = jnp.where(allowed, raw_scores, masked_value)
    new_best = jnp.maximum(row_best, jnp.max(masked, axis=-1))
    weights = jnp.where(allowed, jnp.exp(masked - new_best[..., None]), 0.0)
    value_heads = pieces[1].reshape(seq_count, pieces[1].shape[1], local_kv, HEAD_DIM)
    added = jnp.einsum(
        "skgtn,snkd->skgtd",
        weights.astype(jnp.bfloat16),
        value_heads,
        preferred_element_type=jnp.float32,
    )
    row_total = jnp.sum(weights, axis=-1)
    log_total = new_best + jnp.log(row_total)
    attended = added / row_total[..., None]
    attended_low = (
        jnp.transpose(attended, (0, 3, 1, 2, 4))
        .reshape(row_count, local_heads * HEAD_DIM)
        .astype(jnp.bfloat16)
    )
    attn_part = jnp.dot(attended_low, out_weight, preferred_element_type=jnp.float32)
    middle = stream + lax.psum(attn_part.astype(jnp.bfloat16), "tensor").astype(jnp.float32)
    normed_mid, mlp_norm_pullback = jax.vjp(rms_norm, middle, mlp_scale.astype(jnp.float32))
    mid_low = normed_mid.astype(jnp.bfloat16)
    gate = jnp.dot(mid_low, gate_weight, preferred_element_type=jnp.float32)
    upward = jnp.dot(mid_low, up_weight, preferred_element_type=jnp.float32)
    hidden, silu_pullback = jax.vjp(silu_product, gate, upward)
    hidden_low = hidden.astype(jnp.bfloat16)
    down_part = jnp.dot(hidden_low, down_weight, preferred_element_type=jnp.float32)
    down_sum = lax.psum(down_part.astype(jnp.bfloat16), "tensor").astype(jnp.float32)
    output = (middle + down_sum).astype(jnp.bfloat16).reshape(seq_count, tok_count, width)
    grad_low = out_grad.reshape(row_count, width)
    down_weight_grad = jnp.dot(hidden_low.T, grad_low, preferred_element_type=jnp.float32)
    hidden_grad = jnp.dot(grad_low, down_weight.T, preferred_element_type=jnp.float32)
    gate_grad, upward_grad = silu_pullback(hidden_grad)
    gate_grad_low = gate_grad.astype(jnp.bfloat16)
    upward_grad_low = upward_grad.astype(jnp.bfloat16)
    gate_weight_grad = jnp.dot(mid_low.T, gate_grad_low, preferred_element_type=jnp.float32)
    up_weight_grad = jnp.dot(mid_low.T, upward_grad_low, preferred_element_type=jnp.float32)
    mid_grad_part = jnp.dot(
        gate_grad_low, gate_weight.T, preferred_element_type=jnp.float32
    ) + jnp.dot(upward_grad_low, up_weight.T, preferred_element_type=jnp.float32)
    mid_grad = lax.psum(mid_grad_part.astype(jnp.bfloat16), "tensor").astype(jnp.float32)
    middle_norm_grad, mlp_gain_grad = mlp_norm_pullback(mid_grad)
    middle_grad = grad_low.astype(jnp.float32) + middle_norm_grad
    mlp_grads = (
        lax.psum_scatter(gate_weight_grad, ("dp", "ctx"), scatter_dimension=0, tiled=True),
        lax.psum_scatter(up_weight_grad, ("dp", "ctx"), scatter_dimension=0, tiled=True),
        lax.psum_scatter(down_weight_grad, ("dp", "ctx"), scatter_dimension=1, tiled=True),
        lax.psum_scatter(mlp_gain_grad, ("dp", "ctx"), scatter_dimension=0, tiled=True),
    )
    branch_grad = middle_grad.astype(jnp.bfloat16)
    out_weight_grad = jnp.dot(attended_low.T, branch_grad, preferred_element_type=jnp.float32)
    attended_grad = jnp.dot(branch_grad, out_weight.T, preferred_element_type=jnp.float32).astype(
        jnp.bfloat16
    )
    attended_grad_heads = jnp.transpose(
        attended_grad.reshape(seq_count, tok_count, local_kv, group_size, HEAD_DIM), (0, 2, 3, 1, 4)
    )
    row_delta = jnp.sum(attended_grad_heads.astype(jnp.float32) * attended, axis=-1)

    def key_block_grads(key_block, value_block, first_row):
        raw_scores, allowed = block_scores(key_block, first_row)
        probability = jnp.where(allowed, jnp.exp(raw_scores - log_total[..., None]), 0.0)
        key_count = key_block.shape[1]
        value_heads = value_block.reshape(seq_count, key_count, local_kv, HEAD_DIM)
        key_heads = key_block.reshape(seq_count, key_count, local_kv, HEAD_DIM)
        prob_grad = jnp.einsum(
            "skgtd,snkd->skgtn",
            attended_grad_heads,
            value_heads,
            preferred_element_type=jnp.float32,
        )
        score_grad = (probability * (prob_grad - row_delta[..., None])).astype(jnp.bfloat16)
        query_add = jnp.einsum(
            "skgtn,snkd->skgtd", score_grad, key_heads, preferred_element_type=jnp.float32
        )
        key_add = jnp.einsum(
            "skgtn,stkgd->snkd", score_grad, query_low, preferred_element_type=jnp.float32
        ).reshape(seq_count, key_count, kv_width)
        value_add = jnp.einsum(
            "skgtn,skgtd->snkd",
            probability.astype(jnp.bfloat16),
            attended_grad_heads,
            preferred_element_type=jnp.float32,
        ).reshape(seq_count, key_count, kv_width)
        return (query_add, key_add, value_add)

    query_zero = jnp.zeros(stat_shape + (HEAD_DIM,), jnp.float32)
    kv_zero = jnp.zeros((seq_count, tok_count, kv_width), jnp.float32)

    def cycle_turn(turn_index, state):
        key_block, value_block, key_grad_acc, value_grad_acc, query_grad_acc = state
        owner_rank = (cycle_rank + turn_index) % cycle_size
        query_add, key_add, value_add = key_block_grads(
            key_block, value_block, owner_rank * tok_count
        )
        moved_blocks = from_behind((key_block, value_block), "ctx", -1)
        moved_grads = (
            from_behind((key_grad_acc + key_add).astype(jnp.bfloat16), "ctx", -1).astype(
                jnp.float32
            ),
            from_behind((value_grad_acc + value_add).astype(jnp.bfloat16), "ctx", -1).astype(
                jnp.float32
            ),
        )
        return (
            moved_blocks[0],
            moved_blocks[1],
            moved_grads[0],
            moved_grads[1],
            query_grad_acc + query_add,
        )

    final_state = lax.fori_loop(
        0, cycle_size, cycle_turn, (key_low, value_low, kv_zero, kv_zero, query_zero)
    )
    key_grad_sum = final_state[2]
    value_grad_sum = final_state[3]
    query_grad_sum = final_state[4]
    query_grad = (
        jnp.transpose(query_grad_sum, (0, 3, 1, 2, 4)).reshape(
            seq_count, tok_count, local_heads, HEAD_DIM
        )
        * score_scale
    )
    query_raw_grad, query_gain_grad = query_pullback(query_grad)
    key_raw_grad, key_gain_grad = key_pullback(
        (key_grad_sum * score_scale).reshape(seq_count, tok_count, local_kv, HEAD_DIM)
    )
    query_grad_low = query_raw_grad.reshape(row_count, local_heads * HEAD_DIM).astype(jnp.bfloat16)
    key_grad_low = key_raw_grad.reshape(row_count, kv_width).astype(jnp.bfloat16)
    value_grad_low = value_grad_sum.reshape(row_count, kv_width).astype(jnp.bfloat16)
    query_weight_grad = jnp.dot(normed_low.T, query_grad_low, preferred_element_type=jnp.float32)
    key_weight_grad = jnp.dot(normed_low.T, key_grad_low, preferred_element_type=jnp.float32)
    value_weight_grad = jnp.dot(normed_low.T, value_grad_low, preferred_element_type=jnp.float32)
    normed_grad_part = (
        jnp.dot(query_grad_low, query_weight.T, preferred_element_type=jnp.float32)
        + jnp.dot(key_grad_low, key_weight.T, preferred_element_type=jnp.float32)
        + jnp.dot(value_grad_low, value_weight.T, preferred_element_type=jnp.float32)
    )
    normed_grad, query_gain_total, key_gain_total = (
        lax.psum(normed_grad_part.astype(jnp.bfloat16), "tensor").astype(jnp.float32),
        lax.psum(query_gain_grad.astype(jnp.bfloat16), "tensor").astype(jnp.float32),
        lax.psum(key_gain_grad.astype(jnp.bfloat16), "tensor").astype(jnp.float32),
    )
    stream_norm_grad, attn_gain_grad = attn_norm_pullback(normed_grad)
    input_grad = (
        (middle_grad + stream_norm_grad).astype(jnp.bfloat16).reshape(seq_count, tok_count, width)
    )
    attn_grads = (
        lax.psum_scatter(query_weight_grad, ("dp", "ctx"), scatter_dimension=0, tiled=True),
        lax.psum_scatter(key_weight_grad, ("dp", "ctx"), scatter_dimension=0, tiled=True),
        lax.psum_scatter(value_weight_grad, ("dp", "ctx"), scatter_dimension=0, tiled=True),
        lax.psum_scatter(out_weight_grad, ("dp", "ctx"), scatter_dimension=1, tiled=True),
        lax.psum_scatter(attn_gain_grad, ("dp", "ctx"), scatter_dimension=0, tiled=True),
        lax.psum_scatter(query_gain_total, ("dp", "ctx"), scatter_dimension=0, tiled=True),
        lax.psum_scatter(key_gain_total, ("dp", "ctx"), scatter_dimension=0, tiled=True),
    )
    return (
        output,
        input_grad,
        attn_grads[4],
        attn_grads[0],
        attn_grads[1],
        attn_grads[2],
        attn_grads[5],
        attn_grads[6],
        attn_grads[3],
        mlp_grads[3],
        mlp_grads[0],
        mlp_grads[1],
        mlp_grads[2],
    )


def solution(mesh):
    in_specs = (
        P("dp", "ctx", None),
        P("dp", "ctx"),
        P("dp", "ctx"),
        P("dp", "ctx", None),
        P(("dp", "ctx")),
        P(("dp", "ctx"), "tensor"),
        P(("dp", "ctx"), "tensor"),
        P(("dp", "ctx"), "tensor"),
        P(("dp", "ctx")),
        P(("dp", "ctx")),
        P("tensor", ("dp", "ctx")),
        P(("dp", "ctx")),
        P(("dp", "ctx"), "tensor"),
        P(("dp", "ctx"), "tensor"),
        P("tensor", ("dp", "ctx")),
    )
    out_specs = (
        P("dp", "ctx", None),
        P("dp", "ctx", None),
        P(("dp", "ctx")),
        P(("dp", "ctx"), "tensor"),
        P(("dp", "ctx"), "tensor"),
        P(("dp", "ctx"), "tensor"),
        P(("dp", "ctx")),
        P(("dp", "ctx")),
        P("tensor", ("dp", "ctx")),
        P(("dp", "ctx")),
        P(("dp", "ctx"), "tensor"),
        P(("dp", "ctx"), "tensor"),
        P("tensor", ("dp", "ctx")),
    )

    def step(*args):
        body = on_device_sliced if can_slice(mesh, args[0], args[6], args[12]) else on_device
        return jax.shard_map(
            body, mesh=mesh, in_specs=in_specs, out_specs=out_specs, check_vma=False
        )(*args)

    return step
```

```python
import math

import jax
import jax.numpy as jnp
from jax import lax
from jax.experimental import pallas as pl
from jax.experimental.pallas import tpu as pltpu
from jax.sharding import PartitionSpec as P

HEAD_DIM = 128
BF16 = jnp.bfloat16
F32 = jnp.float32
MESH = pl.DeviceIdType.MESH
TILE = (8, 128)

epsilon = 1e-06
rope_base = 1000000.0
masked_value = -1e30


def from_behind(value, axis, steps):
    count = lax.axis_size(axis)
    pairs = [(source, (source + steps) % count) for source in range(count)]
    return lax.ppermute(value, axis, pairs)


def rope_tables(positions, head_size):
    half_dim = head_size // 2
    frequency = rope_base ** (-(jnp.arange(half_dim, dtype=jnp.float32) * 2.0) / head_size)
    angles = positions.astype(jnp.float32)[..., None] * frequency
    return (jnp.cos(angles), jnp.sin(angles))


def rotate(values, cosine_table, sine_table):
    half_dim = values.shape[-1] // 2
    first_half = values[..., :half_dim]
    second_half = values[..., half_dim:]
    return jnp.concatenate(
        [
            first_half * cosine_table - second_half * sine_table,
            second_half * cosine_table + first_half * sine_table,
        ],
        axis=-1,
    )


def head_norm(raw_heads, gain_vector, cosine_table, sine_table):
    scaled = (
        raw_heads
        * lax.rsqrt(jnp.mean(raw_heads * raw_heads, axis=-1, keepdims=True) + epsilon)
        * gain_vector
    )
    return rotate(scaled, cosine_table, sine_table)


def rms_norm(stream, gain_vector):
    return (
        stream
        * lax.rsqrt(jnp.mean(stream * stream, axis=-1, keepdims=True) + epsilon)
        * gain_vector
    )


def silu_product(gate, upward):
    return jax.nn.silu(gate) * upward


def dot32(left, right, spec):
    return jnp.einsum(spec, left, right, preferred_element_type=F32)


def shift(value, axis, steps):
    count = lax.axis_size(axis)
    pairs = [(source, (source + steps) % count) for source in range(count)]
    return lax.ppermute(value, axis, pairs)


def take_ring(blocks, first):
    return lax.dynamic_slice_in_dim(jnp.concatenate([blocks, blocks]), first, blocks.shape[0], 0)


def reversed_ring(blocks):
    return jnp.concatenate([blocks[:1], blocks[:0:-1]])


def gather_behind(block):
    count = lax.axis_size("ctx")
    return jnp.stack([block] + [shift(block, "ctx", d) for d in range(1, count)])


def scatter_sum(blocks):
    total = blocks[0].astype(F32)
    for d in range(1, blocks.shape[0]):
        total = total + shift(blocks[d], "ctx", -d).astype(F32)
    return total


def swap_by_target(blocks):
    count = lax.axis_size("ctx")
    rank = lax.axis_index("ctx")
    ahead = take_ring(blocks, rank)
    got = jnp.stack([ahead[0]] + [shift(ahead[d], "ctx", d) for d in range(1, count)])
    return take_ring(reversed_ring(got), (count - rank) % count)


def swap_behind(blocks):
    count = lax.axis_size("ctx")
    rank = lax.axis_index("ctx")
    got = jnp.stack([blocks[0]] + [shift(blocks[d], "ctx", -d) for d in range(1, count)])
    return take_ring(got, (count - rank) % count)


def swap_to_behind(blocks):
    count = lax.axis_size("ctx")
    ahead = take_ring(blocks, lax.axis_index("ctx"))
    return jnp.stack([ahead[0]] + [shift(ahead[d], "ctx", d) for d in range(1, count)])


def greet(peers):
    barrier = pltpu.get_barrier_semaphore()
    for peer in peers:
        pl.semaphore_signal(barrier, inc=1, device_id=peer, device_id_type=MESH)
    pl.semaphore_wait(barrier, len(peers))


def remote(source, target, send_sem, recv_sem, peer):
    copy = pltpu.make_async_remote_copy(
        src_ref=source,
        dst_ref=target,
        send_sem=send_sem,
        recv_sem=recv_sem,
        device_id=peer,
        device_id_type=MESH,
    )
    copy.start()
    return copy


def to_tile(values):
    return jnp.pad(values, (0, math.prod(TILE) - values.shape[0])).reshape(TILE)


def spread_small(gains, marks):
    count, pairs = lax.axis_size("ctx"), lax.axis_size("dp")
    owners = count * pairs

    def kernel(gain_ref, mark_ref, gains_ref, marks_ref, gain_send, gain_recv, mark_send, mark_recv):
        rank = lax.axis_index("ctx")
        me = lax.axis_index("dp") * count + rank
        far = [lax.rem(me + k, owners) for k in range(1, owners)]
        far = [{"dp": lax.div(t, count), "ctx": lax.rem(t, count)} for t in far]
        near = [{"ctx": lax.rem(rank + k, count)} for k in range(1, count)]
        greet(far)
        copies = [
            remote(mark_ref, marks_ref.at[rank], mark_send.at[k], mark_recv.at[k], peer)
            for k, peer in enumerate(near)
        ]
        copies += [
            remote(gain_ref, gains_ref.at[me], gain_send.at[k], gain_recv.at[k], peer)
            for k, peer in enumerate(far)
        ]
        gains_ref[me] = gain_ref[...]
        marks_ref[rank] = mark_ref[...]
        for copy in copies:
            copy.wait()

    sems = pltpu.SemaphoreType.DMA
    return pl.pallas_call(
        kernel,
        out_shape=(
            jax.ShapeDtypeStruct((owners, *TILE), F32),
            jax.ShapeDtypeStruct((count, *TILE), jnp.int32),
        ),
        in_specs=[pl.BlockSpec(memory_space=pltpu.VMEM)] * 2,
        out_specs=(pl.BlockSpec(memory_space=pltpu.VMEM),) * 2,
        scratch_shapes=[
            sems((owners - 1,)),
            sems((owners - 1,)),
            sems((count - 1,)),
            sems((count - 1,)),
        ],
        compiler_params=pltpu.CompilerParams(collective_id=0, has_side_effects=True),
        name="spread_small",
    )(gains, marks)


def owner_sums(tiles):
    count, pairs, tensors = lax.axis_size("ctx"), lax.axis_size("dp"), lax.axis_size("tensor")
    total = count * pairs * tensors

    def kernel(tiles_ref, sum_ref, got, send_sem, recv_sem):
        owner = lax.axis_index("dp") * count + lax.axis_index("ctx")
        me = owner * tensors + lax.axis_index("tensor")
        targets = [lax.rem(me + k, total) for k in range(1, total)]
        peers = [
            {
                "dp": lax.div(t, count * tensors),
                "ctx": lax.rem(lax.div(t, tensors), count),
                "tensor": lax.rem(t, tensors),
            }
            for t in targets
        ]
        greet(peers)
        copies = [
            remote(
                tiles_ref.at[lax.div(t, tensors)], got.at[me], send_sem.at[k], recv_sem.at[k], peer
            )
            for k, (t, peer) in enumerate(zip(targets, peers))
        ]
        got[me] = tiles_ref[owner]
        for copy in copies:
            copy.wait()
        value = got[0]
        for source in range(1, total):
            value = value + got[source]
        sum_ref[...] = value

    return pl.pallas_call(
        kernel,
        out_shape=jax.ShapeDtypeStruct(TILE, F32),
        in_specs=[pl.BlockSpec(memory_space=pltpu.VMEM)],
        out_specs=pl.BlockSpec(memory_space=pltpu.VMEM),
        scratch_shapes=[
            pltpu.VMEM((total, *TILE), F32),
            pltpu.SemaphoreType.DMA((total - 1,)),
            pltpu.SemaphoreType.DMA((total - 1,)),
        ],
        compiler_params=pltpu.CompilerParams(collective_id=1, has_side_effects=True),
        name="owner_sums",
    )(tiles)


def slices_of(shard):
    count = lax.axis_size("ctx")
    rows, width = shard.shape
    mine = swap_by_target(shard.reshape(rows, count, width // count).transpose(1, 0, 2))
    mine = mine.reshape(count * rows, width // count)
    full = lax.all_gather(mine, ("tensor", "dp"), axis=0, tiled=True)
    tensors = lax.axis_size("tensor")
    return full.reshape(tensors, full.shape[0] // tensors, full.shape[1])


def shards_of(partial):
    count = lax.axis_size("ctx")
    width = partial.shape[2]
    flat = partial.astype(BF16).reshape(-1, width)
    mine = lax.psum_scatter(flat, ("tensor", "dp"), scatter_dimension=0, tiled=True)
    got = swap_by_target(mine.reshape(count, mine.shape[0] // count, width))
    return got.transpose(1, 0, 2).reshape(got.shape[1], count * width).astype(F32)


def with_twin(own):
    other = shift(own, "tensor", 1)
    first = lax.axis_index("tensor") == 0
    return jnp.concatenate([jnp.where(first, own, other), jnp.where(first, other, own)])


def on_device_sliced(
    inputs,
    segment_ids,
    positions,
    out_grad,
    attn_gain,
    w_query,
    w_key,
    w_value,
    q_gain,
    k_gain,
    w_out,
    mlp_gain,
    w_gate,
    w_up,
    w_down,
):
    _, tok_count, width = inputs.shape
    count = lax.axis_size("ctx")
    tensors = lax.axis_size("tensor")
    rank = lax.axis_index("ctx")
    half = lax.axis_index("tensor")
    own_rows = tok_count // tensors
    rows = own_rows * count
    head_rows = w_out.shape[0]
    score_scale = 1.0 / math.sqrt(HEAD_DIM)

    q_cols = w_query.shape[1] // count
    k_cols = w_key.shape[1] // count
    local_kv = k_cols // HEAD_DIM
    group = q_cols // k_cols
    in_width = q_cols + 2 * k_cols
    in_shard = jnp.concatenate(
        [
            w_query.reshape(-1, count, q_cols),
            w_key.reshape(-1, count, k_cols),
            w_value.reshape(-1, count, k_cols),
        ],
        axis=2,
    ).reshape(w_query.shape[0], count * in_width)
    in_weight = slices_of(in_shard)
    out_weight = lax.all_gather(w_out.T, ("tensor", "dp", "ctx"), axis=0, tiled=True).reshape(
        tensors, width, head_rows
    )
    gate_weight = slices_of(w_gate)
    up_weight = slices_of(w_up)
    down_weight = slices_of(w_down.T)

    piece = attn_gain.shape[0]
    small = q_gain.shape[0]
    own_gains = jnp.concatenate([attn_gain, mlp_gain, q_gain, k_gain]).astype(F32)
    own_marks = jnp.concatenate([segment_ids[0], positions[0]])
    gains, marks = spread_small(to_tile(own_gains), to_tile(own_marks))
    gains = gains.reshape(gains.shape[0], -1)
    attn_scale = gains[:, :piece].reshape(-1)
    mlp_scale = gains[:, piece : 2 * piece].reshape(-1)
    query_scale = gains[:, 2 * piece : 2 * piece + small].reshape(-1)
    key_scale = gains[:, 2 * piece + small : 2 * (piece + small)].reshape(-1)
    marks = marks.reshape(count, -1)[:, : 2 * tok_count].reshape(count, 2, tensors, own_rows)
    behind = (rank - jnp.arange(count)) % count
    marks = marks[behind]
    starts = behind * tok_count
    offsets = starts[:, None] + jnp.arange(own_rows)[None, :]

    def marks_of(which):
        segs = lax.dynamic_index_in_dim(marks[:, 0], which, 1, keepdims=False).reshape(rows)
        return segs, (offsets + which * own_rows).reshape(rows)

    own_segs, own_index = marks_of(half)
    twin_segs, twin_index = marks_of(1 - half)
    own_positions = lax.dynamic_index_in_dim(marks[:, 1], half, 1, keepdims=False).reshape(rows)
    key_segs = jnp.concatenate([own_segs, twin_segs])
    key_index = jnp.concatenate([own_index, twin_index])
    allowed = (key_index[None, :] <= own_index[:, None]) & (key_segs[None, :] == own_segs[:, None])

    stream = lax.dynamic_slice_in_dim(inputs[0], half * own_rows, own_rows, 0).astype(F32)
    grad_own = lax.dynamic_slice_in_dim(out_grad[0], half * own_rows, own_rows, 0)
    normed_attn, attn_norm_pullback = jax.vjp(rms_norm, stream, attn_scale)
    normed_low = gather_behind(normed_attn.astype(BF16)).reshape(rows, width)
    raw = dot32(normed_low, in_weight, "mk,tkc->mtc")
    query_raw = raw[..., :q_cols].reshape(rows, tensors * local_kv * group, HEAD_DIM)
    key_raw = raw[..., q_cols : q_cols + k_cols].reshape(rows, tensors * local_kv, HEAD_DIM)
    kv_heads = tensors * local_kv
    value_low = raw[..., q_cols + k_cols :].astype(BF16).reshape(rows, kv_heads, HEAD_DIM)
    cosine_table, sine_table = rope_tables(own_positions, HEAD_DIM)
    cosine_table = cosine_table[:, None, :]
    sine_table = sine_table[:, None, :]

    def norm_rope(raw_heads, gain_vector):
        return head_norm(raw_heads, gain_vector, cosine_table, sine_table)

    query_rot, query_pullback = jax.vjp(norm_rope, query_raw, query_scale)
    key_rot, key_pullback = jax.vjp(norm_rope, key_raw, key_scale)
    query_low = query_rot.astype(BF16).reshape(rows, kv_heads, group, HEAD_DIM)
    key_low = key_rot.astype(BF16)
    kv_own = jnp.stack([key_low, value_low])
    kv_all = jnp.concatenate([kv_own, shift(kv_own, "tensor", 1)], axis=1)
    keys, values = kv_all[0], kv_all[1]

    scores = dot32(query_low, keys, "mkgd,nkd->kgmn") * score_scale
    masked = jnp.where(allowed, scores, masked_value)
    best = jnp.max(masked, axis=-1, keepdims=True)
    weights = jnp.where(allowed, jnp.exp(masked - best), 0.0)
    total = jnp.sum(weights, axis=-1, keepdims=True)
    prob = weights / total
    prob_low = prob.astype(BF16)
    attended = dot32(prob_low, values, "kgmn,nkd->mkgd")
    attended_heads = attended.astype(BF16).reshape(count, own_rows, tensors, q_cols)
    attended_own = swap_behind(attended_heads)
    attended_own = attended_own.transpose(1, 2, 0, 3).reshape(own_rows, tensors, head_rows)
    middle = stream + dot32(attended_own, out_weight, "mtr,tkr->mk")
    normed_mid, mlp_norm_pullback = jax.vjp(rms_norm, middle, mlp_scale)
    mid_low = gather_behind(normed_mid.astype(BF16)).reshape(rows, width)
    grad_low = gather_behind(grad_own).reshape(rows, width)

    gate = dot32(mid_low, gate_weight, "mk,tkc->tmc")
    upward = dot32(mid_low, up_weight, "mk,tkc->tmc")
    hidden, silu_pullback = jax.vjp(silu_product, gate, upward)
    hidden_low = hidden.astype(BF16)
    hidden_grad = dot32(grad_low, down_weight, "mk,tkc->tmc")
    gate_grad, upward_grad = silu_pullback(hidden_grad)
    gate_grad_low = gate_grad.astype(BF16)
    upward_grad_low = upward_grad.astype(BF16)
    mid_grad_part = dot32(gate_grad_low, gate_weight, "tmc,tkc->mk") + dot32(
        upward_grad_low, up_weight, "tmc,tkc->mk"
    )
    mid_grad = scatter_sum(mid_grad_part.astype(BF16).reshape(count, own_rows, width))
    down_part = dot32(hidden_low, down_weight, "tmc,tkc->mk")
    down_sum = scatter_sum(down_part.astype(BF16).reshape(count, own_rows, width))
    output = with_twin((middle + down_sum).astype(BF16))[None]
    down_weight_grad = shards_of(dot32(grad_low, hidden_low, "mk,tmc->tkc")).T
    gate_weight_grad = shards_of(dot32(mid_low, gate_grad_low, "mk,tmc->tkc"))
    up_weight_grad = shards_of(dot32(mid_low, upward_grad_low, "mk,tmc->tkc"))

    middle_norm_grad, mlp_gain_grad = mlp_norm_pullback(mid_grad)
    middle_grad = grad_own.astype(F32) + middle_norm_grad
    branch_grad = middle_grad.astype(BF16)
    branch_all = gather_behind(branch_grad).reshape(rows, width)
    attended_low = attended_heads.reshape(rows, tensors, q_cols)
    out_weight_grad = shards_of(dot32(branch_all, attended_low, "mk,mtr->tkr")).T
    attended_grad = dot32(branch_grad, out_weight, "mk,tkr->mtr").astype(BF16)
    attended_grad = attended_grad.reshape(own_rows, tensors, count, q_cols).transpose(2, 0, 1, 3)
    attended_grad = swap_to_behind(attended_grad).reshape(rows, kv_heads, group, HEAD_DIM)
    prob_grad = dot32(attended_grad, values, "mkgd,nkd->kgmn")
    delta = jnp.sum(prob * prob_grad, axis=-1, keepdims=True)
    score_grad = (prob * (prob_grad - delta)).astype(BF16)
    query_grad = dot32(score_grad, keys, "kgmn,nkd->mkgd") * score_scale
    key_grad_all = dot32(score_grad, query_low, "kgmn,mkgd->nkd")
    value_grad_all = dot32(prob_low, attended_grad, "kgmn,mkgd->nkd")
    kv_grad_all = jnp.stack([key_grad_all, value_grad_all])
    kv_grad = kv_grad_all[:, :rows] + shift(
        kv_grad_all[:, rows:].astype(BF16), "tensor", 1
    ).astype(F32)
    query_raw_grad, query_gain_grad = query_pullback(query_grad.reshape(query_raw.shape))
    key_raw_grad, key_gain_grad = key_pullback(kv_grad[0] * score_scale)
    raw_grad_low = jnp.concatenate(
        [
            query_raw_grad.astype(BF16).reshape(rows, tensors, q_cols),
            key_raw_grad.astype(BF16).reshape(rows, tensors, k_cols),
            kv_grad[1].astype(BF16).reshape(rows, tensors, k_cols),
        ],
        axis=2,
    )
    normed_grad_part = dot32(raw_grad_low, in_weight, "mtc,tkc->mk")
    normed_grad = scatter_sum(normed_grad_part.astype(BF16).reshape(count, own_rows, width))
    in_weight_grad = shards_of(dot32(normed_low, raw_grad_low, "mk,mtc->tkc"))
    in_weight_grad = in_weight_grad.reshape(-1, count, in_width)
    query_weight_grad = in_weight_grad[..., :q_cols].reshape(w_query.shape)
    key_weight_grad = in_weight_grad[..., q_cols : q_cols + k_cols].reshape(w_key.shape)
    value_weight_grad = in_weight_grad[..., q_cols + k_cols :].reshape(w_value.shape)
    stream_norm_grad, attn_gain_grad = attn_norm_pullback(normed_grad)
    input_grad = with_twin((middle_grad + stream_norm_grad).astype(BF16))[None]

    gain_grads = jnp.concatenate(
        [
            attn_gain_grad.reshape(-1, piece),
            mlp_gain_grad.reshape(-1, piece),
            query_gain_grad.reshape(-1, small),
            key_gain_grad.reshape(-1, small),
        ],
        axis=1,
    )
    gain_grads = owner_sums(jax.vmap(to_tile)(gain_grads)).reshape(-1)
    return (
        output,
        input_grad,
        gain_grads[:piece],
        query_weight_grad,
        key_weight_grad,
        value_weight_grad,
        gain_grads[2 * piece : 2 * piece + small],
        gain_grads[2 * piece + small : 2 * (piece + small)],
        out_weight_grad,
        gain_grads[piece : 2 * piece],
        gate_weight_grad,
        up_weight_grad,
        down_weight_grad,
    )


def can_slice(mesh, inputs, w_key, w_gate):
    tensors, count = mesh.shape["tensor"], mesh.shape["ctx"]
    return (
        tensors == 2
        and inputs.shape[0] == mesh.shape["dp"]
        and (inputs.shape[1] // count) % (16 * tensors) == 0
        and w_key.shape[1] % (tensors * count * HEAD_DIM) == 0
        and inputs.shape[1] // count * 2 <= math.prod(TILE)
        and w_gate.shape[1] % (tensors * count * 128) == 0
    )


def from_behind(value, axis, steps):
    return shift(value, axis, steps)


def on_device(
    inputs,
    segment_ids,
    positions,
    out_grad,
    attn_gain,
    w_query,
    w_key,
    w_value,
    q_gain,
    k_gain,
    w_out,
    mlp_gain,
    w_gate,
    w_up,
    w_down,
):
    seq_count, tok_count, width = inputs.shape
    row_count = seq_count * tok_count
    cycle_size = lax.axis_size("ctx")
    cycle_rank = lax.axis_index("ctx")
    gathered_attn = (
        lax.all_gather(w_query, ("dp", "ctx"), axis=0, tiled=True),
        lax.all_gather(w_key, ("dp", "ctx"), axis=0, tiled=True),
        lax.all_gather(w_value, ("dp", "ctx"), axis=0, tiled=True),
        lax.all_gather(w_out, ("dp", "ctx"), axis=1, tiled=True),
        lax.all_gather(attn_gain, ("dp", "ctx"), axis=0, tiled=True),
        lax.all_gather(q_gain, ("dp", "ctx"), axis=0, tiled=True),
        lax.all_gather(k_gain, ("dp", "ctx"), axis=0, tiled=True),
    )
    query_weight, key_weight, value_weight, out_weight, attn_scale, query_scale, key_scale = (
        gathered_attn
    )
    gathered_mlp = (
        lax.all_gather(w_gate, ("dp", "ctx"), axis=0, tiled=True),
        lax.all_gather(w_up, ("dp", "ctx"), axis=0, tiled=True),
        lax.all_gather(w_down, ("dp", "ctx"), axis=1, tiled=True),
        lax.all_gather(mlp_gain, ("dp", "ctx"), axis=0, tiled=True),
    )
    gate_weight, up_weight, down_weight, mlp_scale = gathered_mlp
    segments_all = lax.all_gather(segment_ids, "ctx", axis=1, tiled=True)
    local_heads = query_weight.shape[1] // HEAD_DIM
    local_kv = key_weight.shape[1] // HEAD_DIM
    group_size = local_heads // local_kv
    kv_width = local_kv * HEAD_DIM
    score_scale = 1.0 / math.sqrt(HEAD_DIM)
    stream = inputs.astype(jnp.float32).reshape(row_count, width)
    normed_attn, attn_norm_pullback = jax.vjp(rms_norm, stream, attn_scale.astype(jnp.float32))
    normed_low = normed_attn.astype(jnp.bfloat16)
    query_raw = jnp.dot(normed_low, query_weight, preferred_element_type=jnp.float32).reshape(
        seq_count, tok_count, local_heads, HEAD_DIM
    )
    key_raw = jnp.dot(normed_low, key_weight, preferred_element_type=jnp.float32).reshape(
        seq_count, tok_count, local_kv, HEAD_DIM
    )
    value_low = (
        jnp.dot(normed_low, value_weight, preferred_element_type=jnp.float32)
        .astype(jnp.bfloat16)
        .reshape(seq_count, tok_count, kv_width)
    )
    cosine_table, sine_table = rope_tables(positions, HEAD_DIM)
    cosine_table = cosine_table[:, :, None, :]
    sine_table = sine_table[:, :, None, :]

    def norm_rope(raw_heads, gain_vector):
        return head_norm(raw_heads, gain_vector, cosine_table, sine_table)

    query_rot, query_pullback = jax.vjp(norm_rope, query_raw, query_scale.astype(jnp.float32))
    key_rot, key_pullback = jax.vjp(norm_rope, key_raw, key_scale.astype(jnp.float32))
    query_low = query_rot.astype(jnp.bfloat16).reshape(
        seq_count, tok_count, local_kv, group_size, HEAD_DIM
    )
    key_low = key_rot.astype(jnp.bfloat16).reshape(seq_count, tok_count, kv_width)
    query_index = cycle_rank * tok_count + jnp.arange(tok_count, dtype=jnp.int32)

    def block_scores(key_block, first_row):
        key_count = key_block.shape[1]
        key_heads = key_block.reshape(seq_count, key_count, local_kv, HEAD_DIM)
        raw_scores = (
            jnp.einsum(
                "stkgd,snkd->skgtn", query_low, key_heads, preferred_element_type=jnp.float32
            )
            * score_scale
        )
        key_index = first_row + jnp.arange(key_count, dtype=jnp.int32)
        key_segments = lax.dynamic_slice_in_dim(segments_all, first_row, key_count, 1)
        allowed = (key_index[None, None, :] <= query_index[None, :, None]) & (
            key_segments[:, None, :] == segment_ids[:, :, None]
        )
        return (raw_scores, allowed[:, None, None, :, :])

    stat_shape = (seq_count, local_kv, group_size, tok_count)
    pieces = (
        lax.all_gather(key_low, "ctx", axis=1, tiled=True),
        lax.all_gather(value_low, "ctx", axis=1, tiled=True),
    )
    row_best = jnp.full(stat_shape, masked_value, jnp.float32)
    raw_scores, allowed = block_scores(pieces[0], jnp.int32(0))
    masked = jnp.where(allowed, raw_scores, masked_value)
    new_best = jnp.maximum(row_best, jnp.max(masked, axis=-1))
    weights = jnp.where(allowed, jnp.exp(masked - new_best[..., None]), 0.0)
    value_heads = pieces[1].reshape(seq_count, pieces[1].shape[1], local_kv, HEAD_DIM)
    added = jnp.einsum(
        "skgtn,snkd->skgtd",
        weights.astype(jnp.bfloat16),
        value_heads,
        preferred_element_type=jnp.float32,
    )
    row_total = jnp.sum(weights, axis=-1)
    log_total = new_best + jnp.log(row_total)
    attended = added / row_total[..., None]
    attended_low = (
        jnp.transpose(attended, (0, 3, 1, 2, 4))
        .reshape(row_count, local_heads * HEAD_DIM)
        .astype(jnp.bfloat16)
    )
    attn_part = jnp.dot(attended_low, out_weight, preferred_element_type=jnp.float32)
    middle = stream + lax.psum(attn_part.astype(jnp.bfloat16), "tensor").astype(jnp.float32)
    normed_mid, mlp_norm_pullback = jax.vjp(rms_norm, middle, mlp_scale.astype(jnp.float32))
    mid_low = normed_mid.astype(jnp.bfloat16)
    gate = jnp.dot(mid_low, gate_weight, preferred_element_type=jnp.float32)
    upward = jnp.dot(mid_low, up_weight, preferred_element_type=jnp.float32)
    hidden, silu_pullback = jax.vjp(silu_product, gate, upward)
    hidden_low = hidden.astype(jnp.bfloat16)
    down_part = jnp.dot(hidden_low, down_weight, preferred_element_type=jnp.float32)
    down_sum = lax.psum(down_part.astype(jnp.bfloat16), "tensor").astype(jnp.float32)
    output = (middle + down_sum).astype(jnp.bfloat16).reshape(seq_count, tok_count, width)
    grad_low = out_grad.reshape(row_count, width)
    down_weight_grad = jnp.dot(hidden_low.T, grad_low, preferred_element_type=jnp.float32)
    hidden_grad = jnp.dot(grad_low, down_weight.T, preferred_element_type=jnp.float32)
    gate_grad, upward_grad = silu_pullback(hidden_grad)
    gate_grad_low = gate_grad.astype(jnp.bfloat16)
    upward_grad_low = upward_grad.astype(jnp.bfloat16)
    gate_weight_grad = jnp.dot(mid_low.T, gate_grad_low, preferred_element_type=jnp.float32)
    up_weight_grad = jnp.dot(mid_low.T, upward_grad_low, preferred_element_type=jnp.float32)
    mid_grad_part = jnp.dot(
        gate_grad_low, gate_weight.T, preferred_element_type=jnp.float32
    ) + jnp.dot(upward_grad_low, up_weight.T, preferred_element_type=jnp.float32)
    mid_grad = lax.psum(mid_grad_part.astype(jnp.bfloat16), "tensor").astype(jnp.float32)
    middle_norm_grad, mlp_gain_grad = mlp_norm_pullback(mid_grad)
    middle_grad = grad_low.astype(jnp.float32) + middle_norm_grad
    mlp_grads = (
        lax.psum_scatter(gate_weight_grad, ("dp", "ctx"), scatter_dimension=0, tiled=True),
        lax.psum_scatter(up_weight_grad, ("dp", "ctx"), scatter_dimension=0, tiled=True),
        lax.psum_scatter(down_weight_grad, ("dp", "ctx"), scatter_dimension=1, tiled=True),
        lax.psum_scatter(mlp_gain_grad, ("dp", "ctx"), scatter_dimension=0, tiled=True),
    )
    branch_grad = middle_grad.astype(jnp.bfloat16)
    out_weight_grad = jnp.dot(attended_low.T, branch_grad, preferred_element_type=jnp.float32)
    attended_grad = jnp.dot(branch_grad, out_weight.T, preferred_element_type=jnp.float32).astype(
        jnp.bfloat16
    )
    attended_grad_heads = jnp.transpose(
        attended_grad.reshape(seq_count, tok_count, local_kv, group_size, HEAD_DIM), (0, 2, 3, 1, 4)
    )
    row_delta = jnp.sum(attended_grad_heads.astype(jnp.float32) * attended, axis=-1)

    def key_block_grads(key_block, value_block, first_row):
        raw_scores, allowed = block_scores(key_block, first_row)
        probability = jnp.where(allowed, jnp.exp(raw_scores - log_total[..., None]), 0.0)
        key_count = key_block.shape[1]
        value_heads = value_block.reshape(seq_count, key_count, local_kv, HEAD_DIM)
        key_heads = key_block.reshape(seq_count, key_count, local_kv, HEAD_DIM)
        prob_grad = jnp.einsum(
            "skgtd,snkd->skgtn",
            attended_grad_heads,
            value_heads,
            preferred_element_type=jnp.float32,
        )
        score_grad = (probability * (prob_grad - row_delta[..., None])).astype(jnp.bfloat16)
        query_add = jnp.einsum(
            "skgtn,snkd->skgtd", score_grad, key_heads, preferred_element_type=jnp.float32
        )
        key_add = jnp.einsum(
            "skgtn,stkgd->snkd", score_grad, query_low, preferred_element_type=jnp.float32
        ).reshape(seq_count, key_count, kv_width)
        value_add = jnp.einsum(
            "skgtn,skgtd->snkd",
            probability.astype(jnp.bfloat16),
            attended_grad_heads,
            preferred_element_type=jnp.float32,
        ).reshape(seq_count, key_count, kv_width)
        return (query_add, key_add, value_add)

    query_zero = jnp.zeros(stat_shape + (HEAD_DIM,), jnp.float32)
    kv_zero = jnp.zeros((seq_count, tok_count, kv_width), jnp.float32)

    def cycle_turn(turn_index, state):
        key_block, value_block, key_grad_acc, value_grad_acc, query_grad_acc = state
        owner_rank = (cycle_rank + turn_index) % cycle_size
        query_add, key_add, value_add = key_block_grads(
            key_block, value_block, owner_rank * tok_count
        )
        moved_blocks = from_behind((key_block, value_block), "ctx", -1)
        moved_grads = (
            from_behind((key_grad_acc + key_add).astype(jnp.bfloat16), "ctx", -1).astype(
                jnp.float32
            ),
            from_behind((value_grad_acc + value_add).astype(jnp.bfloat16), "ctx", -1).astype(
                jnp.float32
            ),
        )
        return (
            moved_blocks[0],
            moved_blocks[1],
            moved_grads[0],
            moved_grads[1],
            query_grad_acc + query_add,
        )

    final_state = lax.fori_loop(
        0, cycle_size, cycle_turn, (key_low, value_low, kv_zero, kv_zero, query_zero)
    )
    key_grad_sum = final_state[2]
    value_grad_sum = final_state[3]
    query_grad_sum = final_state[4]
    query_grad = (
        jnp.transpose(query_grad_sum, (0, 3, 1, 2, 4)).reshape(
            seq_count, tok_count, local_heads, HEAD_DIM
        )
        * score_scale
    )
    query_raw_grad, query_gain_grad = query_pullback(query_grad)
    key_raw_grad, key_gain_grad = key_pullback(
        (key_grad_sum * score_scale).reshape(seq_count, tok_count, local_kv, HEAD_DIM)
    )
    query_grad_low = query_raw_grad.reshape(row_count, local_heads * HEAD_DIM).astype(jnp.bfloat16)
    key_grad_low = key_raw_grad.reshape(row_count, kv_width).astype(jnp.bfloat16)
    value_grad_low = value_grad_sum.reshape(row_count, kv_width).astype(jnp.bfloat16)
    query_weight_grad = jnp.dot(normed_low.T, query_grad_low, preferred_element_type=jnp.float32)
    key_weight_grad = jnp.dot(normed_low.T, key_grad_low, preferred_element_type=jnp.float32)
    value_weight_grad = jnp.dot(normed_low.T, value_grad_low, preferred_element_type=jnp.float32)
    normed_grad_part = (
        jnp.dot(query_grad_low, query_weight.T, preferred_element_type=jnp.float32)
        + jnp.dot(key_grad_low, key_weight.T, preferred_element_type=jnp.float32)
        + jnp.dot(value_grad_low, value_weight.T, preferred_element_type=jnp.float32)
    )
    normed_grad, query_gain_total, key_gain_total = (
        lax.psum(normed_grad_part.astype(jnp.bfloat16), "tensor").astype(jnp.float32),
        lax.psum(query_gain_grad.astype(jnp.bfloat16), "tensor").astype(jnp.float32),
        lax.psum(key_gain_grad.astype(jnp.bfloat16), "tensor").astype(jnp.float32),
    )
    stream_norm_grad, attn_gain_grad = attn_norm_pullback(normed_grad)
    input_grad = (
        (middle_grad + stream_norm_grad).astype(jnp.bfloat16).reshape(seq_count, tok_count, width)
    )
    attn_grads = (
        lax.psum_scatter(query_weight_grad, ("dp", "ctx"), scatter_dimension=0, tiled=True),
        lax.psum_scatter(key_weight_grad, ("dp", "ctx"), scatter_dimension=0, tiled=True),
        lax.psum_scatter(value_weight_grad, ("dp", "ctx"), scatter_dimension=0, tiled=True),
        lax.psum_scatter(out_weight_grad, ("dp", "ctx"), scatter_dimension=1, tiled=True),
        lax.psum_scatter(attn_gain_grad, ("dp", "ctx"), scatter_dimension=0, tiled=True),
        lax.psum_scatter(query_gain_total, ("dp", "ctx"), scatter_dimension=0, tiled=True),
        lax.psum_scatter(key_gain_total, ("dp", "ctx"), scatter_dimension=0, tiled=True),
    )
    return (
        output,
        input_grad,
        attn_grads[4],
        attn_grads[0],
        attn_grads[1],
        attn_grads[2],
        attn_grads[5],
        attn_grads[6],
        attn_grads[3],
        mlp_grads[3],
        mlp_grads[0],
        mlp_grads[1],
        mlp_grads[2],
    )


def solution(mesh):
    in_specs = (
        P("dp", "ctx", None),
        P("dp", "ctx"),
        P("dp", "ctx"),
        P("dp", "ctx", None),
        P(("dp", "ctx")),
        P(("dp", "ctx"), "tensor"),
        P(("dp", "ctx"), "tensor"),
        P(("dp", "ctx"), "tensor"),
        P(("dp", "ctx")),
        P(("dp", "ctx")),
        P("tensor", ("dp", "ctx")),
        P(("dp", "ctx")),
        P(("dp", "ctx"), "tensor"),
        P(("dp", "ctx"), "tensor"),
        P("tensor", ("dp", "ctx")),
    )
    out_specs = (
        P("dp", "ctx", None),
        P("dp", "ctx", None),
        P(("dp", "ctx")),
        P(("dp", "ctx"), "tensor"),
        P(("dp", "ctx"), "tensor"),
        P(("dp", "ctx"), "tensor"),
        P(("dp", "ctx")),
        P(("dp", "ctx")),
        P("tensor", ("dp", "ctx")),
        P(("dp", "ctx")),
        P(("dp", "ctx"), "tensor"),
        P(("dp", "ctx"), "tensor"),
        P("tensor", ("dp", "ctx")),
    )

    def step(*args):
        body = on_device_sliced if can_slice(mesh, args[0], args[6], args[12]) else on_device
        return jax.shard_map(
            body, mesh=mesh, in_specs=in_specs, out_specs=out_specs, check_vma=False
        )(*args)

    return step
```

```python
import math

import jax
import jax.numpy as jnp
from jax import lax
from jax.experimental import pallas as pl
from jax.experimental.pallas import tpu as pltpu
from jax.sharding import PartitionSpec as P

HEAD_DIM = 128
BF16 = jnp.bfloat16
F32 = jnp.float32
MESH = pl.DeviceIdType.MESH
TILE = (8, 128)

epsilon = 1e-06
rope_base = 1000000.0
masked_value = -1e30


def from_behind(value, axis, steps):
    count = lax.axis_size(axis)
    pairs = [(source, (source + steps) % count) for source in range(count)]
    return lax.ppermute(value, axis, pairs)


def rope_tables(positions, head_size):
    half_dim = head_size // 2
    frequency = rope_base ** (-(jnp.arange(half_dim, dtype=jnp.float32) * 2.0) / head_size)
    angles = positions.astype(jnp.float32)[..., None] * frequency
    return (jnp.cos(angles), jnp.sin(angles))


def rotate(values, cosine_table, sine_table):
    half_dim = values.shape[-1] // 2
    first_half = values[..., :half_dim]
    second_half = values[..., half_dim:]
    return jnp.concatenate(
        [
            first_half * cosine_table - second_half * sine_table,
            second_half * cosine_table + first_half * sine_table,
        ],
        axis=-1,
    )


def head_norm(raw_heads, gain_vector, cosine_table, sine_table):
    scaled = (
        raw_heads
        * lax.rsqrt(jnp.mean(raw_heads * raw_heads, axis=-1, keepdims=True) + epsilon)
        * gain_vector
    )
    return rotate(scaled, cosine_table, sine_table)


def rms_norm(stream, gain_vector):
    return (
        stream
        * lax.rsqrt(jnp.mean(stream * stream, axis=-1, keepdims=True) + epsilon)
        * gain_vector
    )


def silu_product(gate, upward):
    return jax.nn.silu(gate) * upward


def dot32(left, right, spec):
    return jnp.einsum(spec, left, right, preferred_element_type=F32)


def shift(value, axis, steps):
    count = lax.axis_size(axis)
    pairs = [(source, (source + steps) % count) for source in range(count)]
    return lax.ppermute(value, axis, pairs)


def take_ring(blocks, first):
    return lax.dynamic_slice_in_dim(jnp.concatenate([blocks, blocks]), first, blocks.shape[0], 0)


def block_ahead(blocks, steps):
    count = lax.axis_size("ctx")
    place = (lax.axis_index("ctx") + steps) % count
    return lax.dynamic_index_in_dim(blocks, place, 0, keepdims=False)


def gather_ctx(block):
    count = lax.axis_size("ctx")
    rank = lax.axis_index("ctx")
    got = jnp.stack([block] + [shift(block, "ctx", -d) for d in range(1, count)])
    return take_ring(got, (count - rank) % count)


def scatter_sum(blocks):
    total = block_ahead(blocks, 0).astype(F32)
    for d in range(1, blocks.shape[0]):
        total = total + shift(block_ahead(blocks, d), "ctx", d).astype(F32)
    return total


def swap_by_target(blocks):
    count = lax.axis_size("ctx")
    rank = lax.axis_index("ctx")
    got = [shift(block_ahead(blocks, d), "ctx", d) for d in range(1, count)]
    got = jnp.stack([block_ahead(blocks, 0)] + got[::-1])
    return take_ring(got, (count - rank) % count)


def greet(peers):
    barrier = pltpu.get_barrier_semaphore()
    for peer in peers:
        pl.semaphore_signal(barrier, inc=1, device_id=peer, device_id_type=MESH)
    pl.semaphore_wait(barrier, len(peers))


def remote(source, target, send_sem, recv_sem, peer):
    copy = pltpu.make_async_remote_copy(
        src_ref=source,
        dst_ref=target,
        send_sem=send_sem,
        recv_sem=recv_sem,
        device_id=peer,
        device_id_type=MESH,
    )
    copy.start()
    return copy


def to_tile(values):
    return jnp.pad(values, (0, math.prod(TILE) - values.shape[0])).reshape(TILE)


def place():
    pair, rank, half = lax.axis_index("dp"), lax.axis_index("ctx"), lax.axis_index("tensor")
    core = lax.rem(pair, 2)
    return {
        "pair": pair,
        "rank": rank,
        "half": half,
        "sibling": pair + 1 - 2 * core,
        "across": lax.rem(pair + 2, 4),
        "twin": 1 - half,
    }


class Relay:
    KINDS = 9

    def __init__(self, here, source, view, rows, send_sem, recv_sem):
        self.here, self.source, self.view, self.rows = here, source, view, rows
        self.send_sem, self.recv_sem = send_sem, recv_sem
        self.copies = {}

    def go(self, kind, source, target, peer):
        self.copies[kind] = remote(
            source, target, self.send_sem.at[kind], self.recv_sem.at[kind], peer
        )

    def first(self):
        p = self.here
        target = self.view(p["half"], p["pair"], 0, self.rows)
        self.go(1, self.source, target, {"dp": p["across"]})
        self.go(2, self.source, target, {"tensor": p["twin"]})
        self.go(0, self.source, target, {"dp": p["sibling"]})

    def second(self):
        p, part = self.here, self.rows // 2
        self.copies[1].wait_recv()
        low = self.view(p["half"], p["across"], 0, part)
        self.go(4, low, low, {"tensor": p["twin"]})
        whole = self.view(p["half"], p["across"], 0, self.rows)
        self.go(3, whole, whole, {"dp": p["sibling"]})
        self.copies[2].wait_recv()
        high = self.view(p["twin"], p["pair"], part, part)
        self.go(6, high, high, {"dp": p["across"]})
        whole = self.view(p["twin"], p["pair"], 0, self.rows)
        self.go(5, whole, whole, {"dp": p["sibling"]})

    def third(self):
        p, part = self.here, self.rows // 2
        self.copies[4].wait_recv()
        low = self.view(p["twin"], p["across"], 0, part)
        self.go(7, low, low, {"dp": p["sibling"]})
        self.copies[6].wait_recv()
        high = self.view(p["twin"], p["across"], part, part)
        self.go(8, high, high, {"dp": p["sibling"]})

    def last(self):
        for kind in (0, 3, 5, 7, 8):
            self.copies[kind].wait_recv()
        for copy in self.copies.values():
            copy.wait_send()


class Chain:
    def __init__(self, rank, count, source, result, send_sem, recv_sem):
        self.rank, self.count, self.source, self.result = rank, count, source, result
        self.send_sem, self.recv_sem = send_sem, recv_sem

    def copy(self, way, step):
        step_to = self.rank + (1 if way == 0 else -1)
        owner = self.rank - step if way == 0 else self.rank + step
        owner = jnp.clip(owner, 0, self.count - 1)
        return pltpu.make_async_remote_copy(
            src_ref=self.source if step == 0 else self.result.at[owner],
            dst_ref=self.result.at[owner],
            send_sem=self.send_sem.at[way, step],
            recv_sem=self.recv_sem.at[way, step],
            device_id={"ctx": jnp.clip(step_to, 0, self.count - 1)},
            device_id_type=MESH,
        )

    def sends(self, way, step):
        if way == 0:
            return (self.rank >= step) & (self.rank < self.count - 1)
        return (self.rank + step < self.count) & (self.rank > 0)

    def receives(self, way, step):
        return self.rank > step if way == 0 else self.rank + step < self.count - 1

    def start(self, step):
        for way in (0, 1):
            if step > 0:

                @pl.when(self.receives(way, step - 1))
                def _():
                    self.copy(way, step - 1).wait_recv()

            @pl.when(self.sends(way, step))
            def _():
                self.copy(way, step).start()

    def finish(self):
        last = self.count - 2
        for way in (0, 1):

            @pl.when(self.receives(way, last))
            def _():
                self.copy(way, last).wait_recv()

            for step in range(self.count - 1):

                @pl.when(self.sends(way, step))
                def _():
                    self.copy(way, step).wait_send()


SEMS = pltpu.SemaphoreType.DMA
ANYWHERE = pl.BlockSpec(memory_space=pl.ANY)
ON_CHIP = pl.BlockSpec(memory_space=pltpu.VMEM)


def enter(gains, marks, block, w_query, w_key, w_value):
    count, pairs = lax.axis_size("ctx"), lax.axis_size("dp")
    owners = count * pairs
    depth = w_query.shape[0]
    widths = [w.shape[1] // count for w in (w_query, w_key, w_value)]
    width = sum(widths)
    spots = [sum(widths[:i]) for i in range(3)]
    rows = block.shape[0]

    def kernel(
        gain_ref, mark_ref, block_ref, wq_ref, wk_ref, wv_ref,
        gains_ref, marks_ref, rows_ref, weight_ref,
        held, gain_send, gain_recv, mark_send, mark_recv,
        swap_send, swap_recv, chain_send, chain_recv, relay_send, relay_recv, local_sem,
    ):
        here = place()
        rank, pair, half = here["rank"], here["pair"], here["half"]
        me = pair * count + rank
        far = [lax.rem(me + k, owners) for k in range(1, owners)]
        far = [{"dp": lax.div(t, count), "ctx": lax.rem(t, count)} for t in far]
        near = [{"ctx": lax.rem(rank + k, count)} for k in range(1, count)]
        greet(far + [{"tensor": here["twin"]}])

        def view(owner_rank):
            def at(t, p, start, size):
                first = pl.multiple_of((p * count + owner_rank) * depth + start, 64)
                return weight_ref.at[pl.ds(first, size), pl.ds(pl.multiple_of(t * width, 128), width)]

            return at

        def columns(ref, i, target):
            return ref.at[:, pl.ds(pl.multiple_of(target * widths[i], 128), widths[i])]

        sources = (wq_ref, wk_ref, wv_ref)
        takes = [
            pltpu.make_async_copy(
                columns(ref, i, rank), held.at[:, pl.ds(spots[i], widths[i])], local_sem.at[i]
            )
            for i, ref in enumerate(sources)
        ]
        for take in takes:
            take.start()
        small = [
            remote(mark_ref, marks_ref.at[rank], mark_send.at[k], mark_recv.at[k], peer)
            for k, peer in enumerate(near)
        ]
        small += [
            remote(gain_ref, gains_ref.at[me], gain_send.at[k], gain_recv.at[k], peer)
            for k, peer in enumerate(far)
        ]
        own_rows = pl.ds(pl.multiple_of(me * depth, depth), depth)
        swaps = []
        for k, peer in enumerate(near):
            swaps.append([])
            for i, ref in enumerate(sources):
                spot = pl.ds(pl.multiple_of(half * width + spots[i], 128), widths[i])
                swaps[k].append(
                    remote(
                        columns(ref, i, peer["ctx"]),
                        weight_ref.at[own_rows, spot],
                        swap_send.at[k, i],
                        swap_recv.at[k, i],
                        peer,
                    )
                )
        chain = Chain(rank, count, block_ref, rows_ref, chain_send, chain_recv)
        chain.start(0)
        gains_ref[me] = gain_ref[...]
        marks_ref[rank] = mark_ref[...]
        for take in takes:
            take.wait()
        keep = pltpu.make_async_copy(held, view(rank)(half, pair, 0, depth), local_sem.at[3])
        keep.start()
        relays = [Relay(here, held, view(rank), depth, relay_send.at[0], relay_recv.at[0])]
        relays[0].first()
        for k in range(1, count):
            owner = lax.rem(rank - k + count, count)
            for swap in swaps[k - 1]:
                swap.wait_recv()
            at = view(owner)
            relays.append(
                Relay(here, at(half, pair, 0, depth), at, depth, relay_send.at[k], relay_recv.at[k])
            )
            relays[k].first()
            relays[k - 1].second()
            if k > 1:
                relays[k - 2].third()
            if k < count - 1:
                chain.start(k)
        relays[-1].second()
        relays[-2].third()
        relays[-1].third()
        for relay in relays:
            relay.last()
        keep.wait()
        chain.finish()
        for swap in swaps:
            for copy in swap:
                copy.wait_send()
        for copy in small:
            copy.wait()

    return pl.pallas_call(
        kernel,
        out_shape=(
            jax.ShapeDtypeStruct((owners, *TILE), F32),
            jax.ShapeDtypeStruct((count, *TILE), jnp.int32),
            jax.ShapeDtypeStruct((count, rows, block.shape[1]), block.dtype),
            jax.ShapeDtypeStruct((owners * depth, 2 * width), w_query.dtype),
        ),
        in_specs=[ON_CHIP] * 2 + [ANYWHERE] * 4,
        out_specs=(ON_CHIP, ON_CHIP, ANYWHERE, ANYWHERE),
        scratch_shapes=[
            pltpu.VMEM((depth, width), w_query.dtype),
            SEMS((owners - 1,)),
            SEMS((owners - 1,)),
            SEMS((count - 1,)),
            SEMS((count - 1,)),
            SEMS((count - 1, 3)),
            SEMS((count - 1, 3)),
            SEMS((2, count - 1)),
            SEMS((2, count - 1)),
            SEMS((count, Relay.KINDS)),
            SEMS((count, Relay.KINDS)),
            SEMS((4,)),
        ],
        compiler_params=pltpu.CompilerParams(collective_id=0, has_side_effects=True),
        name="enter",
    )(gains, marks, block, w_query, w_key, w_value)


def spread_mlp(first, second, pieces):
    count, pairs = lax.axis_size("ctx"), lax.axis_size("dp")
    kinds, depth, width = pieces[0].shape
    rows, features = first.shape

    def kernel(first_ref, second_ref, *rest):
        piece_refs, rest = rest[:count], rest[count:]
        firsts_ref, seconds_ref = rest[:2]
        weight_refs, rest = rest[2 : 2 + kinds], rest[2 + kinds :]
        held, chain_send, chain_recv, relay_send, relay_recv, take_sem, keep_sem = rest
        here = place()
        rank, pair, half = here["rank"], here["pair"], here["half"]
        greet(
            [{"ctx": lax.rem(rank + k, count)} for k in range(1, count)]
            + [{"dp": here["sibling"]}, {"dp": here["across"]}, {"tensor": here["twin"]}]
        )
        takes = []
        for i in range(kinds):
            for d, ref in enumerate(piece_refs):
                owner = lax.rem(rank - d + count, count)
                take = pltpu.make_async_copy(
                    ref.at[i],
                    held.at[i, pl.ds(pl.multiple_of(owner * depth, depth), depth)],
                    take_sem.at[i, d],
                )
                take.start()
                takes.append(take)
        chains = [
            Chain(rank, count, first_ref, firsts_ref, chain_send.at[0], chain_recv.at[0]),
            Chain(rank, count, second_ref, seconds_ref, chain_send.at[1], chain_recv.at[1]),
        ]
        chains[0].start(0)
        block = count * depth

        def view(i):
            def at(t, p, start, size):
                first = pl.multiple_of(p * block + start, 64)
                return weight_refs[i].at[
                    pl.ds(first, size), pl.ds(pl.multiple_of(t * width, 128), width)
                ]

            return at

        relays, keeps = [], []
        for i in range(kinds):
            for take in takes[i * count : (i + 1) * count]:
                take.wait()
            keeps.append(
                pltpu.make_async_copy(held.at[i], view(i)(half, pair, 0, block), keep_sem.at[i])
            )
            keeps[i].start()
            relays.append(
                Relay(here, held.at[i], view(i), block, relay_send.at[i], relay_recv.at[i])
            )
            relays[i].first()
        chains[0].start(1)
        relays[0].second()
        chains[0].start(2)
        chains[1].start(0)
        relays[0].third()
        relays[1].second()
        chains[1].start(1)
        relays[1].third()
        relays[2].second()
        chains[1].start(2)
        relays[2].third()
        for relay in relays:
            relay.last()
        for keep in keeps:
            keep.wait()
        for chain in chains:
            chain.finish()

    return pl.pallas_call(
        kernel,
        out_shape=(
            jax.ShapeDtypeStruct((count, rows, features), first.dtype),
            jax.ShapeDtypeStruct((count, rows, features), second.dtype),
        )
        + (jax.ShapeDtypeStruct((pairs * count * depth, 2 * width), pieces[0].dtype),) * kinds,
        in_specs=[ANYWHERE] * (2 + count),
        out_specs=(ANYWHERE,) * (2 + kinds),
        scratch_shapes=[
            pltpu.VMEM((kinds, count * depth, width), pieces[0].dtype),
            SEMS((2, 2, count - 1)),
            SEMS((2, 2, count - 1)),
            SEMS((kinds, Relay.KINDS)),
            SEMS((kinds, Relay.KINDS)),
            SEMS((kinds, count)),
            SEMS((kinds,)),
        ],
        compiler_params=pltpu.CompilerParams(
            collective_id=2, has_side_effects=True, vmem_limit_bytes=16 * 1024 * 1024
        ),
        name="spread_mlp",
    )(first, second, *pieces)


def swap_ctx(blocks, collective_id):
    count = lax.axis_size("ctx")

    def kernel(blocks_ref, got_ref, held, send_sem, recv_sem, local_sem):
        rank = lax.axis_index("ctx")
        peers = [lax.rem(rank + k, count) for k in range(1, count)]
        greet([{"ctx": peer} for peer in peers])
        copies = [
            remote(
                blocks_ref.at[peer], got_ref.at[rank], send_sem.at[k], recv_sem.at[k], {"ctx": peer}
            )
            for k, peer in enumerate(peers)
        ]
        take = pltpu.make_async_copy(blocks_ref.at[rank], held, local_sem.at[0])
        take.start()
        take.wait()
        keep = pltpu.make_async_copy(held, got_ref.at[rank], local_sem.at[1])
        keep.start()
        keep.wait()
        for copy in copies:
            copy.wait()

    return pl.pallas_call(
        kernel,
        out_shape=jax.ShapeDtypeStruct(blocks.shape, blocks.dtype),
        in_specs=[ANYWHERE],
        out_specs=ANYWHERE,
        scratch_shapes=[
            pltpu.VMEM(blocks.shape[1:], blocks.dtype),
            SEMS((count - 1,)),
            SEMS((count - 1,)),
            SEMS((2,)),
        ],
        compiler_params=pltpu.CompilerParams(collective_id=collective_id, has_side_effects=True),
        name=f"swap_ctx_{collective_id}",
    )(blocks)


def owner_sums(tiles):
    count, pairs, tensors = lax.axis_size("ctx"), lax.axis_size("dp"), lax.axis_size("tensor")
    total = count * pairs * tensors

    def kernel(tiles_ref, sum_ref, got, send_sem, recv_sem):
        owner = lax.axis_index("dp") * count + lax.axis_index("ctx")
        me = owner * tensors + lax.axis_index("tensor")
        targets = [lax.rem(me + k, total) for k in range(1, total)]
        peers = [
            {
                "dp": lax.div(t, count * tensors),
                "ctx": lax.rem(lax.div(t, tensors), count),
                "tensor": lax.rem(t, tensors),
            }
            for t in targets
        ]
        greet(peers)
        copies = [
            remote(
                tiles_ref.at[lax.div(t, tensors)], got.at[me], send_sem.at[k], recv_sem.at[k], peer
            )
            for k, (t, peer) in enumerate(zip(targets, peers))
        ]
        got[me] = tiles_ref[owner]
        for copy in copies:
            copy.wait()
        value = got[0]
        for source in range(1, total):
            value = value + got[source]
        sum_ref[...] = value

    return pl.pallas_call(
        kernel,
        out_shape=jax.ShapeDtypeStruct(TILE, F32),
        in_specs=[pl.BlockSpec(memory_space=pltpu.VMEM)],
        out_specs=pl.BlockSpec(memory_space=pltpu.VMEM),
        scratch_shapes=[
            pltpu.VMEM((total, *TILE), F32),
            pltpu.SemaphoreType.DMA((total - 1,)),
            pltpu.SemaphoreType.DMA((total - 1,)),
        ],
        compiler_params=pltpu.CompilerParams(collective_id=1, has_side_effects=True),
        name="owner_sums",
    )(tiles)


def weight_partial(rows_side, columns_side):
    tensors = lax.axis_size("tensor")
    cols = columns_side.shape[1] // tensors
    return jnp.stack(
        [
            jnp.dot(
                rows_side.T, columns_side[:, t * cols : (t + 1) * cols], preferred_element_type=F32
            ).astype(BF16)
            for t in range(tensors)
        ]
    )


def shards_of(partial):
    count = lax.axis_size("ctx")
    width = partial.shape[2]
    flat = partial.astype(BF16).reshape(-1, width)
    mine = lax.psum_scatter(flat, ("tensor", "dp"), scatter_dimension=0, tiled=True)
    got = swap_by_target(mine.reshape(count, mine.shape[0] // count, width))
    return got.transpose(1, 0, 2).reshape(got.shape[1], count * width).astype(F32)


def with_twin(own):
    other = shift(own, "tensor", 1)
    first = lax.axis_index("tensor") == 0
    return jnp.concatenate([jnp.where(first, own, other), jnp.where(first, other, own)])


def on_device_sliced(
    inputs,
    segment_ids,
    positions,
    out_grad,
    attn_gain,
    w_query,
    w_key,
    w_value,
    q_gain,
    k_gain,
    w_out,
    mlp_gain,
    w_gate,
    w_up,
    w_down,
):
    _, tok_count, width = inputs.shape
    count = lax.axis_size("ctx")
    tensors = lax.axis_size("tensor")
    rank = lax.axis_index("ctx")
    half = lax.axis_index("tensor")
    own_rows = tok_count // tensors
    rows = own_rows * count
    head_rows = w_out.shape[0]
    score_scale = 1.0 / math.sqrt(HEAD_DIM)

    q_cols = w_query.shape[1] // count
    k_cols = w_key.shape[1] // count
    local_kv = k_cols // HEAD_DIM
    kv_heads = tensors * local_kv
    group = q_cols // k_cols
    in_width = q_cols + 2 * k_cols
    piece = attn_gain.shape[0]
    small = q_gain.shape[0]

    input_own = lax.dynamic_slice_in_dim(inputs[0], half * own_rows, own_rows, 0)
    grad_own = lax.dynamic_slice_in_dim(out_grad[0], half * own_rows, own_rows, 0)
    own_gains = jnp.concatenate([attn_gain, mlp_gain, q_gain, k_gain]).astype(F32)
    own_marks = jnp.concatenate([segment_ids[0], positions[0]])
    gains, marks, input_all, in_weight = enter(
        to_tile(own_gains), to_tile(own_marks), input_own, w_query, w_key, w_value
    )
    out_weight = lax.all_gather(w_out.T, ("tensor", "dp", "ctx"), axis=0, tiled=True).reshape(
        tensors, width, head_rows
    )
    gains = gains.reshape(gains.shape[0], -1)
    attn_scale = gains[:, :piece].reshape(-1)
    mlp_scale = gains[:, piece : 2 * piece].reshape(-1)
    query_scale = gains[:, 2 * piece : 2 * piece + small].reshape(-1)
    key_scale = gains[:, 2 * piece + small : 2 * (piece + small)].reshape(-1)

    mlp_shards = jnp.stack([w_gate, w_up, w_down.T]).reshape(3, -1, count, w_gate.shape[1] // count)
    mlp_shards, in_weight = lax.optimization_barrier((mlp_shards, in_weight))
    mlp_pieces = [
        shift(
            lax.dynamic_index_in_dim(mlp_shards, (rank + d) % count, 2, keepdims=False), "ctx", d
        )
        if d
        else lax.dynamic_index_in_dim(mlp_shards, rank, 2, keepdims=False)
        for d in range(count)
    ]

    marks = marks.reshape(count, -1)[:, : 2 * tok_count].reshape(count, 2, tensors, own_rows)
    offsets = jnp.arange(count)[:, None] * tok_count + jnp.arange(own_rows)[None, :]

    def marks_of(which):
        segs = lax.dynamic_index_in_dim(marks[:, 0], which, 1, keepdims=False).reshape(rows)
        return segs, (offsets + which * own_rows).reshape(rows)

    own_segs, own_index = marks_of(half)
    twin_segs, twin_index = marks_of(1 - half)
    own_positions = lax.dynamic_index_in_dim(marks[:, 1], half, 1, keepdims=False).reshape(rows)

    def allowed_of(key_segs, key_index):
        return (key_index[None, :] <= own_index[:, None]) & (key_segs[None, :] == own_segs[:, None])

    allowed = (allowed_of(own_segs, own_index), allowed_of(twin_segs, twin_index))

    stream = input_own.astype(F32)
    input_all = lax.dynamic_update_index_in_dim(input_all, input_own, rank, 0)
    normed_low = rms_norm(input_all.reshape(rows, width).astype(F32), attn_scale).astype(BF16)
    _, attn_norm_pullback = jax.vjp(rms_norm, stream, attn_scale)
    raw = jnp.dot(normed_low, in_weight, preferred_element_type=F32)
    raw = raw.reshape(rows, tensors, in_width)
    query_raw = raw[..., :q_cols].reshape(rows, kv_heads * group, HEAD_DIM)
    key_raw = raw[..., q_cols : q_cols + k_cols].reshape(rows, kv_heads, HEAD_DIM)
    value_low = raw[..., q_cols + k_cols :].astype(BF16).reshape(rows, kv_heads, HEAD_DIM)
    cosine_table, sine_table = rope_tables(own_positions, HEAD_DIM)
    cosine_table = cosine_table[:, None, :]
    sine_table = sine_table[:, None, :]

    def norm_rope(raw_heads, gain_vector):
        return head_norm(raw_heads, gain_vector, cosine_table, sine_table)

    key_rot, key_pullback = jax.vjp(norm_rope, key_raw, key_scale)
    key_low = key_rot.astype(BF16)
    kv_own = jnp.stack([key_low, value_low])
    kv_twin = shift(kv_own, "tensor", 1)
    query_rot, query_pullback = jax.vjp(norm_rope, query_raw, query_scale)
    query_low = query_rot.astype(BF16).reshape(rows, kv_heads, group, HEAD_DIM)
    keys = (kv_own[0], kv_twin[0])
    values = (kv_own[1], kv_twin[1])

    scores = [
        jnp.where(ok, dot32(query_low, key, "mkgd,nkd->kgmn") * score_scale, masked_value)
        for ok, key in zip(allowed, keys)
    ]
    best = jnp.maximum(*[jnp.max(s, axis=-1, keepdims=True) for s in scores])
    weights = [jnp.where(ok, jnp.exp(s - best), 0.0) for ok, s in zip(allowed, scores)]
    total = sum(jnp.sum(w, axis=-1, keepdims=True) for w in weights)
    prob = [w / total for w in weights]
    prob_low = [p.astype(BF16) for p in prob]
    attended = sum(dot32(p, v, "kgmn,nkd->mkgd") for p, v in zip(prob_low, values))
    attended_low = attended.astype(BF16).reshape(rows, tensors * q_cols)
    attended_own = swap_ctx(attended_low.reshape(count, own_rows, tensors * q_cols), 3)
    attended_own = attended_own.reshape(count, own_rows, tensors, q_cols)
    attended_own = attended_own.transpose(1, 2, 0, 3).reshape(own_rows, tensors, head_rows)
    middle = stream + dot32(attended_own, out_weight, "mtr,tkr->mk")
    normed_mid, mlp_norm_pullback = jax.vjp(rms_norm, middle, mlp_scale)
    mid_own = normed_mid.astype(BF16)
    mid_low, grad_low, gate_weight, up_weight, down_weight = spread_mlp(
        mid_own, grad_own, mlp_pieces
    )
    mid_low = lax.dynamic_update_index_in_dim(mid_low, mid_own, rank, 0).reshape(rows, width)
    grad_low = lax.dynamic_update_index_in_dim(grad_low, grad_own, rank, 0).reshape(rows, width)

    gate = jnp.dot(mid_low, gate_weight, preferred_element_type=F32)
    upward = jnp.dot(mid_low, up_weight, preferred_element_type=F32)
    hidden, silu_pullback = jax.vjp(silu_product, gate, upward)
    hidden_low = hidden.astype(BF16)
    hidden_grad = jnp.dot(grad_low, down_weight, preferred_element_type=F32)
    gate_grad, upward_grad = silu_pullback(hidden_grad)
    gate_grad_low = gate_grad.astype(BF16)
    upward_grad_low = upward_grad.astype(BF16)
    mid_grad_part = jnp.dot(gate_grad_low, gate_weight.T, preferred_element_type=F32) + jnp.dot(
        upward_grad_low, up_weight.T, preferred_element_type=F32
    )
    mid_grad = scatter_sum(mid_grad_part.astype(BF16).reshape(count, own_rows, width))
    mlp_grads = [
        weight_partial(mid_low, gate_grad_low),
        weight_partial(mid_low, upward_grad_low),
        weight_partial(grad_low, hidden_low),
    ]
    down_part = jnp.dot(hidden_low, down_weight.T, preferred_element_type=F32).astype(BF16)
    mid_grad, down_part, mlp_grads = lax.optimization_barrier((mid_grad, down_part, mlp_grads))
    gate_weight_grad, up_weight_grad, down_weight_grad = [shards_of(g) for g in mlp_grads]
    down_weight_grad = down_weight_grad.T

    middle_norm_grad, mlp_gain_grad = mlp_norm_pullback(mid_grad)
    middle_grad = grad_own.astype(F32) + middle_norm_grad
    branch_grad = middle_grad.astype(BF16)
    attended_grad = dot32(branch_grad, out_weight, "mk,tkr->mtr").astype(BF16)
    attended_grad = attended_grad.reshape(own_rows, tensors, count, q_cols).transpose(2, 0, 1, 3)
    attended_grad = swap_ctx(attended_grad.reshape(count, own_rows, tensors * q_cols), 4)
    branch_grad, down_part, attended_grad = lax.optimization_barrier(
        (branch_grad, down_part, attended_grad)
    )
    down_sum = scatter_sum(down_part.reshape(count, own_rows, width))
    output = with_twin((middle + down_sum).astype(BF16))[None]
    branch_all = gather_ctx(branch_grad).reshape(rows, width)
    out_weight_grad = shards_of(weight_partial(branch_all, attended_low)).T
    attended_grad = attended_grad.reshape(rows, kv_heads, group, HEAD_DIM)
    prob_grad = [dot32(attended_grad, v, "mkgd,nkd->kgmn") for v in values]
    delta = sum(jnp.sum(p * g, axis=-1, keepdims=True) for p, g in zip(prob, prob_grad))
    score_grad = [(p * (g - delta)).astype(BF16) for p, g in zip(prob, prob_grad)]

    def key_side(i):
        return jnp.stack(
            [
                dot32(score_grad[i], query_low, "kgmn,mkgd->nkd"),
                dot32(prob_low[i], attended_grad, "kgmn,mkgd->nkd"),
            ]
        )

    kv_back = shift(key_side(1).astype(BF16), "tensor", 1)
    kv_grad = key_side(0) + kv_back.astype(F32)
    query_grad = sum(dot32(g, k, "kgmn,nkd->mkgd") for g, k in zip(score_grad, keys)) * score_scale
    query_raw_grad, query_gain_grad = query_pullback(query_grad.reshape(query_raw.shape))
    key_raw_grad, key_gain_grad = key_pullback(kv_grad[0] * score_scale)
    raw_grad_low = jnp.concatenate(
        [
            query_raw_grad.astype(BF16).reshape(rows, tensors, q_cols),
            key_raw_grad.astype(BF16).reshape(rows, tensors, k_cols),
            kv_grad[1].astype(BF16).reshape(rows, tensors, k_cols),
        ],
        axis=2,
    ).reshape(rows, tensors * in_width)
    normed_grad_part = jnp.dot(raw_grad_low, in_weight.T, preferred_element_type=F32)
    normed_grad = scatter_sum(normed_grad_part.astype(BF16).reshape(count, own_rows, width))
    in_weight_grad = shards_of(weight_partial(normed_low, raw_grad_low))
    in_weight_grad = in_weight_grad.reshape(-1, count, in_width)
    query_weight_grad = in_weight_grad[..., :q_cols].reshape(w_query.shape)
    key_weight_grad = in_weight_grad[..., q_cols : q_cols + k_cols].reshape(w_key.shape)
    value_weight_grad = in_weight_grad[..., q_cols + k_cols :].reshape(w_value.shape)
    stream_norm_grad, attn_gain_grad = attn_norm_pullback(normed_grad)
    input_grad = with_twin((middle_grad + stream_norm_grad).astype(BF16))[None]

    gain_grads = jnp.concatenate(
        [
            attn_gain_grad.reshape(-1, piece),
            mlp_gain_grad.reshape(-1, piece),
            query_gain_grad.reshape(-1, small),
            key_gain_grad.reshape(-1, small),
        ],
        axis=1,
    )
    gain_grads = owner_sums(jax.vmap(to_tile)(gain_grads)).reshape(-1)
    return (
        output,
        input_grad,
        gain_grads[:piece],
        query_weight_grad,
        key_weight_grad,
        value_weight_grad,
        gain_grads[2 * piece : 2 * piece + small],
        gain_grads[2 * piece + small : 2 * (piece + small)],
        out_weight_grad,
        gain_grads[piece : 2 * piece],
        gate_weight_grad,
        up_weight_grad,
        down_weight_grad,
    )


def can_slice(mesh, inputs, w_key, w_gate):
    tensors, count = mesh.shape["tensor"], mesh.shape["ctx"]
    return (
        (mesh.shape["dp"], count, tensors) == (4, 4, 2)
        and inputs.shape[0] == mesh.shape["dp"]
        and (inputs.shape[1] // count) % (16 * tensors) == 0
        and w_key.shape[1] % (tensors * count * HEAD_DIM) == 0
        and inputs.shape[1] // count * 2 <= math.prod(TILE)
        and w_gate.shape[1] % (tensors * count * 128) == 0
    )


def from_behind(value, axis, steps):
    count = lax.axis_size(axis)
    pairs = [(source, (source + steps) % count) for source in range(count)]
    return lax.ppermute(value, axis, pairs)


def rope_tables(positions, head_size):
    half_dim = head_size // 2
    frequency = rope_base ** (-(jnp.arange(half_dim, dtype=jnp.float32) * 2.0) / head_size)
    angles = positions.astype(jnp.float32)[..., None] * frequency
    return (jnp.cos(angles), jnp.sin(angles))


def rotate(values, cosine_table, sine_table):
    half_dim = values.shape[-1] // 2
    first_half = values[..., :half_dim]
    second_half = values[..., half_dim:]
    return jnp.concatenate(
        [
            first_half * cosine_table - second_half * sine_table,
            second_half * cosine_table + first_half * sine_table,
        ],
        axis=-1,
    )


def head_norm(raw_heads, gain_vector, cosine_table, sine_table):
    scaled = (
        raw_heads
        * lax.rsqrt(jnp.mean(raw_heads * raw_heads, axis=-1, keepdims=True) + epsilon)
        * gain_vector
    )
    return rotate(scaled, cosine_table, sine_table)


def rms_norm(stream, gain_vector):
    return (
        stream
        * lax.rsqrt(jnp.mean(stream * stream, axis=-1, keepdims=True) + epsilon)
        * gain_vector
    )


def silu_product(gate, upward):
    return jax.nn.silu(gate) * upward


def dot32(left, right, spec):
    return jnp.einsum(spec, left, right, preferred_element_type=F32)


def shift(value, axis, steps):
    count = lax.axis_size(axis)
    pairs = [(source, (source + steps) % count) for source in range(count)]
    return lax.ppermute(value, axis, pairs)


def take_ring(blocks, first):
    return lax.dynamic_slice_in_dim(jnp.concatenate([blocks, blocks]), first, blocks.shape[0], 0)


def block_ahead(blocks, steps):
    count = lax.axis_size("ctx")
    place = (lax.axis_index("ctx") + steps) % count
    return lax.dynamic_index_in_dim(blocks, place, 0, keepdims=False)


def gather_ctx(block):
    count = lax.axis_size("ctx")
    rank = lax.axis_index("ctx")
    got = jnp.stack([block] + [shift(block, "ctx", -d) for d in range(1, count)])
    return take_ring(got, (count - rank) % count)


def scatter_sum(blocks):
    total = block_ahead(blocks, 0).astype(F32)
    for d in range(1, blocks.shape[0]):
        total = total + shift(block_ahead(blocks, d), "ctx", d).astype(F32)
    return total


def swap_by_target(blocks):
    count = lax.axis_size("ctx")
    rank = lax.axis_index("ctx")
    got = [shift(block_ahead(blocks, d), "ctx", d) for d in range(1, count)]
    got = jnp.stack([block_ahead(blocks, 0)] + got[::-1])
    return take_ring(got, (count - rank) % count)


def greet(peers):
    barrier = pltpu.get_barrier_semaphore()
    for peer in peers:
        pl.semaphore_signal(barrier, inc=1, device_id=peer, device_id_type=MESH)
    pl.semaphore_wait(barrier, len(peers))


def remote(source, target, send_sem, recv_sem, peer):
    copy = pltpu.make_async_remote_copy(
        src_ref=source,
        dst_ref=target,
        send_sem=send_sem,
        recv_sem=recv_sem,
        device_id=peer,
        device_id_type=MESH,
    )
    copy.start()
    return copy


def to_tile(values):
    return jnp.pad(values, (0, math.prod(TILE) - values.shape[0])).reshape(TILE)


def place():
    pair, rank, half = lax.axis_index("dp"), lax.axis_index("ctx"), lax.axis_index("tensor")
    core = lax.rem(pair, 2)
    return {
        "pair": pair,
        "rank": rank,
        "half": half,
        "sibling": pair + 1 - 2 * core,
        "across": lax.rem(pair + 2, 4),
        "twin": 1 - half,
    }


class Relay:
    KINDS = 9

    def __init__(self, here, source, view, rows, send_sem, recv_sem):
        self.here, self.source, self.view, self.rows = here, source, view, rows
        self.send_sem, self.recv_sem = send_sem, recv_sem
        self.copies = {}

    def go(self, kind, source, target, peer):
        self.copies[kind] = remote(
            source, target, self.send_sem.at[kind], self.recv_sem.at[kind], peer
        )

    def first(self):
        p = self.here
        target = self.view(p["half"], p["pair"], 0, self.rows)
        self.go(1, self.source, target, {"dp": p["across"]})
        self.go(2, self.source, target, {"tensor": p["twin"]})
        self.go(0, self.source, target, {"dp": p["sibling"]})

    def second(self):
        p, part = self.here, self.rows // 2
        self.copies[1].wait_recv()
        low = self.view(p["half"], p["across"], 0, part)
        self.go(4, low, low, {"tensor": p["twin"]})
        whole = self.view(p["half"], p["across"], 0, self.rows)
        self.go(3, whole, whole, {"dp": p["sibling"]})
        self.copies[2].wait_recv()
        high = self.view(p["twin"], p["pair"], part, part)
        self.go(6, high, high, {"dp": p["across"]})
        whole = self.view(p["twin"], p["pair"], 0, self.rows)
        self.go(5, whole, whole, {"dp": p["sibling"]})

    def third(self):
        p, part = self.here, self.rows // 2
        self.copies[4].wait_recv()
        low = self.view(p["twin"], p["across"], 0, part)
        self.go(7, low, low, {"dp": p["sibling"]})
        self.copies[6].wait_recv()
        high = self.view(p["twin"], p["across"], part, part)
        self.go(8, high, high, {"dp": p["sibling"]})

    def last(self):
        for kind in (0, 3, 5, 7, 8):
            self.copies[kind].wait_recv()
        for copy in self.copies.values():
            copy.wait_send()


class Chain:
    def __init__(self, rank, count, source, result, send_sem, recv_sem):
        self.rank, self.count, self.source, self.result = rank, count, source, result
        self.send_sem, self.recv_sem = send_sem, recv_sem

    def copy(self, way, step):
        step_to = self.rank + (1 if way == 0 else -1)
        owner = self.rank - step if way == 0 else self.rank + step
        owner = jnp.clip(owner, 0, self.count - 1)
        return pltpu.make_async_remote_copy(
            src_ref=self.source if step == 0 else self.result.at[owner],
            dst_ref=self.result.at[owner],
            send_sem=self.send_sem.at[way, step],
            recv_sem=self.recv_sem.at[way, step],
            device_id={"ctx": jnp.clip(step_to, 0, self.count - 1)},
            device_id_type=MESH,
        )

    def sends(self, way, step):
        if way == 0:
            return (self.rank >= step) & (self.rank < self.count - 1)
        return (self.rank + step < self.count) & (self.rank > 0)

    def receives(self, way, step):
        return self.rank > step if way == 0 else self.rank + step < self.count - 1

    def start(self, step):
        for way in (0, 1):
            if step > 0:

                @pl.when(self.receives(way, step - 1))
                def _():
                    self.copy(way, step - 1).wait_recv()

            @pl.when(self.sends(way, step))
            def _():
                self.copy(way, step).start()

    def finish(self):
        last = self.count - 2
        for way in (0, 1):

            @pl.when(self.receives(way, last))
            def _():
                self.copy(way, last).wait_recv()

            for step in range(self.count - 1):

                @pl.when(self.sends(way, step))
                def _():
                    self.copy(way, step).wait_send()


SEMS = pltpu.SemaphoreType.DMA
ANYWHERE = pl.BlockSpec(memory_space=pl.ANY)
ON_CHIP = pl.BlockSpec(memory_space=pltpu.VMEM)


def enter(gains, marks, block, w_query, w_key, w_value):
    count, pairs = lax.axis_size("ctx"), lax.axis_size("dp")
    owners = count * pairs
    depth = w_query.shape[0]
    widths = [w.shape[1] // count for w in (w_query, w_key, w_value)]
    width = sum(widths)
    spots = [sum(widths[:i]) for i in range(3)]
    rows = block.shape[0]

    def kernel(
        gain_ref, mark_ref, block_ref, wq_ref, wk_ref, wv_ref,
        gains_ref, marks_ref, rows_ref, weight_ref,
        held, gain_send, gain_recv, mark_send, mark_recv,
        swap_send, swap_recv, chain_send, chain_recv, relay_send, relay_recv, local_sem,
    ):
        here = place()
        rank, pair, half = here["rank"], here["pair"], here["half"]
        me = pair * count + rank
        far = [lax.rem(me + k, owners) for k in range(1, owners)]
        far = [{"dp": lax.div(t, count), "ctx": lax.rem(t, count)} for t in far]
        near = [{"ctx": lax.rem(rank + k, count)} for k in range(1, count)]
        greet(far + [{"tensor": here["twin"]}])

        def view(owner_rank):
            def at(t, p, start, size):
                first = pl.multiple_of((p * count + owner_rank) * depth + start, 64)
                return weight_ref.at[pl.ds(first, size), pl.ds(pl.multiple_of(t * width, 128), width)]

            return at

        def columns(ref, i, target):
            return ref.at[:, pl.ds(pl.multiple_of(target * widths[i], 128), widths[i])]

        sources = (wq_ref, wk_ref, wv_ref)
        takes = [
            pltpu.make_async_copy(
                columns(ref, i, rank), held.at[:, pl.ds(spots[i], widths[i])], local_sem.at[i]
            )
            for i, ref in enumerate(sources)
        ]
        for take in takes:
            take.start()
        small = [
            remote(mark_ref, marks_ref.at[rank], mark_send.at[k], mark_recv.at[k], peer)
            for k, peer in enumerate(near)
        ]
        small += [
            remote(gain_ref, gains_ref.at[me], gain_send.at[k], gain_recv.at[k], peer)
            for k, peer in enumerate(far)
        ]
        own_rows = pl.ds(pl.multiple_of(me * depth, depth), depth)
        swaps = []
        for k, peer in enumerate(near):
            swaps.append([])
            for i, ref in enumerate(sources):
                spot = pl.ds(pl.multiple_of(half * width + spots[i], 128), widths[i])
                swaps[k].append(
                    remote(
                        columns(ref, i, peer["ctx"]),
                        weight_ref.at[own_rows, spot],
                        swap_send.at[k, i],
                        swap_recv.at[k, i],
                        peer,
                    )
                )
        chain = Chain(rank, count, block_ref, rows_ref, chain_send, chain_recv)
        chain.start(0)
        gains_ref[me] = gain_ref[...]
        marks_ref[rank] = mark_ref[...]
        for take in takes:
            take.wait()
        keep = pltpu.make_async_copy(held, view(rank)(half, pair, 0, depth), local_sem.at[3])
        keep.start()
        relays = [Relay(here, held, view(rank), depth, relay_send.at[0], relay_recv.at[0])]
        relays[0].first()
        for k in range(1, count):
            owner = lax.rem(rank - k + count, count)
            for swap in swaps[k - 1]:
                swap.wait_recv()
            at = view(owner)
            relays.append(
                Relay(here, at(half, pair, 0, depth), at, depth, relay_send.at[k], relay_recv.at[k])
            )
            relays[k].first()
            relays[k - 1].second()
            if k > 1:
                relays[k - 2].third()
            if k < count - 1:
                chain.start(k)
        relays[-1].second()
        relays[-2].third()
        relays[-1].third()
        for relay in relays:
            relay.last()
        keep.wait()
        chain.finish()
        for swap in swaps:
            for copy in swap:
                copy.wait_send()
        for copy in small:
            copy.wait()

    return pl.pallas_call(
        kernel,
        out_shape=(
            jax.ShapeDtypeStruct((owners, *TILE), F32),
            jax.ShapeDtypeStruct((count, *TILE), jnp.int32),
            jax.ShapeDtypeStruct((count, rows, block.shape[1]), block.dtype),
            jax.ShapeDtypeStruct((owners * depth, 2 * width), w_query.dtype),
        ),
        in_specs=[ON_CHIP] * 2 + [ANYWHERE] * 4,
        out_specs=(ON_CHIP, ON_CHIP, ANYWHERE, ANYWHERE),
        scratch_shapes=[
            pltpu.VMEM((depth, width), w_query.dtype),
            SEMS((owners - 1,)),
            SEMS((owners - 1,)),
            SEMS((count - 1,)),
            SEMS((count - 1,)),
            SEMS((count - 1, 3)),
            SEMS((count - 1, 3)),
            SEMS((2, count - 1)),
            SEMS((2, count - 1)),
            SEMS((count, Relay.KINDS)),
            SEMS((count, Relay.KINDS)),
            SEMS((4,)),
        ],
        compiler_params=pltpu.CompilerParams(collective_id=0, has_side_effects=True),
        name="enter",
    )(gains, marks, block, w_query, w_key, w_value)


def spread_mlp(first, second, pieces):
    count, pairs = lax.axis_size("ctx"), lax.axis_size("dp")
    kinds, depth, width = pieces[0].shape
    rows, features = first.shape

    def kernel(first_ref, second_ref, *rest):
        piece_refs, rest = rest[:count], rest[count:]
        firsts_ref, seconds_ref = rest[:2]
        weight_refs, rest = rest[2 : 2 + kinds], rest[2 + kinds :]
        held, chain_send, chain_recv, relay_send, relay_recv, take_sem, keep_sem = rest
        here = place()
        rank, pair, half = here["rank"], here["pair"], here["half"]
        greet(
            [{"ctx": lax.rem(rank + k, count)} for k in range(1, count)]
            + [{"dp": here["sibling"]}, {"dp": here["across"]}, {"tensor": here["twin"]}]
        )
        takes = []
        for i in range(kinds):
            for d, ref in enumerate(piece_refs):
                owner = lax.rem(rank - d + count, count)
                take = pltpu.make_async_copy(
                    ref.at[i],
                    held.at[i, pl.ds(pl.multiple_of(owner * depth, depth), depth)],
                    take_sem.at[i, d],
                )
                take.start()
                takes.append(take)
        chains = [
            Chain(rank, count, first_ref, firsts_ref, chain_send.at[0], chain_recv.at[0]),
            Chain(rank, count, second_ref, seconds_ref, chain_send.at[1], chain_recv.at[1]),
        ]
        chains[0].start(0)
        block = count * depth

        def view(i):
            def at(t, p, start, size):
                first = pl.multiple_of(p * block + start, 64)
                return weight_refs[i].at[
                    pl.ds(first, size), pl.ds(pl.multiple_of(t * width, 128), width)
                ]

            return at

        relays, keeps = [], []
        for i in range(kinds):
            for take in takes[i * count : (i + 1) * count]:
                take.wait()
            keeps.append(
                pltpu.make_async_copy(held.at[i], view(i)(half, pair, 0, block), keep_sem.at[i])
            )
            keeps[i].start()
            relays.append(
                Relay(here, held.at[i], view(i), block, relay_send.at[i], relay_recv.at[i])
            )
            relays[i].first()
        chains[0].start(1)
        relays[0].second()
        chains[0].start(2)
        chains[1].start(0)
        relays[0].third()
        relays[1].second()
        chains[1].start(1)
        relays[1].third()
        relays[2].second()
        chains[1].start(2)
        relays[2].third()
        for relay in relays:
            relay.last()
        for keep in keeps:
            keep.wait()
        for chain in chains:
            chain.finish()

    return pl.pallas_call(
        kernel,
        out_shape=(
            jax.ShapeDtypeStruct((count, rows, features), first.dtype),
            jax.ShapeDtypeStruct((count, rows, features), second.dtype),
        )
        + (jax.ShapeDtypeStruct((pairs * count * depth, 2 * width), pieces[0].dtype),) * kinds,
        in_specs=[ANYWHERE] * (2 + count),
        out_specs=(ANYWHERE,) * (2 + kinds),
        scratch_shapes=[
            pltpu.VMEM((kinds, count * depth, width), pieces[0].dtype),
            SEMS((2, 2, count - 1)),
            SEMS((2, 2, count - 1)),
            SEMS((kinds, Relay.KINDS)),
            SEMS((kinds, Relay.KINDS)),
            SEMS((kinds, count)),
            SEMS((kinds,)),
        ],
        compiler_params=pltpu.CompilerParams(
            collective_id=2, has_side_effects=True, vmem_limit_bytes=16 * 1024 * 1024
        ),
        name="spread_mlp",
    )(first, second, *pieces)


def swap_ctx(blocks, collective_id):
    count = lax.axis_size("ctx")

    def kernel(blocks_ref, got_ref, held, send_sem, recv_sem, local_sem):
        rank = lax.axis_index("ctx")
        peers = [lax.rem(rank + k, count) for k in range(1, count)]
        greet([{"ctx": peer} for peer in peers])
        copies = [
            remote(
                blocks_ref.at[peer], got_ref.at[rank], send_sem.at[k], recv_sem.at[k], {"ctx": peer}
            )
            for k, peer in enumerate(peers)
        ]
        take = pltpu.make_async_copy(blocks_ref.at[rank], held, local_sem.at[0])
        take.start()
        take.wait()
        keep = pltpu.make_async_copy(held, got_ref.at[rank], local_sem.at[1])
        keep.start()
        keep.wait()
        for copy in copies:
            copy.wait()

    return pl.pallas_call(
        kernel,
        out_shape=jax.ShapeDtypeStruct(blocks.shape, blocks.dtype),
        in_specs=[ANYWHERE],
        out_specs=ANYWHERE,
        scratch_shapes=[
            pltpu.VMEM(blocks.shape[1:], blocks.dtype),
            SEMS((count - 1,)),
            SEMS((count - 1,)),
            SEMS((2,)),
        ],
        compiler_params=pltpu.CompilerParams(collective_id=collective_id, has_side_effects=True),
        name=f"swap_ctx_{collective_id}",
    )(blocks)


def owner_sums(tiles):
    count, pairs, tensors = lax.axis_size("ctx"), lax.axis_size("dp"), lax.axis_size("tensor")
    total = count * pairs * tensors

    def kernel(tiles_ref, sum_ref, got, send_sem, recv_sem):
        owner = lax.axis_index("dp") * count + lax.axis_index("ctx")
        me = owner * tensors + lax.axis_index("tensor")
        targets = [lax.rem(me + k, total) for k in range(1, total)]
        peers = [
            {
                "dp": lax.div(t, count * tensors),
                "ctx": lax.rem(lax.div(t, tensors), count),
                "tensor": lax.rem(t, tensors),
            }
            for t in targets
        ]
        greet(peers)
        copies = [
            remote(
                tiles_ref.at[lax.div(t, tensors)], got.at[me], send_sem.at[k], recv_sem.at[k], peer
            )
            for k, (t, peer) in enumerate(zip(targets, peers))
        ]
        got[me] = tiles_ref[owner]
        for copy in copies:
            copy.wait()
        value = got[0]
        for source in range(1, total):
            value = value + got[source]
        sum_ref[...] = value

    return pl.pallas_call(
        kernel,
        out_shape=jax.ShapeDtypeStruct(TILE, F32),
        in_specs=[pl.BlockSpec(memory_space=pltpu.VMEM)],
        out_specs=pl.BlockSpec(memory_space=pltpu.VMEM),
        scratch_shapes=[
            pltpu.VMEM((total, *TILE), F32),
            pltpu.SemaphoreType.DMA((total - 1,)),
            pltpu.SemaphoreType.DMA((total - 1,)),
        ],
        compiler_params=pltpu.CompilerParams(collective_id=1, has_side_effects=True),
        name="owner_sums",
    )(tiles)


def weight_partial(rows_side, columns_side):
    tensors = lax.axis_size("tensor")
    cols = columns_side.shape[1] // tensors
    return jnp.stack(
        [
            jnp.dot(
                rows_side.T, columns_side[:, t * cols : (t + 1) * cols], preferred_element_type=F32
            ).astype(BF16)
            for t in range(tensors)
        ]
    )


def shards_of(partial):
    count = lax.axis_size("ctx")
    width = partial.shape[2]
    flat = partial.astype(BF16).reshape(-1, width)
    mine = lax.psum_scatter(flat, ("tensor", "dp"), scatter_dimension=0, tiled=True)
    got = swap_by_target(mine.reshape(count, mine.shape[0] // count, width))
    return got.transpose(1, 0, 2).reshape(got.shape[1], count * width).astype(F32)


def with_twin(own):
    other = shift(own, "tensor", 1)
    first = lax.axis_index("tensor") == 0
    return jnp.concatenate([jnp.where(first, own, other), jnp.where(first, other, own)])


def on_device_sliced(
    inputs,
    segment_ids,
    positions,
    out_grad,
    attn_gain,
    w_query,
    w_key,
    w_value,
    q_gain,
    k_gain,
    w_out,
    mlp_gain,
    w_gate,
    w_up,
    w_down,
):
    _, tok_count, width = inputs.shape
    count = lax.axis_size("ctx")
    tensors = lax.axis_size("tensor")
    rank = lax.axis_index("ctx")
    half = lax.axis_index("tensor")
    own_rows = tok_count // tensors
    rows = own_rows * count
    head_rows = w_out.shape[0]
    score_scale = 1.0 / math.sqrt(HEAD_DIM)

    q_cols = w_query.shape[1] // count
    k_cols = w_key.shape[1] // count
    local_kv = k_cols // HEAD_DIM
    kv_heads = tensors * local_kv
    group = q_cols // k_cols
    in_width = q_cols + 2 * k_cols
    piece = attn_gain.shape[0]
    small = q_gain.shape[0]

    input_own = lax.dynamic_slice_in_dim(inputs[0], half * own_rows, own_rows, 0)
    grad_own = lax.dynamic_slice_in_dim(out_grad[0], half * own_rows, own_rows, 0)
    own_gains = jnp.concatenate([attn_gain, mlp_gain, q_gain, k_gain]).astype(F32)
    own_marks = jnp.concatenate([segment_ids[0], positions[0]])
    gains, marks, input_all, in_weight = enter(
        to_tile(own_gains), to_tile(own_marks), input_own, w_query, w_key, w_value
    )
    out_weight = lax.all_gather(w_out.T, ("tensor", "dp", "ctx"), axis=0, tiled=True).reshape(
        tensors, width, head_rows
    )
    gains = gains.reshape(gains.shape[0], -1)
    attn_scale = gains[:, :piece].reshape(-1)
    mlp_scale = gains[:, piece : 2 * piece].reshape(-1)
    query_scale = gains[:, 2 * piece : 2 * piece + small].reshape(-1)
    key_scale = gains[:, 2 * piece + small : 2 * (piece + small)].reshape(-1)

    mlp_shards = jnp.stack([w_gate, w_up, w_down.T]).reshape(3, -1, count, w_gate.shape[1] // count)
    mlp_shards, in_weight = lax.optimization_barrier((mlp_shards, in_weight))
    mlp_pieces = [
        shift(
            lax.dynamic_index_in_dim(mlp_shards, (rank + d) % count, 2, keepdims=False), "ctx", d
        )
        if d
        else lax.dynamic_index_in_dim(mlp_shards, rank, 2, keepdims=False)
        for d in range(count)
    ]

    marks = marks.reshape(count, -1)[:, : 2 * tok_count].reshape(count, 2, tensors, own_rows)
    offsets = jnp.arange(count)[:, None] * tok_count + jnp.arange(own_rows)[None, :]

    def marks_of(which):
        segs = lax.dynamic_index_in_dim(marks[:, 0], which, 1, keepdims=False).reshape(rows)
        return segs, (offsets + which * own_rows).reshape(rows)

    own_segs, own_index = marks_of(half)
    twin_segs, twin_index = marks_of(1 - half)
    own_positions = lax.dynamic_index_in_dim(marks[:, 1], half, 1, keepdims=False).reshape(rows)

    def allowed_of(key_segs, key_index):
        return (key_index[None, :] <= own_index[:, None]) & (key_segs[None, :] == own_segs[:, None])

    allowed = (allowed_of(own_segs, own_index), allowed_of(twin_segs, twin_index))

    stream = input_own.astype(F32)
    input_all = lax.dynamic_update_index_in_dim(input_all, input_own, rank, 0)
    normed_low = rms_norm(input_all.reshape(rows, width).astype(F32), attn_scale).astype(BF16)
    _, attn_norm_pullback = jax.vjp(rms_norm, stream, attn_scale)
    raw = jnp.dot(normed_low, in_weight, preferred_element_type=F32)
    raw = raw.reshape(rows, tensors, in_width)
    query_raw = raw[..., :q_cols].reshape(rows, kv_heads * group, HEAD_DIM)
    key_raw = raw[..., q_cols : q_cols + k_cols].reshape(rows, kv_heads, HEAD_DIM)
    value_low = raw[..., q_cols + k_cols :].astype(BF16).reshape(rows, kv_heads, HEAD_DIM)
    cosine_table, sine_table = rope_tables(own_positions, HEAD_DIM)
    cosine_table = cosine_table[:, None, :]
    sine_table = sine_table[:, None, :]

    def norm_rope(raw_heads, gain_vector):
        return head_norm(raw_heads, gain_vector, cosine_table, sine_table)

    key_rot, key_pullback = jax.vjp(norm_rope, key_raw, key_scale)
    key_low = key_rot.astype(BF16)
    kv_own = jnp.stack([key_low, value_low])
    kv_twin = shift(kv_own, "tensor", 1)
    query_rot, query_pullback = jax.vjp(norm_rope, query_raw, query_scale)
    query_low = query_rot.astype(BF16).reshape(rows, kv_heads, group, HEAD_DIM)
    keys = (kv_own[0], kv_twin[0])
    values = (kv_own[1], kv_twin[1])

    scores = [
        jnp.where(ok, dot32(query_low, key, "mkgd,nkd->kgmn") * score_scale, masked_value)
        for ok, key in zip(allowed, keys)
    ]
    best = jnp.maximum(*[jnp.max(s, axis=-1, keepdims=True) for s in scores])
    weights = [jnp.where(ok, jnp.exp(s - best), 0.0) for ok, s in zip(allowed, scores)]
    total = sum(jnp.sum(w, axis=-1, keepdims=True) for w in weights)
    prob = [w / total for w in weights]
    prob_low = [p.astype(BF16) for p in prob]
    attended = sum(dot32(p, v, "kgmn,nkd->mkgd") for p, v in zip(prob_low, values))
    attended_low = attended.astype(BF16).reshape(rows, tensors * q_cols)
    attended_own = swap_ctx(attended_low.reshape(count, own_rows, tensors * q_cols), 3)
    attended_own = attended_own.reshape(count, own_rows, tensors, q_cols)
    attended_own = attended_own.transpose(1, 2, 0, 3).reshape(own_rows, tensors, head_rows)
    middle = stream + dot32(attended_own, out_weight, "mtr,tkr->mk")
    normed_mid, mlp_norm_pullback = jax.vjp(rms_norm, middle, mlp_scale)
    mid_own = normed_mid.astype(BF16)
    mid_low, grad_low, gate_weight, up_weight, down_weight = spread_mlp(
        mid_own, grad_own, mlp_pieces
    )
    mid_low = lax.dynamic_update_index_in_dim(mid_low, mid_own, rank, 0).reshape(rows, width)
    grad_low = lax.dynamic_update_index_in_dim(grad_low, grad_own, rank, 0).reshape(rows, width)

    gate = jnp.dot(mid_low, gate_weight, preferred_element_type=F32)
    upward = jnp.dot(mid_low, up_weight, preferred_element_type=F32)
    hidden, silu_pullback = jax.vjp(silu_product, gate, upward)
    hidden_low = hidden.astype(BF16)
    hidden_grad = jnp.dot(grad_low, down_weight, preferred_element_type=F32)
    gate_grad, upward_grad = silu_pullback(hidden_grad)
    gate_grad_low = gate_grad.astype(BF16)
    upward_grad_low = upward_grad.astype(BF16)
    mid_grad_part = jnp.dot(gate_grad_low, gate_weight.T, preferred_element_type=F32) + jnp.dot(
        upward_grad_low, up_weight.T, preferred_element_type=F32
    )
    mid_grad = scatter_sum(mid_grad_part.astype(BF16).reshape(count, own_rows, width))
    mlp_grads = [
        weight_partial(mid_low, gate_grad_low),
        weight_partial(mid_low, upward_grad_low),
        weight_partial(grad_low, hidden_low),
    ]
    down_part = jnp.dot(hidden_low, down_weight.T, preferred_element_type=F32).astype(BF16)
    mid_grad, down_part, mlp_grads = lax.optimization_barrier((mid_grad, down_part, mlp_grads))
    gate_weight_grad, up_weight_grad, down_weight_grad = [shards_of(g) for g in mlp_grads]
    down_weight_grad = down_weight_grad.T

    middle_norm_grad, mlp_gain_grad = mlp_norm_pullback(mid_grad)
    middle_grad = grad_own.astype(F32) + middle_norm_grad
    branch_grad = middle_grad.astype(BF16)
    attended_grad = dot32(branch_grad, out_weight, "mk,tkr->mtr").astype(BF16)
    attended_grad = attended_grad.reshape(own_rows, tensors, count, q_cols).transpose(2, 0, 1, 3)
    attended_grad = swap_ctx(attended_grad.reshape(count, own_rows, tensors * q_cols), 4)
    branch_grad, down_part, attended_grad = lax.optimization_barrier(
        (branch_grad, down_part, attended_grad)
    )
    down_sum = scatter_sum(down_part.reshape(count, own_rows, width))
    output = with_twin((middle + down_sum).astype(BF16))[None]
    branch_all = gather_ctx(branch_grad).reshape(rows, width)
    out_weight_grad = shards_of(weight_partial(branch_all, attended_low)).T
    attended_grad = attended_grad.reshape(rows, kv_heads, group, HEAD_DIM)
    prob_grad = [dot32(attended_grad, v, "mkgd,nkd->kgmn") for v in values]
    delta = sum(jnp.sum(p * g, axis=-1, keepdims=True) for p, g in zip(prob, prob_grad))
    score_grad = [(p * (g - delta)).astype(BF16) for p, g in zip(prob, prob_grad)]

    def key_side(i):
        return jnp.stack(
            [
                dot32(score_grad[i], query_low, "kgmn,mkgd->nkd"),
                dot32(prob_low[i], attended_grad, "kgmn,mkgd->nkd"),
            ]
        )

    kv_back = shift(key_side(1).astype(BF16), "tensor", 1)
    kv_grad = key_side(0) + kv_back.astype(F32)
    query_grad = sum(dot32(g, k, "kgmn,nkd->mkgd") for g, k in zip(score_grad, keys)) * score_scale
    query_raw_grad, query_gain_grad = query_pullback(query_grad.reshape(query_raw.shape))
    key_raw_grad, key_gain_grad = key_pullback(kv_grad[0] * score_scale)
    raw_grad_low = jnp.concatenate(
        [
            query_raw_grad.astype(BF16).reshape(rows, tensors, q_cols),
            key_raw_grad.astype(BF16).reshape(rows, tensors, k_cols),
            kv_grad[1].astype(BF16).reshape(rows, tensors, k_cols),
        ],
        axis=2,
    ).reshape(rows, tensors * in_width)
    normed_grad_part = jnp.dot(raw_grad_low, in_weight.T, preferred_element_type=F32)
    normed_grad = scatter_sum(normed_grad_part.astype(BF16).reshape(count, own_rows, width))
    in_weight_grad = shards_of(weight_partial(normed_low, raw_grad_low))
    in_weight_grad = in_weight_grad.reshape(-1, count, in_width)
    query_weight_grad = in_weight_grad[..., :q_cols].reshape(w_query.shape)
    key_weight_grad = in_weight_grad[..., q_cols : q_cols + k_cols].reshape(w_key.shape)
    value_weight_grad = in_weight_grad[..., q_cols + k_cols :].reshape(w_value.shape)
    stream_norm_grad, attn_gain_grad = attn_norm_pullback(normed_grad)
    input_grad = with_twin((middle_grad + stream_norm_grad).astype(BF16))[None]

    gain_grads = jnp.concatenate(
        [
            attn_gain_grad.reshape(-1, piece),
            mlp_gain_grad.reshape(-1, piece),
            query_gain_grad.reshape(-1, small),
            key_gain_grad.reshape(-1, small),
        ],
        axis=1,
    )
    gain_grads = owner_sums(jax.vmap(to_tile)(gain_grads)).reshape(-1)
    return (
        output,
        input_grad,
        gain_grads[:piece],
        query_weight_grad,
        key_weight_grad,
        value_weight_grad,
        gain_grads[2 * piece : 2 * piece + small],
        gain_grads[2 * piece + small : 2 * (piece + small)],
        out_weight_grad,
        gain_grads[piece : 2 * piece],
        gate_weight_grad,
        up_weight_grad,
        down_weight_grad,
    )


def can_slice(mesh, inputs, w_key, w_gate):
    tensors, count = mesh.shape["tensor"], mesh.shape["ctx"]
    return (
        tensors == 2
        and inputs.shape[0] == mesh.shape["dp"]
        and (inputs.shape[1] // count) % (16 * tensors) == 0
        and w_key.shape[1] % (tensors * count * HEAD_DIM) == 0
        and inputs.shape[1] // count * 2 <= math.prod(TILE)
        and w_gate.shape[1] % (tensors * count * 128) == 0
    )


def from_behind(value, axis, steps):
    return shift(value, axis, steps)


def on_device(
    inputs,
    segment_ids,
    positions,
    out_grad,
    attn_gain,
    w_query,
    w_key,
    w_value,
    q_gain,
    k_gain,
    w_out,
    mlp_gain,
    w_gate,
    w_up,
    w_down,
):
    seq_count, tok_count, width = inputs.shape
    row_count = seq_count * tok_count
    cycle_size = lax.axis_size("ctx")
    cycle_rank = lax.axis_index("ctx")
    gathered_attn = (
        lax.all_gather(w_query, ("dp", "ctx"), axis=0, tiled=True),
        lax.all_gather(w_key, ("dp", "ctx"), axis=0, tiled=True),
        lax.all_gather(w_value, ("dp", "ctx"), axis=0, tiled=True),
        lax.all_gather(w_out, ("dp", "ctx"), axis=1, tiled=True),
        lax.all_gather(attn_gain, ("dp", "ctx"), axis=0, tiled=True),
        lax.all_gather(q_gain, ("dp", "ctx"), axis=0, tiled=True),
        lax.all_gather(k_gain, ("dp", "ctx"), axis=0, tiled=True),
    )
    query_weight, key_weight, value_weight, out_weight, attn_scale, query_scale, key_scale = (
        gathered_attn
    )
    gathered_mlp = (
        lax.all_gather(w_gate, ("dp", "ctx"), axis=0, tiled=True),
        lax.all_gather(w_up, ("dp", "ctx"), axis=0, tiled=True),
        lax.all_gather(w_down, ("dp", "ctx"), axis=1, tiled=True),
        lax.all_gather(mlp_gain, ("dp", "ctx"), axis=0, tiled=True),
    )
    gate_weight, up_weight, down_weight, mlp_scale = gathered_mlp
    segments_all = lax.all_gather(segment_ids, "ctx", axis=1, tiled=True)
    local_heads = query_weight.shape[1] // HEAD_DIM
    local_kv = key_weight.shape[1] // HEAD_DIM
    group_size = local_heads // local_kv
    kv_width = local_kv * HEAD_DIM
    score_scale = 1.0 / math.sqrt(HEAD_DIM)
    stream = inputs.astype(jnp.float32).reshape(row_count, width)
    normed_attn, attn_norm_pullback = jax.vjp(rms_norm, stream, attn_scale.astype(jnp.float32))
    normed_low = normed_attn.astype(jnp.bfloat16)
    query_raw = jnp.dot(normed_low, query_weight, preferred_element_type=jnp.float32).reshape(
        seq_count, tok_count, local_heads, HEAD_DIM
    )
    key_raw = jnp.dot(normed_low, key_weight, preferred_element_type=jnp.float32).reshape(
        seq_count, tok_count, local_kv, HEAD_DIM
    )
    value_low = (
        jnp.dot(normed_low, value_weight, preferred_element_type=jnp.float32)
        .astype(jnp.bfloat16)
        .reshape(seq_count, tok_count, kv_width)
    )
    cosine_table, sine_table = rope_tables(positions, HEAD_DIM)
    cosine_table = cosine_table[:, :, None, :]
    sine_table = sine_table[:, :, None, :]

    def norm_rope(raw_heads, gain_vector):
        return head_norm(raw_heads, gain_vector, cosine_table, sine_table)

    query_rot, query_pullback = jax.vjp(norm_rope, query_raw, query_scale.astype(jnp.float32))
    key_rot, key_pullback = jax.vjp(norm_rope, key_raw, key_scale.astype(jnp.float32))
    query_low = query_rot.astype(jnp.bfloat16).reshape(
        seq_count, tok_count, local_kv, group_size, HEAD_DIM
    )
    key_low = key_rot.astype(jnp.bfloat16).reshape(seq_count, tok_count, kv_width)
    query_index = cycle_rank * tok_count + jnp.arange(tok_count, dtype=jnp.int32)

    def block_scores(key_block, first_row):
        key_count = key_block.shape[1]
        key_heads = key_block.reshape(seq_count, key_count, local_kv, HEAD_DIM)
        raw_scores = (
            jnp.einsum(
                "stkgd,snkd->skgtn", query_low, key_heads, preferred_element_type=jnp.float32
            )
            * score_scale
        )
        key_index = first_row + jnp.arange(key_count, dtype=jnp.int32)
        key_segments = lax.dynamic_slice_in_dim(segments_all, first_row, key_count, 1)
        allowed = (key_index[None, None, :] <= query_index[None, :, None]) & (
            key_segments[:, None, :] == segment_ids[:, :, None]
        )
        return (raw_scores, allowed[:, None, None, :, :])

    stat_shape = (seq_count, local_kv, group_size, tok_count)
    pieces = (
        lax.all_gather(key_low, "ctx", axis=1, tiled=True),
        lax.all_gather(value_low, "ctx", axis=1, tiled=True),
    )
    row_best = jnp.full(stat_shape, masked_value, jnp.float32)
    raw_scores, allowed = block_scores(pieces[0], jnp.int32(0))
    masked = jnp.where(allowed, raw_scores, masked_value)
    new_best = jnp.maximum(row_best, jnp.max(masked, axis=-1))
    weights = jnp.where(allowed, jnp.exp(masked - new_best[..., None]), 0.0)
    value_heads = pieces[1].reshape(seq_count, pieces[1].shape[1], local_kv, HEAD_DIM)
    added = jnp.einsum(
        "skgtn,snkd->skgtd",
        weights.astype(jnp.bfloat16),
        value_heads,
        preferred_element_type=jnp.float32,
    )
    row_total = jnp.sum(weights, axis=-1)
    log_total = new_best + jnp.log(row_total)
    attended = added / row_total[..., None]
    attended_low = (
        jnp.transpose(attended, (0, 3, 1, 2, 4))
        .reshape(row_count, local_heads * HEAD_DIM)
        .astype(jnp.bfloat16)
    )
    attn_part = jnp.dot(attended_low, out_weight, preferred_element_type=jnp.float32)
    middle = stream + lax.psum(attn_part.astype(jnp.bfloat16), "tensor").astype(jnp.float32)
    normed_mid, mlp_norm_pullback = jax.vjp(rms_norm, middle, mlp_scale.astype(jnp.float32))
    mid_low = normed_mid.astype(jnp.bfloat16)
    gate = jnp.dot(mid_low, gate_weight, preferred_element_type=jnp.float32)
    upward = jnp.dot(mid_low, up_weight, preferred_element_type=jnp.float32)
    hidden, silu_pullback = jax.vjp(silu_product, gate, upward)
    hidden_low = hidden.astype(jnp.bfloat16)
    down_part = jnp.dot(hidden_low, down_weight, preferred_element_type=jnp.float32)
    down_sum = lax.psum(down_part.astype(jnp.bfloat16), "tensor").astype(jnp.float32)
    output = (middle + down_sum).astype(jnp.bfloat16).reshape(seq_count, tok_count, width)
    grad_low = out_grad.reshape(row_count, width)
    down_weight_grad = jnp.dot(hidden_low.T, grad_low, preferred_element_type=jnp.float32)
    hidden_grad = jnp.dot(grad_low, down_weight.T, preferred_element_type=jnp.float32)
    gate_grad, upward_grad = silu_pullback(hidden_grad)
    gate_grad_low = gate_grad.astype(jnp.bfloat16)
    upward_grad_low = upward_grad.astype(jnp.bfloat16)
    gate_weight_grad = jnp.dot(mid_low.T, gate_grad_low, preferred_element_type=jnp.float32)
    up_weight_grad = jnp.dot(mid_low.T, upward_grad_low, preferred_element_type=jnp.float32)
    mid_grad_part = jnp.dot(
        gate_grad_low, gate_weight.T, preferred_element_type=jnp.float32
    ) + jnp.dot(upward_grad_low, up_weight.T, preferred_element_type=jnp.float32)
    mid_grad = lax.psum(mid_grad_part.astype(jnp.bfloat16), "tensor").astype(jnp.float32)
    middle_norm_grad, mlp_gain_grad = mlp_norm_pullback(mid_grad)
    middle_grad = grad_low.astype(jnp.float32) + middle_norm_grad
    mlp_grads = (
        lax.psum_scatter(gate_weight_grad, ("dp", "ctx"), scatter_dimension=0, tiled=True),
        lax.psum_scatter(up_weight_grad, ("dp", "ctx"), scatter_dimension=0, tiled=True),
        lax.psum_scatter(down_weight_grad, ("dp", "ctx"), scatter_dimension=1, tiled=True),
        lax.psum_scatter(mlp_gain_grad, ("dp", "ctx"), scatter_dimension=0, tiled=True),
    )
    branch_grad = middle_grad.astype(jnp.bfloat16)
    out_weight_grad = jnp.dot(attended_low.T, branch_grad, preferred_element_type=jnp.float32)
    attended_grad = jnp.dot(branch_grad, out_weight.T, preferred_element_type=jnp.float32).astype(
        jnp.bfloat16
    )
    attended_grad_heads = jnp.transpose(
        attended_grad.reshape(seq_count, tok_count, local_kv, group_size, HEAD_DIM), (0, 2, 3, 1, 4)
    )
    row_delta = jnp.sum(attended_grad_heads.astype(jnp.float32) * attended, axis=-1)

    def key_block_grads(key_block, value_block, first_row):
        raw_scores, allowed = block_scores(key_block, first_row)
        probability = jnp.where(allowed, jnp.exp(raw_scores - log_total[..., None]), 0.0)
        key_count = key_block.shape[1]
        value_heads = value_block.reshape(seq_count, key_count, local_kv, HEAD_DIM)
        key_heads = key_block.reshape(seq_count, key_count, local_kv, HEAD_DIM)
        prob_grad = jnp.einsum(
            "skgtd,snkd->skgtn",
            attended_grad_heads,
            value_heads,
            preferred_element_type=jnp.float32,
        )
        score_grad = (probability * (prob_grad - row_delta[..., None])).astype(jnp.bfloat16)
        query_add = jnp.einsum(
            "skgtn,snkd->skgtd", score_grad, key_heads, preferred_element_type=jnp.float32
        )
        key_add = jnp.einsum(
            "skgtn,stkgd->snkd", score_grad, query_low, preferred_element_type=jnp.float32
        ).reshape(seq_count, key_count, kv_width)
        value_add = jnp.einsum(
            "skgtn,skgtd->snkd",
            probability.astype(jnp.bfloat16),
            attended_grad_heads,
            preferred_element_type=jnp.float32,
        ).reshape(seq_count, key_count, kv_width)
        return (query_add, key_add, value_add)

    query_zero = jnp.zeros(stat_shape + (HEAD_DIM,), jnp.float32)
    kv_zero = jnp.zeros((seq_count, tok_count, kv_width), jnp.float32)

    def cycle_turn(turn_index, state):
        key_block, value_block, key_grad_acc, value_grad_acc, query_grad_acc = state
        owner_rank = (cycle_rank + turn_index) % cycle_size
        query_add, key_add, value_add = key_block_grads(
            key_block, value_block, owner_rank * tok_count
        )
        moved_blocks = from_behind((key_block, value_block), "ctx", -1)
        moved_grads = (
            from_behind((key_grad_acc + key_add).astype(jnp.bfloat16), "ctx", -1).astype(
                jnp.float32
            ),
            from_behind((value_grad_acc + value_add).astype(jnp.bfloat16), "ctx", -1).astype(
                jnp.float32
            ),
        )
        return (
            moved_blocks[0],
            moved_blocks[1],
            moved_grads[0],
            moved_grads[1],
            query_grad_acc + query_add,
        )

    final_state = lax.fori_loop(
        0, cycle_size, cycle_turn, (key_low, value_low, kv_zero, kv_zero, query_zero)
    )
    key_grad_sum = final_state[2]
    value_grad_sum = final_state[3]
    query_grad_sum = final_state[4]
    query_grad = (
        jnp.transpose(query_grad_sum, (0, 3, 1, 2, 4)).reshape(
            seq_count, tok_count, local_heads, HEAD_DIM
        )
        * score_scale
    )
    query_raw_grad, query_gain_grad = query_pullback(query_grad)
    key_raw_grad, key_gain_grad = key_pullback(
        (key_grad_sum * score_scale).reshape(seq_count, tok_count, local_kv, HEAD_DIM)
    )
    query_grad_low = query_raw_grad.reshape(row_count, local_heads * HEAD_DIM).astype(jnp.bfloat16)
    key_grad_low = key_raw_grad.reshape(row_count, kv_width).astype(jnp.bfloat16)
    value_grad_low = value_grad_sum.reshape(row_count, kv_width).astype(jnp.bfloat16)
    query_weight_grad = jnp.dot(normed_low.T, query_grad_low, preferred_element_type=jnp.float32)
    key_weight_grad = jnp.dot(normed_low.T, key_grad_low, preferred_element_type=jnp.float32)
    value_weight_grad = jnp.dot(normed_low.T, value_grad_low, preferred_element_type=jnp.float32)
    normed_grad_part = (
        jnp.dot(query_grad_low, query_weight.T, preferred_element_type=jnp.float32)
        + jnp.dot(key_grad_low, key_weight.T, preferred_element_type=jnp.float32)
        + jnp.dot(value_grad_low, value_weight.T, preferred_element_type=jnp.float32)
    )
    normed_grad, query_gain_total, key_gain_total = (
        lax.psum(normed_grad_part.astype(jnp.bfloat16), "tensor").astype(jnp.float32),
        lax.psum(query_gain_grad.astype(jnp.bfloat16), "tensor").astype(jnp.float32),
        lax.psum(key_gain_grad.astype(jnp.bfloat16), "tensor").astype(jnp.float32),
    )
    stream_norm_grad, attn_gain_grad = attn_norm_pullback(normed_grad)
    input_grad = (
        (middle_grad + stream_norm_grad).astype(jnp.bfloat16).reshape(seq_count, tok_count, width)
    )
    attn_grads = (
        lax.psum_scatter(query_weight_grad, ("dp", "ctx"), scatter_dimension=0, tiled=True),
        lax.psum_scatter(key_weight_grad, ("dp", "ctx"), scatter_dimension=0, tiled=True),
        lax.psum_scatter(value_weight_grad, ("dp", "ctx"), scatter_dimension=0, tiled=True),
        lax.psum_scatter(out_weight_grad, ("dp", "ctx"), scatter_dimension=1, tiled=True),
        lax.psum_scatter(attn_gain_grad, ("dp", "ctx"), scatter_dimension=0, tiled=True),
        lax.psum_scatter(query_gain_total, ("dp", "ctx"), scatter_dimension=0, tiled=True),
        lax.psum_scatter(key_gain_total, ("dp", "ctx"), scatter_dimension=0, tiled=True),
    )
    return (
        output,
        input_grad,
        attn_grads[4],
        attn_grads[0],
        attn_grads[1],
        attn_grads[2],
        attn_grads[5],
        attn_grads[6],
        attn_grads[3],
        mlp_grads[3],
        mlp_grads[0],
        mlp_grads[1],
        mlp_grads[2],
    )


def solution(mesh):
    in_specs = (
        P("dp", "ctx", None),
        P("dp", "ctx"),
        P("dp", "ctx"),
        P("dp", "ctx", None),
        P(("dp", "ctx")),
        P(("dp", "ctx"), "tensor"),
        P(("dp", "ctx"), "tensor"),
        P(("dp", "ctx"), "tensor"),
        P(("dp", "ctx")),
        P(("dp", "ctx")),
        P("tensor", ("dp", "ctx")),
        P(("dp", "ctx")),
        P(("dp", "ctx"), "tensor"),
        P(("dp", "ctx"), "tensor"),
        P("tensor", ("dp", "ctx")),
    )
    out_specs = (
        P("dp", "ctx", None),
        P("dp", "ctx", None),
        P(("dp", "ctx")),
        P(("dp", "ctx"), "tensor"),
        P(("dp", "ctx"), "tensor"),
        P(("dp", "ctx"), "tensor"),
        P(("dp", "ctx")),
        P(("dp", "ctx")),
        P("tensor", ("dp", "ctx")),
        P(("dp", "ctx")),
        P(("dp", "ctx"), "tensor"),
        P(("dp", "ctx"), "tensor"),
        P("tensor", ("dp", "ctx")),
    )

    def step(*args):
        body = on_device_sliced if can_slice(mesh, args[0], args[6], args[12]) else on_device
        return jax.shard_map(
            body, mesh=mesh, in_specs=in_specs, out_specs=out_specs, check_vma=False
        )(*args)

    return step
```

```python
import math
from types import SimpleNamespace

import jax
import jax.numpy as jnp
from jax import lax
from jax.experimental import pallas as pl
from jax.experimental.pallas import tpu as pltpu
from jax.sharding import PartitionSpec as P

HEAD_DIM = 128
BF16 = jnp.bfloat16
F32 = jnp.float32
MESH = pl.DeviceIdType.MESH
TILE = (8, 128)
DP, CTX, TENSOR = "dp", "ctx", "tensor"

epsilon = 1e-06
rope_base = 1000000.0
masked_value = -1e30


def from_behind(value, axis, steps):
    count = lax.axis_size(axis)
    pairs = [(source, (source + steps) % count) for source in range(count)]
    return lax.ppermute(value, axis, pairs)


def rope_tables(positions, head_size):
    half_dim = head_size // 2
    frequency = rope_base ** (-(jnp.arange(half_dim, dtype=jnp.float32) * 2.0) / head_size)
    angles = positions.astype(jnp.float32)[..., None] * frequency
    return (jnp.cos(angles), jnp.sin(angles))


def rotate(values, cosine_table, sine_table):
    half_dim = values.shape[-1] // 2
    first_half = values[..., :half_dim]
    second_half = values[..., half_dim:]
    return jnp.concatenate(
        [
            first_half * cosine_table - second_half * sine_table,
            second_half * cosine_table + first_half * sine_table,
        ],
        axis=-1,
    )


def head_norm(raw_heads, gain_vector, cosine_table, sine_table):
    scaled = (
        raw_heads
        * lax.rsqrt(jnp.mean(raw_heads * raw_heads, axis=-1, keepdims=True) + epsilon)
        * gain_vector
    )
    return rotate(scaled, cosine_table, sine_table)


def rms_norm(stream, gain_vector):
    return (
        stream
        * lax.rsqrt(jnp.mean(stream * stream, axis=-1, keepdims=True) + epsilon)
        * gain_vector
    )


def silu_product(gate, upward):
    return jax.nn.silu(gate) * upward


def dot32(left, right, spec):
    return jnp.einsum(spec, left, right, preferred_element_type=F32)


def shift(value, axis, steps):
    count = lax.axis_size(axis)
    pairs = [(source, (source + steps) % count) for source in range(count)]
    return lax.ppermute(value, axis, pairs)


def take_ring(blocks, first):
    return lax.dynamic_slice_in_dim(jnp.concatenate([blocks, blocks]), first, blocks.shape[0], 0)


def block_ahead(blocks, steps):
    count = lax.axis_size(CTX)
    place = (lax.axis_index(CTX) + steps) % count
    return lax.dynamic_index_in_dim(blocks, place, 0, keepdims=False)


def gather_ctx(block):
    count = lax.axis_size(CTX)
    rank = lax.axis_index(CTX)
    got = jnp.stack([block] + [shift(block, CTX, -d) for d in range(1, count)])
    return take_ring(got, (count - rank) % count)


def scatter_sum(blocks):
    total = block_ahead(blocks, 0).astype(F32)
    for d in range(1, blocks.shape[0]):
        total = total + shift(block_ahead(blocks, d), CTX, d).astype(F32)
    return total


def swap_by_target(blocks):
    count = lax.axis_size(CTX)
    rank = lax.axis_index(CTX)
    got = [shift(block_ahead(blocks, d), CTX, d) for d in range(1, count)]
    got = jnp.stack([block_ahead(blocks, 0)] + got[::-1])
    return take_ring(got, (count - rank) % count)


def greet(peers):
    barrier = pltpu.get_barrier_semaphore()
    for peer in peers:
        pl.semaphore_signal(barrier, inc=1, device_id=peer, device_id_type=MESH)
    pl.semaphore_wait(barrier, len(peers))


def remote(source, target, send_sem, recv_sem, peer):
    copy = pltpu.make_async_remote_copy(
        src_ref=source,
        dst_ref=target,
        send_sem=send_sem,
        recv_sem=recv_sem,
        device_id=peer,
        device_id_type=MESH,
    )
    copy.start()
    return copy


def to_tile(values):
    return jnp.pad(values, (0, math.prod(TILE) - values.shape[0])).reshape(TILE)


def place():
    pair, rank, half = lax.axis_index(DP), lax.axis_index(CTX), lax.axis_index(TENSOR)
    core = lax.rem(pair, 2)
    return SimpleNamespace(
        pair=pair,
        rank=rank,
        half=half,
        sibling=pair + 1 - 2 * core,
        across=lax.rem(pair + 2, 4),
        twin=1 - half,
    )


class Relay:
    KINDS = 9

    def __init__(self, here, source, view, rows, send_sem, recv_sem):
        self.here, self.source, self.view, self.rows = here, source, view, rows
        self.send_sem, self.recv_sem = send_sem, recv_sem
        self.copies = {}

    def go(self, kind, source, target, peer):
        self.copies[kind] = remote(
            source, target, self.send_sem.at[kind], self.recv_sem.at[kind], peer
        )

    def first(self):
        p = self.here
        target = self.view(p.half, p.pair, 0, self.rows)
        self.go(1, self.source, target, {DP: p.across})
        self.go(2, self.source, target, {TENSOR: p.twin})
        self.go(0, self.source, target, {DP: p.sibling})

    def second(self):
        p, part = self.here, self.rows // 2
        self.copies[1].wait_recv()
        low = self.view(p.half, p.across, 0, part)
        self.go(4, low, low, {TENSOR: p.twin})
        whole = self.view(p.half, p.across, 0, self.rows)
        self.go(3, whole, whole, {DP: p.sibling})
        self.copies[2].wait_recv()
        high = self.view(p.twin, p.pair, part, part)
        self.go(6, high, high, {DP: p.across})
        whole = self.view(p.twin, p.pair, 0, self.rows)
        self.go(5, whole, whole, {DP: p.sibling})

    def third(self):
        p, part = self.here, self.rows // 2
        self.copies[4].wait_recv()
        low = self.view(p.twin, p.across, 0, part)
        self.go(7, low, low, {DP: p.sibling})
        self.copies[6].wait_recv()
        high = self.view(p.twin, p.across, part, part)
        self.go(8, high, high, {DP: p.sibling})

    def last(self):
        for kind in (0, 3, 5, 7, 8):
            self.copies[kind].wait_recv()
        for copy in self.copies.values():
            copy.wait_send()


class Chain:
    def __init__(self, rank, count, source, result, send_sem, recv_sem):
        self.rank, self.count, self.source, self.result = rank, count, source, result
        self.send_sem, self.recv_sem = send_sem, recv_sem

    def copy(self, way, step):
        step_to = self.rank + (1 if way == 0 else -1)
        owner = self.rank - step if way == 0 else self.rank + step
        owner = jnp.clip(owner, 0, self.count - 1)
        return pltpu.make_async_remote_copy(
            src_ref=self.source if step == 0 else self.result.at[owner],
            dst_ref=self.result.at[owner],
            send_sem=self.send_sem.at[way, step],
            recv_sem=self.recv_sem.at[way, step],
            device_id={CTX: jnp.clip(step_to, 0, self.count - 1)},
            device_id_type=MESH,
        )

    def sends(self, way, step):
        if way == 0:
            return (self.rank >= step) & (self.rank < self.count - 1)
        return (self.rank + step < self.count) & (self.rank > 0)

    def receives(self, way, step):
        return self.rank > step if way == 0 else self.rank + step < self.count - 1

    def start(self, step):
        for way in (0, 1):
            if step > 0:

                @pl.when(self.receives(way, step - 1))
                def _():
                    self.copy(way, step - 1).wait_recv()

            @pl.when(self.sends(way, step))
            def _():
                self.copy(way, step).start()

    def finish(self):
        last = self.count - 2
        for way in (0, 1):

            @pl.when(self.receives(way, last))
            def _():
                self.copy(way, last).wait_recv()

            for step in range(self.count - 1):

                @pl.when(self.sends(way, step))
                def _():
                    self.copy(way, step).wait_send()


SEMS = pltpu.SemaphoreType.DMA
ANYWHERE = pl.BlockSpec(memory_space=pl.ANY)
ON_CHIP = pl.BlockSpec(memory_space=pltpu.VMEM)


def enter(gains, marks, block, w_query, w_key, w_value, out_shard):
    count, pairs = lax.axis_size(CTX), lax.axis_size(DP)
    owners = count * pairs
    depth = w_query.shape[0]
    widths = [w.shape[1] // count for w in (w_query, w_key, w_value)]
    width = sum(widths)
    spots = [sum(widths[:i]) for i in range(3)]
    rows = block.shape[0]

    def kernel(
        gain_ref, mark_ref, block_ref, wq_ref, wk_ref, wv_ref, wo_ref,
        gains_ref, marks_ref, rows_ref, weight_ref, out_ref,
        held, held_out, out_send, out_recv, out_relay_send, out_relay_recv, gain_send, gain_recv, mark_send, mark_recv,
        swap_send, swap_recv, chain_send, chain_recv, relay_send, relay_recv, local_sem,
    ):
        here = place()
        rank, pair, half = here.rank, here.pair, here.half
        me = pair * count + rank
        far = [lax.rem(me + k, owners) for k in range(1, owners)]
        far = [{DP: lax.div(t, count), CTX: lax.rem(t, count)} for t in far]
        near = [{CTX: lax.rem(rank + k, count)} for k in range(1, count)]
        greet(far + [{TENSOR: here.twin}])

        def view(owner_rank):
            def at(t, p, start, size):
                first = pl.multiple_of((p * count + owner_rank) * depth + start, 64)
                return weight_ref.at[pl.ds(first, size), pl.ds(pl.multiple_of(t * width, 128), width)]

            return at

        def out_view(owner_rank):
            def at(t, p, start, size):
                first = t * owners * depth + (p * count + owner_rank) * depth + start
                return out_ref.at[pl.ds(pl.multiple_of(first, 64), size)]

            return at

        def columns(ref, i, target):
            return ref.at[:, pl.ds(pl.multiple_of(target * widths[i], 128), widths[i])]

        sources = (wq_ref, wk_ref, wv_ref)
        takes = [
            pltpu.make_async_copy(
                columns(ref, i, rank), held.at[:, pl.ds(spots[i], widths[i])], local_sem.at[i]
            )
            for i, ref in enumerate(sources)
        ]
        takes.append(pltpu.make_async_copy(wo_ref, held_out, local_sem.at[4]))
        for take in takes:
            take.start()
        small = [
            remote(mark_ref, marks_ref.at[rank], mark_send.at[k], mark_recv.at[k], peer)
            for k, peer in enumerate(near)
        ]
        small += [
            remote(gain_ref, gains_ref.at[me], gain_send.at[k], gain_recv.at[k], peer)
            for k, peer in enumerate(far)
        ]
        own_rows = pl.ds(pl.multiple_of(me * depth, depth), depth)
        swaps = []
        for k, peer in enumerate(near):
            swaps.append([])
            for i, ref in enumerate(sources):
                spot = pl.ds(pl.multiple_of(half * width + spots[i], 128), widths[i])
                swaps[k].append(
                    remote(
                        columns(ref, i, peer[CTX]),
                        weight_ref.at[own_rows, spot],
                        swap_send.at[k, i],
                        swap_recv.at[k, i],
                        peer,
                    )
                )
        chain = Chain(rank, count, block_ref, rows_ref, chain_send, chain_recv)
        chain.start(0)
        out_own = out_view(rank)(half, pair, 0, depth)
        outs = [
            remote(wo_ref, out_own, out_send.at[k], out_recv.at[k], peer)
            for k, peer in enumerate(near)
        ]
        gains_ref[me] = gain_ref[...]
        marks_ref[rank] = mark_ref[...]
        for take in takes:
            take.wait()
        keep = pltpu.make_async_copy(held, view(rank)(half, pair, 0, depth), local_sem.at[3])
        keep.start()
        keep_out = pltpu.make_async_copy(held_out, out_own, local_sem.at[5])
        keep_out.start()
        relays = [Relay(here, held, view(rank), depth, relay_send.at[0], relay_recv.at[0])]
        relays[0].first()
        for k in range(1, count):
            owner = lax.rem(rank - k + count, count)
            for swap in swaps[k - 1]:
                swap.wait_recv()
            at = view(owner)
            relays.append(
                Relay(here, at(half, pair, 0, depth), at, depth, relay_send.at[k], relay_recv.at[k])
            )
            relays[k].first()
            relays[k - 1].second()
            if k > 1:
                relays[k - 2].third()

        def out_relay(k):
            owner = lax.rem(rank - k + count, count)
            at = out_view(owner)
            source = at(half, pair, 0, depth) if k else held_out
            return Relay(here, source, at, depth, out_relay_send.at[k], out_relay_recv.at[k])

        out_relays = [out_relay(k) for k in range(count)]
        out_relays[0].first()
        chain.start(1)
        relays[-1].second()
        relays[-2].third()
        for k in range(1, count):
            outs[k - 1].wait_recv()
            out_relays[k].first()
            out_relays[k - 1].second()
            (relays[-1] if k == 1 else out_relays[k - 2]).third()
        chain.start(2)
        out_relays[-1].second()
        out_relays[-2].third()
        out_relays[-1].third()
        for relay in relays + out_relays:
            relay.last()
        keep.wait()
        keep_out.wait()
        for copy in outs:
            copy.wait_send()
        chain.finish()
        for swap in swaps:
            for copy in swap:
                copy.wait_send()
        for copy in small:
            copy.wait()

    return pl.pallas_call(
        kernel,
        out_shape=(
            jax.ShapeDtypeStruct((owners, *TILE), F32),
            jax.ShapeDtypeStruct((count, *TILE), jnp.int32),
            jax.ShapeDtypeStruct((count, rows, block.shape[1]), block.dtype),
            jax.ShapeDtypeStruct((owners * depth, 2 * width), w_query.dtype),
            jax.ShapeDtypeStruct((2 * owners * depth, out_shard.shape[1]), out_shard.dtype),
        ),
        in_specs=[ON_CHIP] * 2 + [ANYWHERE] * 5,
        out_specs=(ON_CHIP, ON_CHIP, ANYWHERE, ANYWHERE, ANYWHERE),
        scratch_shapes=[
            pltpu.VMEM((depth, width), w_query.dtype),
            pltpu.VMEM(out_shard.shape, out_shard.dtype),
            SEMS((count - 1,)),
            SEMS((count - 1,)),
            SEMS((count, Relay.KINDS)),
            SEMS((count, Relay.KINDS)),
            SEMS((owners - 1,)),
            SEMS((owners - 1,)),
            SEMS((count - 1,)),
            SEMS((count - 1,)),
            SEMS((count - 1, 3)),
            SEMS((count - 1, 3)),
            SEMS((2, count - 1)),
            SEMS((2, count - 1)),
            SEMS((count, Relay.KINDS)),
            SEMS((count, Relay.KINDS)),
            SEMS((6,)),
        ],
        compiler_params=pltpu.CompilerParams(collective_id=0, has_side_effects=True),
        name="enter",
    )(gains, marks, block, w_query, w_key, w_value, out_shard)


def spread_mlp(first, second, pieces):
    count, pairs = lax.axis_size(CTX), lax.axis_size(DP)
    kinds, depth, width = pieces[0].shape
    rows, features = first.shape

    def kernel(first_ref, second_ref, *rest):
        piece_refs, rest = rest[:count], rest[count:]
        firsts_ref, seconds_ref = rest[:2]
        weight_refs, rest = rest[2 : 2 + kinds], rest[2 + kinds :]
        held, chain_send, chain_recv, relay_send, relay_recv, take_sem, keep_sem = rest
        here = place()
        rank, pair, half = here.rank, here.pair, here.half
        greet(
            [{CTX: lax.rem(rank + k, count)} for k in range(1, count)]
            + [{DP: here.sibling}, {DP: here.across}, {TENSOR: here.twin}]
        )
        takes = []
        for i in range(kinds):
            for d, ref in enumerate(piece_refs):
                owner = lax.rem(rank - d + count, count)
                take = pltpu.make_async_copy(
                    ref.at[i],
                    held.at[i, pl.ds(pl.multiple_of(owner * depth, depth), depth)],
                    take_sem.at[i, d],
                )
                take.start()
                takes.append(take)
        chains = [
            Chain(rank, count, first_ref, firsts_ref, chain_send.at[0], chain_recv.at[0]),
            Chain(rank, count, second_ref, seconds_ref, chain_send.at[1], chain_recv.at[1]),
        ]
        chains[0].start(0)
        block = count * depth

        def view(i):
            def at(t, p, start, size):
                first = pl.multiple_of(p * block + start, 64)
                return weight_refs[i].at[
                    pl.ds(first, size), pl.ds(pl.multiple_of(t * width, 128), width)
                ]

            return at

        relays, keeps = [], []
        for i in range(kinds):
            for take in takes[i * count : (i + 1) * count]:
                take.wait()
            keeps.append(
                pltpu.make_async_copy(held.at[i], view(i)(half, pair, 0, block), keep_sem.at[i])
            )
            keeps[i].start()
            relays.append(
                Relay(here, held.at[i], view(i), block, relay_send.at[i], relay_recv.at[i])
            )
            relays[i].first()
        chains[0].start(1)
        relays[0].second()
        chains[0].start(2)
        chains[1].start(0)
        relays[0].third()
        relays[1].second()
        chains[1].start(1)
        relays[1].third()
        relays[2].second()
        chains[1].start(2)
        relays[2].third()
        for relay in relays:
            relay.last()
        for keep in keeps:
            keep.wait()
        for chain in chains:
            chain.finish()

    return pl.pallas_call(
        kernel,
        out_shape=(
            jax.ShapeDtypeStruct((count, rows, features), first.dtype),
            jax.ShapeDtypeStruct((count, rows, features), second.dtype),
        )
        + (jax.ShapeDtypeStruct((pairs * count * depth, 2 * width), pieces[0].dtype),) * kinds,
        in_specs=[ANYWHERE] * (2 + count),
        out_specs=(ANYWHERE,) * (2 + kinds),
        scratch_shapes=[
            pltpu.VMEM((kinds, count * depth, width), pieces[0].dtype),
            SEMS((2, 2, count - 1)),
            SEMS((2, 2, count - 1)),
            SEMS((kinds, Relay.KINDS)),
            SEMS((kinds, Relay.KINDS)),
            SEMS((kinds, count)),
            SEMS((kinds,)),
        ],
        compiler_params=pltpu.CompilerParams(
            collective_id=2, has_side_effects=True, vmem_limit_bytes=16 * 1024 * 1024
        ),
        name="spread_mlp",
    )(first, second, *pieces)


def swap_ctx(blocks, collective_id):
    count = lax.axis_size(CTX)

    def kernel(blocks_ref, got_ref, held, send_sem, recv_sem, local_sem):
        rank = lax.axis_index(CTX)
        peers = [lax.rem(rank + k, count) for k in range(1, count)]
        greet([{CTX: peer} for peer in peers])
        copies = [
            remote(
                blocks_ref.at[peer], got_ref.at[rank], send_sem.at[k], recv_sem.at[k], {CTX: peer}
            )
            for k, peer in enumerate(peers)
        ]
        take = pltpu.make_async_copy(blocks_ref.at[rank], held, local_sem.at[0])
        take.start()
        take.wait()
        keep = pltpu.make_async_copy(held, got_ref.at[rank], local_sem.at[1])
        keep.start()
        keep.wait()
        for copy in copies:
            copy.wait()

    return pl.pallas_call(
        kernel,
        out_shape=jax.ShapeDtypeStruct(blocks.shape, blocks.dtype),
        in_specs=[ANYWHERE],
        out_specs=ANYWHERE,
        scratch_shapes=[
            pltpu.VMEM(blocks.shape[1:], blocks.dtype),
            SEMS((count - 1,)),
            SEMS((count - 1,)),
            SEMS((2,)),
        ],
        compiler_params=pltpu.CompilerParams(collective_id=collective_id, has_side_effects=True),
        name=f"swap_ctx_{collective_id}",
    )(blocks)


def sum_tail(blocks, partial):
    count = lax.axis_size(CTX)
    tensors, depth, width = partial.shape
    part = depth // 4
    low = part // 2
    own = part // count
    tile = 64

    def kernel(
        blocks_ref, partial_ref, got_ref, owned_ref,
        held, kept, near, mine, far, near_b, far_b, result,
        send_sem, recv_sem, block_send, block_recv, swap_send, swap_recv, local_sem,
    ):
        here = place()
        rank, pair, half = here.rank, here.pair, here.half
        core, side = lax.rem(pair, 2), lax.div(pair, 2)
        peers = [lax.rem(rank + k, count) for k in range(1, count)]
        greet(
            [{CTX: peer} for peer in peers]
            + [{DP: here.sibling}, {DP: here.across}, {TENSOR: here.twin}]
        )

        def rows_of(t, x, c):
            return partial_ref.at[t, pl.ds(pl.multiple_of((x * 2 + c) * part, part), part)]

        copies = {}
        for t in range(tensors):
            for x in range(2):
                copies[0, t, x] = remote(
                    rows_of(t, x, 1 - core),
                    near.at[t, x],
                    send_sem.at[t * 2 + x],
                    recv_sem.at[t * 2 + x],
                    {DP: here.sibling},
                )
        takes = [
            pltpu.make_async_copy(rows_of(t, x, core), kept.at[t, x], local_sem.at[t * 2 + x])
            for t in range(tensors)
            for x in range(2)
        ]
        for take in takes:
            take.start()
        moves = [
            remote(
                blocks_ref.at[peer], got_ref.at[rank], block_send.at[k], block_recv.at[k], {CTX: peer}
            )
            for k, peer in enumerate(peers)
        ]
        take_own = pltpu.make_async_copy(blocks_ref.at[rank], held, local_sem.at[4])
        take_own.start()

        def add(target, left, right, size):
            @pl.loop(0, size // tile)
            def _(i):
                at = pl.ds(pl.multiple_of(i * tile, tile), tile)
                target[at] = (left[at].astype(F32) + right[at].astype(F32)).astype(BF16)

        for t in range(tensors):
            for x in range(2):
                takes[t * 2 + x].wait()
                copies[0, t, x].wait_recv()
                add(mine.at[t, x], kept.at[t, x], near.at[t, x], part)
        first, second = pl.ds(0, low), pl.ds(low, low)
        for i in range(2):
            copies[1, i] = remote(
                mine.at[here.twin, i, first],
                far.at[i],
                send_sem.at[4 + i],
                recv_sem.at[4 + i],
                {TENSOR: here.twin},
            )
            copies[2, i] = remote(
                mine.at[i, 1 - side, second],
                far_b.at[i],
                send_sem.at[6 + i],
                recv_sem.at[6 + i],
                {DP: here.across},
            )
        for i in range(2):
            copies[1, i].wait_recv()
            add(near.at[0, i], mine.at[half, i, first], far.at[i], low)
            copies[2, i].wait_recv()
            add(near.at[1, i], mine.at[i, side, second], far_b.at[i], low)
        copies[3] = remote(
            near.at[0, 1 - side, first],
            near_b.at[0],
            send_sem.at[8],
            recv_sem.at[8],
            {DP: here.across},
        )
        copies[4] = remote(
            near.at[1, here.twin, first],
            near_b.at[1],
            send_sem.at[9],
            recv_sem.at[9],
            {TENSOR: here.twin},
        )
        take_own.wait()
        keep_own = pltpu.make_async_copy(held, got_ref.at[rank], local_sem.at[5])
        keep_own.start()
        copies[3].wait_recv()
        add(result.at[first], near.at[0, side, first], near_b.at[0], low)
        copies[4].wait_recv()
        add(result.at[second], near.at[1, half, first], near_b.at[1], low)

        def rows_for(target):
            return result.at[pl.ds(pl.multiple_of(target * own, own), own)]

        swaps = [
            remote(
                rows_for(peer), owned_ref.at[rank], swap_send.at[k], swap_recv.at[k], {CTX: peer}
            )
            for k, peer in enumerate(peers)
        ]
        keep = pltpu.make_async_copy(rows_for(rank), owned_ref.at[rank], local_sem.at[6])
        keep.start()
        for copy in swaps + moves:
            copy.wait()
        for copy in copies.values():
            copy.wait_send()
        keep.wait()
        keep_own.wait()

    sixteen = 10
    return pl.pallas_call(
        kernel,
        out_shape=(
            jax.ShapeDtypeStruct(blocks.shape, BF16),
            jax.ShapeDtypeStruct((count, own, width), BF16),
        ),
        in_specs=[ANYWHERE, ANYWHERE],
        out_specs=(ANYWHERE, ANYWHERE),
        scratch_shapes=[
            pltpu.VMEM(blocks.shape[1:], BF16),
            pltpu.VMEM((tensors, 2, part, width), BF16),
            pltpu.VMEM((tensors, 2, part, width), BF16),
            pltpu.VMEM((tensors, 2, part, width), BF16),
            pltpu.VMEM((2, low, width), BF16),
            pltpu.VMEM((2, low, width), BF16),
            pltpu.VMEM((2, low, width), BF16),
            pltpu.VMEM((part, width), BF16),
            SEMS((sixteen,)),
            SEMS((sixteen,)),
            SEMS((count - 1,)),
            SEMS((count - 1,)),
            SEMS((count - 1,)),
            SEMS((count - 1,)),
            SEMS((7,)),
        ],
        compiler_params=pltpu.CompilerParams(
            collective_id=5, has_side_effects=True, vmem_limit_bytes=24 * 1024 * 1024
        ),
        name="sum_tail",
    )(blocks, partial)


def owner_sums(tiles):
    count, pairs, tensors = lax.axis_size(CTX), lax.axis_size(DP), lax.axis_size(TENSOR)
    total = count * pairs * tensors

    def kernel(tiles_ref, sum_ref, got, send_sem, recv_sem):
        owner = lax.axis_index(DP) * count + lax.axis_index(CTX)
        half = lax.axis_index(TENSOR)
        me = owner * tensors + half
        targets = [lax.rem(me + k, total) for k in range(1, total)]
        peers = [
            {
                DP: lax.div(t, count * tensors),
                CTX: lax.rem(lax.div(t, tensors), count),
                TENSOR: lax.rem(t, tensors),
            }
            for t in targets
        ]
        greet(peers)
        copies = [
            remote(
                tiles_ref.at[lax.div(t, tensors)], got.at[me], send_sem.at[k], recv_sem.at[k], peer
            )
            for k, (t, peer) in enumerate(zip(targets, peers))
        ]
        got[me] = tiles_ref[owner]
        for copy in copies:
            copy.wait()
        value = got[0]
        for source in range(1, total):
            value = value + got[source]
        sum_ref[...] = value

    return pl.pallas_call(
        kernel,
        out_shape=jax.ShapeDtypeStruct(TILE, F32),
        in_specs=[ON_CHIP],
        out_specs=ON_CHIP,
        scratch_shapes=[
            pltpu.VMEM((total, *TILE), F32),
            SEMS((total - 1,)),
            SEMS((total - 1,)),
        ],
        compiler_params=pltpu.CompilerParams(collective_id=1, has_side_effects=True),
        name="owner_sums",
    )(tiles)


def whole(shape):
    return pl.BlockSpec(shape, lambda *_: (0,) * len(shape))


def turned(values, cosines, sines):
    return values * cosines + pltpu.roll(values, HEAD_DIM // 2, 1) * sines


def unturned(grads, cosines, sines):
    return grads * cosines + pltpu.roll(grads * sines, HEAD_DIM // 2, 1)


def head_scale(raw):
    return lax.rsqrt(jnp.mean(raw * raw, axis=-1, keepdims=True) + epsilon)


def qkv_forward(blocks, scale, weight, cosines, sines, query_gain, key_gain):
    count, rows, width = blocks.shape
    cols = weight.shape[1]

    def kernel(x_ref, s_ref, w_ref, cos_ref, sin_ref, qg_ref, kg_ref, n_ref, raw_ref, q_ref, kv_ref):
        x = x_ref[0].astype(F32)
        normed = x * lax.rsqrt(jnp.mean(x * x, axis=-1, keepdims=True) + epsilon) * s_ref[...]
        normed = normed.astype(BF16)
        n_ref[...] = normed
        raw = jnp.dot(normed, w_ref[...], preferred_element_type=F32)
        cosine, sine = cos_ref[...], sin_ref[...]
        for head in range(8):
            t, part = head // 4, head % 4
            values = raw[:, head * HEAD_DIM : (head + 1) * HEAD_DIM]
            if part < 3:
                at = (2 * t + part if part < 2 else 4 + t) * HEAD_DIM
                raw_ref[:, at : at + HEAD_DIM] = values
                gain = qg_ref[...] if part < 2 else kg_ref[...]
                values = turned(values * head_scale(values) * gain, cosine, sine)
            if part < 2:
                at = (2 * t + part) * HEAD_DIM
                q_ref[:, at : at + HEAD_DIM] = values.astype(BF16)
            else:
                at = (t if part == 2 else 2 + t) * HEAD_DIM
                kv_ref[:, at : at + HEAD_DIM] = values.astype(BF16)

    def rows_of(size):
        return pl.BlockSpec((rows, size), lambda i: (i, 0))

    total = count * rows
    return pl.pallas_call(
        kernel,
        grid=(count,),
        out_shape=(
            jax.ShapeDtypeStruct((total, width), BF16),
            jax.ShapeDtypeStruct((total, 6 * HEAD_DIM), F32),
            jax.ShapeDtypeStruct((total, 4 * HEAD_DIM), BF16),
            jax.ShapeDtypeStruct((total, 4 * HEAD_DIM), BF16),
        ),
        in_specs=[
            pl.BlockSpec((1, rows, width), lambda i: (i, 0, 0)),
            whole((1, width)),
            whole((width, cols)),
            rows_of(HEAD_DIM),
            rows_of(HEAD_DIM),
            whole((1, HEAD_DIM)),
            whole((1, HEAD_DIM)),
        ],
        out_specs=(rows_of(width), rows_of(6 * HEAD_DIM), rows_of(4 * HEAD_DIM), rows_of(4 * HEAD_DIM)),
        cost_estimate=pl.CostEstimate(
            flops=2 * total * width * cols, bytes_accessed=2 * width * (cols + total), transcendentals=0
        ),
        compiler_params=pltpu.CompilerParams(vmem_limit_bytes=24 * 1024 * 1024),
        name="qkv_forward",
    )(blocks, scale, weight, cosines, sines, query_gain, key_gain)


def probabilities(q, keys, marks):
    seg, index, key_seg, key_index = marks
    scores = []
    for i, key in enumerate(keys):
        s = lax.dot_general(q, key, (((1,), (1,)), ((), ())), preferred_element_type=F32)
        ok = (key_index[i : i + 1] <= index) & (key_seg[i : i + 1] == seg)
        scores.append(jnp.where(ok, s * (1.0 / math.sqrt(HEAD_DIM)), masked_value))
    best = jnp.maximum(*[jnp.max(s, axis=-1, keepdims=True) for s in scores])
    weights = [jnp.exp(s - best) for s in scores]
    total = sum(jnp.sum(w, axis=-1, keepdims=True) for w in weights)
    return [w / total for w in weights]


def key_specs(rows):
    tensors = 2
    specs = []
    for place in (0, tensors):
        specs.append(pl.BlockSpec((rows, HEAD_DIM), lambda t, g, p=place: (0, p + t)))
    return specs * 2


def attend(query, kv_own, kv_twin, marks):
    rows = query.shape[0]

    def kernel(q_ref, k0_ref, v0_ref, k1_ref, v1_ref, *rest):
        marks, out_ref = [ref[...] for ref in rest[:4]], rest[4]
        prob = probabilities(q_ref[...], (k0_ref[...], k1_ref[...]), marks)
        out = jnp.dot(prob[0].astype(BF16), v0_ref[...], preferred_element_type=F32)
        out = out + jnp.dot(prob[1].astype(BF16), v1_ref[...], preferred_element_type=F32)
        out_ref[...] = out.astype(BF16)

    head = pl.BlockSpec((rows, HEAD_DIM), lambda t, g: (0, 2 * t + g))
    return pl.pallas_call(
        kernel,
        grid=(2, 2),
        out_shape=jax.ShapeDtypeStruct(query.shape, BF16),
        in_specs=[head] + key_specs(rows) + [whole(m.shape) for m in marks],
        out_specs=head,
        cost_estimate=pl.CostEstimate(
            flops=32 * rows * rows * HEAD_DIM, bytes_accessed=8 * rows * 512, transcendentals=8 * rows * rows
        ),
        compiler_params=pltpu.CompilerParams(vmem_limit_bytes=32 * 1024 * 1024),
        name="attend",
    )(query, kv_own, kv_own, kv_twin, kv_twin, *marks)


def attend_back(query, kv_own, kv_twin, grad, marks):
    rows = query.shape[0]

    def kernel(q_ref, g_ref, k0_ref, v0_ref, k1_ref, v1_ref, *rest):
        marks = [ref[...] for ref in rest[:4]]
        dq_ref, own_ref, twin_ref, held = rest[4:]
        q, g = q_ref[...], g_ref[...]
        keys = (k0_ref[...], k1_ref[...])
        prob = probabilities(q, keys, marks)
        prob_grad = [
            lax.dot_general(g, v[...], (((1,), (1,)), ((), ())), preferred_element_type=F32)
            for v in (v0_ref, v1_ref)
        ]
        delta = sum(jnp.sum(p * d, axis=-1, keepdims=True) for p, d in zip(prob, prob_grad))
        score = [(p * (d - delta)).astype(BF16) for p, d in zip(prob, prob_grad)]
        dq_ref[...] = sum(
            jnp.dot(s, k, preferred_element_type=F32) for s, k in zip(score, keys)
        )

        def back(left, right):
            return lax.dot_general(
                left, right, (((0,), (0,)), ((), ())), preferred_element_type=F32
            )

        parts = [
            back(score[0], q),
            back(prob[0].astype(BF16), g),
            back(score[1], q),
            back(prob[1].astype(BF16), g),
        ]

        @pl.when(pl.program_id(1) == 0)
        def _():
            own_ref[0], own_ref[1] = parts[0], parts[1]
            held[0], held[1] = parts[2], parts[3]

        @pl.when(pl.program_id(1) == 1)
        def _():
            own_ref[0] += parts[0]
            own_ref[1] += parts[1]
            twin_ref[0] = (held[0] + parts[2]).astype(BF16)
            twin_ref[1] = (held[1] + parts[3]).astype(BF16)

    head = pl.BlockSpec((rows, HEAD_DIM), lambda t, g: (0, 2 * t + g))
    pair = pl.BlockSpec((2, rows, HEAD_DIM), lambda t, g: (0, 0, t))
    return pl.pallas_call(
        kernel,
        grid=(2, 2),
        out_shape=(
            jax.ShapeDtypeStruct(query.shape, F32),
            jax.ShapeDtypeStruct((2, rows, 2 * HEAD_DIM), F32),
            jax.ShapeDtypeStruct((2, rows, 2 * HEAD_DIM), BF16),
        ),
        in_specs=[head, head] + key_specs(rows) + [whole(m.shape) for m in marks],
        out_specs=(head, pair, pair),
        scratch_shapes=[pltpu.VMEM((2, rows, HEAD_DIM), F32)],
        cost_estimate=pl.CostEstimate(
            flops=80 * rows * rows * HEAD_DIM, bytes_accessed=20 * rows * 512, transcendentals=8 * rows * rows
        ),
        compiler_params=pltpu.CompilerParams(vmem_limit_bytes=48 * 1024 * 1024),
        name="attend_back",
    )(query, grad, kv_own, kv_own, kv_twin, kv_twin, *marks)


def qkv_back(raw, query_grad, kv_own, kv_back, cosines, sines, query_gain, key_gain):
    rows = 128
    total = raw.shape[0]
    scale = 1.0 / math.sqrt(HEAD_DIM)

    def kernel(raw_ref, dq_ref, own_ref, back_ref, cos_ref, sin_ref, qg_ref, kg_ref, out_ref, gain_ref):
        cosine, sine = cos_ref[...], sin_ref[...]
        sums = [jnp.zeros((1, HEAD_DIM), F32)] * 2
        kv = own_ref[...] + back_ref[...].astype(F32)
        for t in range(2):
            for part in range(3):
                which = 0 if part < 2 else 1
                at = (2 * t + part if part < 2 else 4 + t) * HEAD_DIM
                values = raw_ref[:, at : at + HEAD_DIM]
                if part < 2:
                    grad = dq_ref[:, at : at + HEAD_DIM]
                else:
                    grad = kv[0, :, t * HEAD_DIM : (t + 1) * HEAD_DIM]
                grad = unturned(grad * scale, cosine, sine)
                r = head_scale(values)
                normed = values * r
                sums[which] = sums[which] + jnp.sum(grad * normed, axis=0, keepdims=True)
                grad = grad * (qg_ref[...] if part < 2 else kg_ref[...])
                grad = r * (grad - normed * jnp.mean(grad * normed, axis=-1, keepdims=True))
                at = (4 * t + part) * HEAD_DIM
                out_ref[:, at : at + HEAD_DIM] = grad.astype(BF16)
            at = (4 * t + 3) * HEAD_DIM
            out_ref[:, at : at + HEAD_DIM] = kv[1, :, t * HEAD_DIM : (t + 1) * HEAD_DIM].astype(BF16)

        @pl.when(pl.program_id(0) == 0)
        def _():
            gain_ref[...] = jnp.zeros_like(gain_ref)

        gain_ref[0:1] += sums[0]
        gain_ref[1:2] += sums[1]

    def rows_of(size):
        return pl.BlockSpec((rows, size), lambda i: (i, 0))

    pair = pl.BlockSpec((2, rows, 2 * HEAD_DIM), lambda i: (0, i, 0))
    return pl.pallas_call(
        kernel,
        grid=(total // rows,),
        out_shape=(
            jax.ShapeDtypeStruct((total, 8 * HEAD_DIM), BF16),
            jax.ShapeDtypeStruct(TILE, F32),
        ),
        in_specs=[
            rows_of(6 * HEAD_DIM),
            rows_of(4 * HEAD_DIM),
            pair,
            pair,
            rows_of(HEAD_DIM),
            rows_of(HEAD_DIM),
            whole((1, HEAD_DIM)),
            whole((1, HEAD_DIM)),
        ],
        out_specs=(rows_of(8 * HEAD_DIM), whole(TILE)),
        cost_estimate=pl.CostEstimate(
            flops=40 * total * 768, bytes_accessed=10 * total * 1024, transcendentals=0
        ),
        compiler_params=pltpu.CompilerParams(vmem_limit_bytes=24 * 1024 * 1024),
        name="qkv_back",
    )(raw, query_grad, kv_own, kv_back, cosines, sines, query_gain, key_gain)


def weight_partials(pairs):
    tokens, depth = pairs[0][0].shape
    tensors = lax.axis_size(TENSOR)
    widths = [right.shape[1] // tensors for _, right in pairs]
    tile = 512

    def kernel(*refs):
        out_ref = refs[-1]
        first = 0
        for i, width in enumerate(widths):
            product = lax.dot_general(
                refs[2 * i][...],
                refs[2 * i + 1][...],
                (((0,), (0,)), ((), ())),
                preferred_element_type=F32,
            )
            out_ref[0, :, first : first + width] = product.astype(BF16)
            first += width

    in_specs = []
    for width in widths:
        in_specs.append(pl.BlockSpec((tokens, tile), lambda t, k: (0, k)))
        in_specs.append(pl.BlockSpec((tokens, width), lambda t, k: (0, t)))
    return pl.pallas_call(
        kernel,
        grid=(tensors, depth // tile),
        out_shape=jax.ShapeDtypeStruct((tensors, depth, sum(widths)), BF16),
        in_specs=in_specs,
        out_specs=pl.BlockSpec((1, tile, sum(widths)), lambda t, k: (t, k, 0)),
        cost_estimate=pl.CostEstimate(
            flops=2 * tokens * depth * sum(widths) * tensors,
            bytes_accessed=2 * depth * tensors * sum(widths) + 4 * tokens * depth,
            transcendentals=0,
        ),
        compiler_params=pltpu.CompilerParams(vmem_limit_bytes=24 * 1024 * 1024),
        name="weight_partials",
    )(*[side for pair in pairs for side in pair])


def scattered(partial):
    count = lax.axis_size(CTX)
    width = partial.shape[2]
    mine = lax.psum_scatter(
        partial.reshape(-1, width), (TENSOR, DP), scatter_dimension=0, tiled=True
    )
    return mine.reshape(count, mine.shape[0] // count, width)


def parts_of(got, widths):
    shards, first = [], 0
    for width in widths:
        part = got[:, :, first : first + width].transpose(1, 0, 2)
        shards.append(part.reshape(part.shape[0], -1).astype(F32))
        first += width
    return shards


def shards_of(mine, widths):
    return parts_of(swap_by_target(mine), widths)


def with_twin(own):
    other = shift(own, TENSOR, 1)
    first = lax.axis_index(TENSOR) == 0
    return jnp.concatenate([jnp.where(first, own, other), jnp.where(first, other, own)])


def on_device_sliced(
    inputs,
    segment_ids,
    positions,
    out_grad,
    attn_gain,
    w_query,
    w_key,
    w_value,
    q_gain,
    k_gain,
    w_out,
    mlp_gain,
    w_gate,
    w_up,
    w_down,
):
    _, tok_count, width = inputs.shape
    count = lax.axis_size(CTX)
    tensors = lax.axis_size(TENSOR)
    rank = lax.axis_index(CTX)
    half = lax.axis_index(TENSOR)
    own_rows = tok_count // tensors
    rows = own_rows * count
    head_rows = w_out.shape[0]
    q_cols = w_query.shape[1] // count
    k_cols = w_key.shape[1] // count
    in_width = q_cols + 2 * k_cols
    piece = attn_gain.shape[0]
    small = q_gain.shape[0]

    input_own = lax.dynamic_slice_in_dim(inputs[0], half * own_rows, own_rows, 0)
    grad_own = lax.dynamic_slice_in_dim(out_grad[0], half * own_rows, own_rows, 0)
    own_gains = jnp.concatenate([attn_gain, mlp_gain, q_gain, k_gain]).astype(F32)
    own_marks = jnp.concatenate([segment_ids[0], positions[0]])
    gains, marks, input_all, in_weight, out_weight = enter(
        to_tile(own_gains), to_tile(own_marks), input_own, w_query, w_key, w_value, w_out.T
    )
    out_weight = [out_weight[t * width : (t + 1) * width] for t in range(tensors)]
    gains = gains.reshape(gains.shape[0], -1)
    attn_scale = gains[:, :piece].reshape(-1)
    mlp_scale = gains[:, piece : 2 * piece].reshape(-1)
    query_scale = gains[:, 2 * piece : 2 * piece + small].reshape(-1)
    key_scale = gains[:, 2 * piece + small : 2 * (piece + small)].reshape(-1)

    late_gate, late_up, late_down, in_weight = lax.optimization_barrier(
        (w_gate, w_up, w_down, in_weight)
    )
    mlp_shards = jnp.stack([late_gate, late_up, late_down.T])
    mlp_shards = mlp_shards.reshape(3, -1, count, w_gate.shape[1] // count)
    mlp_pieces = [
        shift(
            lax.dynamic_index_in_dim(mlp_shards, (rank + d) % count, 2, keepdims=False), CTX, d
        )
        if d
        else lax.dynamic_index_in_dim(mlp_shards, rank, 2, keepdims=False)
        for d in range(count)
    ]

    own_segs = lax.dynamic_index_in_dim(marks, half, 1, keepdims=False).reshape(rows)
    twin_segs = lax.dynamic_index_in_dim(marks, 1 - half, 1, keepdims=False).reshape(rows)
    own_positions = lax.dynamic_index_in_dim(marks, 2 + half, 1, keepdims=False).reshape(rows)
    order = jnp.arange(rows, dtype=jnp.int32)
    order = order // own_rows * tok_count + order % own_rows
    own_index, twin_index = order + half * own_rows, order + (1 - half) * own_rows
    token_marks = (
        own_segs[:, None],
        own_index[:, None],
        jnp.stack([own_segs, twin_segs]),
        jnp.stack([own_index, twin_index]),
    )
    cosine_table, sine_table = rope_tables(own_positions, HEAD_DIM)
    cosine_table = jnp.concatenate([cosine_table, cosine_table], axis=1)
    sine_table = jnp.concatenate([-sine_table, sine_table], axis=1)
    head_gains = (query_scale[None], key_scale[None])

    stream = input_own.astype(F32)
    input_all = lax.dynamic_update_index_in_dim(input_all, input_own, rank, 0)
    _, attn_norm_pullback = jax.vjp(rms_norm, stream, attn_scale)
    normed_low, raw, query_low, kv_own = qkv_forward(
        input_all, attn_scale[None], in_weight, cosine_table, sine_table, *head_gains
    )
    kv_twin = shift(kv_own, TENSOR, 1)
    attended_low = attend(query_low, kv_own, kv_twin, token_marks)
    attended_own = swap_ctx(attended_low.reshape(count, own_rows, tensors * q_cols), 3)
    attended_own = attended_own.reshape(count, own_rows, tensors, q_cols)
    attended_own = attended_own.transpose(1, 2, 0, 3).reshape(own_rows, tensors, head_rows)
    middle = stream
    for t in range(tensors):
        middle = middle + jnp.dot(
            attended_own[:, t], out_weight[t].T, preferred_element_type=F32
        )
    normed_mid, mlp_norm_pullback = jax.vjp(rms_norm, middle, mlp_scale)
    mid_own = normed_mid.astype(BF16)
    mid_low, grad_low, gate_weight, up_weight, down_weight = spread_mlp(
        mid_own, grad_own, mlp_pieces
    )
    mid_low = lax.dynamic_update_index_in_dim(mid_low, mid_own, rank, 0).reshape(rows, width)
    grad_low = lax.dynamic_update_index_in_dim(grad_low, grad_own, rank, 0).reshape(rows, width)

    gate = jnp.dot(mid_low, gate_weight, preferred_element_type=F32)
    upward = jnp.dot(mid_low, up_weight, preferred_element_type=F32)
    hidden, silu_pullback = jax.vjp(silu_product, gate, upward)
    hidden_low = hidden.astype(BF16)
    down_weight_part = weight_partials([(grad_low, hidden_low)])
    down_mine = scattered(down_weight_part)
    grad_low, _ = lax.optimization_barrier((grad_low, down_weight_part))
    hidden_grad = jnp.dot(grad_low, down_weight, preferred_element_type=F32)
    gate_grad, upward_grad = silu_pullback(hidden_grad)
    gate_grad_low = gate_grad.astype(BF16)
    upward_grad_low = upward_grad.astype(BF16)
    mid_grad_part = jnp.dot(gate_grad_low, gate_weight.T, preferred_element_type=F32) + jnp.dot(
        upward_grad_low, up_weight.T, preferred_element_type=F32
    )
    mid_grad_part, gate_grad_low, upward_grad_low, hidden_low = lax.optimization_barrier(
        (mid_grad_part.astype(BF16), gate_grad_low, upward_grad_low, hidden_low)
    )
    mid_grad_part = mid_grad_part.reshape(count, own_rows, width)
    arrived = [shift(block_ahead(mid_grad_part, d), CTX, d) for d in range(1, count)]
    arrived[0], gate_grad_low, upward_grad_low = lax.optimization_barrier(
        (arrived[0], gate_grad_low, upward_grad_low)
    )
    gate_up_part = weight_partials([(mid_low, gate_grad_low), (mid_low, upward_grad_low)])
    down_part = jnp.dot(hidden_low, down_weight.T, preferred_element_type=F32).astype(BF16)
    mid_grad = block_ahead(mid_grad_part, 0).astype(F32)
    for block in arrived:
        mid_grad = mid_grad + block.astype(F32)
    mid_grad, down_part, gate_up_part, down_mine = lax.optimization_barrier(
        (mid_grad, down_part, gate_up_part, down_mine)
    )
    gate_up_mine = scattered(gate_up_part)
    ff_cols = w_gate.shape[1] // count

    down_sum = scatter_sum(down_part.reshape(count, own_rows, width))
    middle_norm_grad, mlp_gain_grad = mlp_norm_pullback(mid_grad)
    middle_grad = grad_own.astype(F32) + middle_norm_grad
    branch_grad = middle_grad.astype(BF16)
    attended_grad = jnp.stack(
        [jnp.dot(branch_grad, w, preferred_element_type=F32).astype(BF16) for w in out_weight]
    )
    attended_grad = attended_grad.reshape(tensors, own_rows, count, q_cols).transpose(2, 1, 0, 3)
    attended_grad = swap_ctx(attended_grad.reshape(count, own_rows, tensors * q_cols), 4)
    branch_grad, attended_grad = lax.optimization_barrier((branch_grad, attended_grad))
    branch_all = gather_ctx(branch_grad).reshape(rows, width)
    attended_grad = attended_grad.reshape(rows, tensors * q_cols)
    query_grad, kv_grad, kv_back = attend_back(query_low, kv_own, kv_twin, attended_grad, token_marks)
    kv_back = shift(kv_back, TENSOR, 1)
    raw_grad_low, head_gain_grads = qkv_back(
        raw, query_grad, kv_grad, kv_back, cosine_table, sine_table, *head_gains
    )
    (down_weight_grad,) = shards_of(down_mine, [ff_cols])
    gate_up_got = swap_by_target(gate_up_mine)
    gate_weight_grad, up_weight_grad = parts_of(gate_up_got, [ff_cols, ff_cols])
    down_weight_grad = down_weight_grad.T
    output = with_twin((middle + down_sum).astype(BF16))[None]
    early = (output, branch_all, down_weight_grad, gate_weight_grad, up_weight_grad)
    raw_grad_low, early = lax.optimization_barrier((raw_grad_low, early))
    output, branch_all, down_weight_grad, gate_weight_grad, up_weight_grad = early
    normed_grad_part = jnp.dot(raw_grad_low, in_weight.T, preferred_element_type=F32)
    attn_part = weight_partials([(normed_low, raw_grad_low), (branch_all, attended_low)])
    normed_grad, attn_got = sum_tail(
        normed_grad_part.astype(BF16).reshape(count, own_rows, width), attn_part
    )
    normed_grad = sum(normed_grad[i].astype(F32) for i in range(count))
    in_weight_grad, out_weight_grad = parts_of(attn_got, [in_width, q_cols])
    in_weight_grad = in_weight_grad.reshape(-1, count, in_width)
    query_weight_grad = in_weight_grad[..., :q_cols].reshape(w_query.shape)
    key_weight_grad = in_weight_grad[..., q_cols : q_cols + k_cols].reshape(w_key.shape)
    value_weight_grad = in_weight_grad[..., q_cols + k_cols :].reshape(w_value.shape)
    stream_norm_grad, attn_gain_grad = attn_norm_pullback(normed_grad)
    gain_grads = jnp.concatenate(
        [
            attn_gain_grad.reshape(-1, piece),
            mlp_gain_grad.reshape(-1, piece),
            head_gain_grads[0].reshape(-1, small),
            head_gain_grads[1].reshape(-1, small),
        ],
        axis=1,
    )
    gain_grads = owner_sums(jax.vmap(to_tile)(gain_grads)).reshape(-1)
    input_grad = with_twin((middle_grad + stream_norm_grad).astype(BF16))[None]
    return (
        output,
        input_grad,
        gain_grads[:piece],
        query_weight_grad,
        key_weight_grad,
        value_weight_grad,
        gain_grads[2 * piece : 2 * piece + small],
        gain_grads[2 * piece + small : 2 * (piece + small)],
        out_weight_grad.T,
        gain_grads[piece : 2 * piece],
        gate_weight_grad,
        up_weight_grad,
        down_weight_grad,
    )


def can_slice(mesh, inputs, w_query, w_key, w_gate):
    tensors, count = mesh.shape[TENSOR], mesh.shape[CTX]
    return (
        (mesh.shape[DP], count, tensors) == (4, 4, 2)
        and inputs.shape[0] == mesh.shape[DP]
        and inputs.shape[1] == count * tensors * TILE[1]
        and w_key.shape[1] == tensors * count * HEAD_DIM
        and w_query.shape[1] == 2 * w_key.shape[1]
        and w_gate.shape[1] % (tensors * count * 128) == 0
    )


def on_device(
    inputs,
    segment_ids,
    positions,
    out_grad,
    attn_gain,
    w_query,
    w_key,
    w_value,
    q_gain,
    k_gain,
    w_out,
    mlp_gain,
    w_gate,
    w_up,
    w_down,
):
    seq_count, tok_count, width = inputs.shape
    row_count = seq_count * tok_count
    cycle_size = lax.axis_size(CTX)
    cycle_rank = lax.axis_index(CTX)
    gathered_attn = (
        lax.all_gather(w_query, (DP, CTX), axis=0, tiled=True),
        lax.all_gather(w_key, (DP, CTX), axis=0, tiled=True),
        lax.all_gather(w_value, (DP, CTX), axis=0, tiled=True),
        lax.all_gather(w_out, (DP, CTX), axis=1, tiled=True),
        lax.all_gather(attn_gain, (DP, CTX), axis=0, tiled=True),
        lax.all_gather(q_gain, (DP, CTX), axis=0, tiled=True),
        lax.all_gather(k_gain, (DP, CTX), axis=0, tiled=True),
    )
    query_weight, key_weight, value_weight, out_weight, attn_scale, query_scale, key_scale = (
        gathered_attn
    )
    gathered_mlp = (
        lax.all_gather(w_gate, (DP, CTX), axis=0, tiled=True),
        lax.all_gather(w_up, (DP, CTX), axis=0, tiled=True),
        lax.all_gather(w_down, (DP, CTX), axis=1, tiled=True),
        lax.all_gather(mlp_gain, (DP, CTX), axis=0, tiled=True),
    )
    gate_weight, up_weight, down_weight, mlp_scale = gathered_mlp
    segments_all = lax.all_gather(segment_ids, CTX, axis=1, tiled=True)
    local_heads = query_weight.shape[1] // HEAD_DIM
    local_kv = key_weight.shape[1] // HEAD_DIM
    group_size = local_heads // local_kv
    kv_width = local_kv * HEAD_DIM
    score_scale = 1.0 / math.sqrt(HEAD_DIM)
    stream = inputs.astype(jnp.float32).reshape(row_count, width)
    normed_attn, attn_norm_pullback = jax.vjp(rms_norm, stream, attn_scale.astype(jnp.float32))
    normed_low = normed_attn.astype(jnp.bfloat16)
    query_raw = jnp.dot(normed_low, query_weight, preferred_element_type=jnp.float32).reshape(
        seq_count, tok_count, local_heads, HEAD_DIM
    )
    key_raw = jnp.dot(normed_low, key_weight, preferred_element_type=jnp.float32).reshape(
        seq_count, tok_count, local_kv, HEAD_DIM
    )
    value_low = (
        jnp.dot(normed_low, value_weight, preferred_element_type=jnp.float32)
        .astype(jnp.bfloat16)
        .reshape(seq_count, tok_count, kv_width)
    )
    cosine_table, sine_table = rope_tables(positions, HEAD_DIM)
    cosine_table = cosine_table[:, :, None, :]
    sine_table = sine_table[:, :, None, :]

    def norm_rope(raw_heads, gain_vector):
        return head_norm(raw_heads, gain_vector, cosine_table, sine_table)

    query_rot, query_pullback = jax.vjp(norm_rope, query_raw, query_scale.astype(jnp.float32))
    key_rot, key_pullback = jax.vjp(norm_rope, key_raw, key_scale.astype(jnp.float32))
    query_low = query_rot.astype(jnp.bfloat16).reshape(
        seq_count, tok_count, local_kv, group_size, HEAD_DIM
    )
    key_low = key_rot.astype(jnp.bfloat16).reshape(seq_count, tok_count, kv_width)
    query_index = cycle_rank * tok_count + jnp.arange(tok_count, dtype=jnp.int32)

    def block_scores(key_block, first_row):
        key_count = key_block.shape[1]
        key_heads = key_block.reshape(seq_count, key_count, local_kv, HEAD_DIM)
        raw_scores = (
            jnp.einsum(
                "stkgd,snkd->skgtn", query_low, key_heads, preferred_element_type=jnp.float32
            )
            * score_scale
        )
        key_index = first_row + jnp.arange(key_count, dtype=jnp.int32)
        key_segments = lax.dynamic_slice_in_dim(segments_all, first_row, key_count, 1)
        allowed = (key_index[None, None, :] <= query_index[None, :, None]) & (
            key_segments[:, None, :] == segment_ids[:, :, None]
        )
        return (raw_scores, allowed[:, None, None, :, :])

    stat_shape = (seq_count, local_kv, group_size, tok_count)
    pieces = (
        lax.all_gather(key_low, CTX, axis=1, tiled=True),
        lax.all_gather(value_low, CTX, axis=1, tiled=True),
    )
    row_best = jnp.full(stat_shape, masked_value, jnp.float32)
    raw_scores, allowed = block_scores(pieces[0], jnp.int32(0))
    masked = jnp.where(allowed, raw_scores, masked_value)
    new_best = jnp.maximum(row_best, jnp.max(masked, axis=-1))
    weights = jnp.where(allowed, jnp.exp(masked - new_best[..., None]), 0.0)
    value_heads = pieces[1].reshape(seq_count, pieces[1].shape[1], local_kv, HEAD_DIM)
    added = jnp.einsum(
        "skgtn,snkd->skgtd",
        weights.astype(jnp.bfloat16),
        value_heads,
        preferred_element_type=jnp.float32,
    )
    row_total = jnp.sum(weights, axis=-1)
    log_total = new_best + jnp.log(row_total)
    attended = added / row_total[..., None]
    attended_low = (
        jnp.transpose(attended, (0, 3, 1, 2, 4))
        .reshape(row_count, local_heads * HEAD_DIM)
        .astype(jnp.bfloat16)
    )
    attn_part = jnp.dot(attended_low, out_weight, preferred_element_type=jnp.float32)
    middle = stream + lax.psum(attn_part.astype(jnp.bfloat16), TENSOR).astype(jnp.float32)
    normed_mid, mlp_norm_pullback = jax.vjp(rms_norm, middle, mlp_scale.astype(jnp.float32))
    mid_low = normed_mid.astype(jnp.bfloat16)
    gate = jnp.dot(mid_low, gate_weight, preferred_element_type=jnp.float32)
    upward = jnp.dot(mid_low, up_weight, preferred_element_type=jnp.float32)
    hidden, silu_pullback = jax.vjp(silu_product, gate, upward)
    hidden_low = hidden.astype(jnp.bfloat16)
    down_part = jnp.dot(hidden_low, down_weight, preferred_element_type=jnp.float32)
    down_sum = lax.psum(down_part.astype(jnp.bfloat16), TENSOR).astype(jnp.float32)
    output = (middle + down_sum).astype(jnp.bfloat16).reshape(seq_count, tok_count, width)
    grad_low = out_grad.reshape(row_count, width)
    down_weight_grad = jnp.dot(hidden_low.T, grad_low, preferred_element_type=jnp.float32)
    hidden_grad = jnp.dot(grad_low, down_weight.T, preferred_element_type=jnp.float32)
    gate_grad, upward_grad = silu_pullback(hidden_grad)
    gate_grad_low = gate_grad.astype(jnp.bfloat16)
    upward_grad_low = upward_grad.astype(jnp.bfloat16)
    gate_weight_grad = jnp.dot(mid_low.T, gate_grad_low, preferred_element_type=jnp.float32)
    up_weight_grad = jnp.dot(mid_low.T, upward_grad_low, preferred_element_type=jnp.float32)
    mid_grad_part = jnp.dot(
        gate_grad_low, gate_weight.T, preferred_element_type=jnp.float32
    ) + jnp.dot(upward_grad_low, up_weight.T, preferred_element_type=jnp.float32)
    mid_grad = lax.psum(mid_grad_part.astype(jnp.bfloat16), TENSOR).astype(jnp.float32)
    middle_norm_grad, mlp_gain_grad = mlp_norm_pullback(mid_grad)
    middle_grad = grad_low.astype(jnp.float32) + middle_norm_grad
    mlp_grads = (
        lax.psum_scatter(gate_weight_grad, (DP, CTX), scatter_dimension=0, tiled=True),
        lax.psum_scatter(up_weight_grad, (DP, CTX), scatter_dimension=0, tiled=True),
        lax.psum_scatter(down_weight_grad, (DP, CTX), scatter_dimension=1, tiled=True),
        lax.psum_scatter(mlp_gain_grad, (DP, CTX), scatter_dimension=0, tiled=True),
    )
    branch_grad = middle_grad.astype(jnp.bfloat16)
    out_weight_grad = jnp.dot(attended_low.T, branch_grad, preferred_element_type=jnp.float32)
    attended_grad = jnp.dot(branch_grad, out_weight.T, preferred_element_type=jnp.float32).astype(
        jnp.bfloat16
    )
    attended_grad_heads = jnp.transpose(
        attended_grad.reshape(seq_count, tok_count, local_kv, group_size, HEAD_DIM), (0, 2, 3, 1, 4)
    )
    row_delta = jnp.sum(attended_grad_heads.astype(jnp.float32) * attended, axis=-1)

    def key_block_grads(key_block, value_block, first_row):
        raw_scores, allowed = block_scores(key_block, first_row)
        probability = jnp.where(allowed, jnp.exp(raw_scores - log_total[..., None]), 0.0)
        key_count = key_block.shape[1]
        value_heads = value_block.reshape(seq_count, key_count, local_kv, HEAD_DIM)
        key_heads = key_block.reshape(seq_count, key_count, local_kv, HEAD_DIM)
        prob_grad = jnp.einsum(
            "skgtd,snkd->skgtn",
            attended_grad_heads,
            value_heads,
            preferred_element_type=jnp.float32,
        )
        score_grad = (probability * (prob_grad - row_delta[..., None])).astype(jnp.bfloat16)
        query_add = jnp.einsum(
            "skgtn,snkd->skgtd", score_grad, key_heads, preferred_element_type=jnp.float32
        )
        key_add = jnp.einsum(
            "skgtn,stkgd->snkd", score_grad, query_low, preferred_element_type=jnp.float32
        ).reshape(seq_count, key_count, kv_width)
        value_add = jnp.einsum(
            "skgtn,skgtd->snkd",
            probability.astype(jnp.bfloat16),
            attended_grad_heads,
            preferred_element_type=jnp.float32,
        ).reshape(seq_count, key_count, kv_width)
        return (query_add, key_add, value_add)

    query_zero = jnp.zeros(stat_shape + (HEAD_DIM,), jnp.float32)
    kv_zero = jnp.zeros((seq_count, tok_count, kv_width), jnp.float32)

    def cycle_turn(turn_index, state):
        key_block, value_block, key_grad_acc, value_grad_acc, query_grad_acc = state
        owner_rank = (cycle_rank + turn_index) % cycle_size
        query_add, key_add, value_add = key_block_grads(
            key_block, value_block, owner_rank * tok_count
        )
        moved_blocks = from_behind((key_block, value_block), CTX, -1)
        moved_grads = (
            from_behind((key_grad_acc + key_add).astype(jnp.bfloat16), CTX, -1).astype(
                jnp.float32
            ),
            from_behind((value_grad_acc + value_add).astype(jnp.bfloat16), CTX, -1).astype(
                jnp.float32
            ),
        )
        return (
            moved_blocks[0],
            moved_blocks[1],
            moved_grads[0],
            moved_grads[1],
            query_grad_acc + query_add,
        )

    final_state = lax.fori_loop(
        0, cycle_size, cycle_turn, (key_low, value_low, kv_zero, kv_zero, query_zero)
    )
    key_grad_sum = final_state[2]
    value_grad_sum = final_state[3]
    query_grad_sum = final_state[4]
    query_grad = (
        jnp.transpose(query_grad_sum, (0, 3, 1, 2, 4)).reshape(
            seq_count, tok_count, local_heads, HEAD_DIM
        )
        * score_scale
    )
    query_raw_grad, query_gain_grad = query_pullback(query_grad)
    key_raw_grad, key_gain_grad = key_pullback(
        (key_grad_sum * score_scale).reshape(seq_count, tok_count, local_kv, HEAD_DIM)
    )
    query_grad_low = query_raw_grad.reshape(row_count, local_heads * HEAD_DIM).astype(jnp.bfloat16)
    key_grad_low = key_raw_grad.reshape(row_count, kv_width).astype(jnp.bfloat16)
    value_grad_low = value_grad_sum.reshape(row_count, kv_width).astype(jnp.bfloat16)
    query_weight_grad = jnp.dot(normed_low.T, query_grad_low, preferred_element_type=jnp.float32)
    key_weight_grad = jnp.dot(normed_low.T, key_grad_low, preferred_element_type=jnp.float32)
    value_weight_grad = jnp.dot(normed_low.T, value_grad_low, preferred_element_type=jnp.float32)
    normed_grad_part = (
        jnp.dot(query_grad_low, query_weight.T, preferred_element_type=jnp.float32)
        + jnp.dot(key_grad_low, key_weight.T, preferred_element_type=jnp.float32)
        + jnp.dot(value_grad_low, value_weight.T, preferred_element_type=jnp.float32)
    )
    normed_grad, query_gain_total, key_gain_total = (
        lax.psum(normed_grad_part.astype(jnp.bfloat16), TENSOR).astype(jnp.float32),
        lax.psum(query_gain_grad.astype(jnp.bfloat16), TENSOR).astype(jnp.float32),
        lax.psum(key_gain_grad.astype(jnp.bfloat16), TENSOR).astype(jnp.float32),
    )
    stream_norm_grad, attn_gain_grad = attn_norm_pullback(normed_grad)
    input_grad = (
        (middle_grad + stream_norm_grad).astype(jnp.bfloat16).reshape(seq_count, tok_count, width)
    )
    attn_grads = (
        lax.psum_scatter(query_weight_grad, (DP, CTX), scatter_dimension=0, tiled=True),
        lax.psum_scatter(key_weight_grad, (DP, CTX), scatter_dimension=0, tiled=True),
        lax.psum_scatter(value_weight_grad, (DP, CTX), scatter_dimension=0, tiled=True),
        lax.psum_scatter(out_weight_grad, (DP, CTX), scatter_dimension=1, tiled=True),
        lax.psum_scatter(attn_gain_grad, (DP, CTX), scatter_dimension=0, tiled=True),
        lax.psum_scatter(query_gain_total, (DP, CTX), scatter_dimension=0, tiled=True),
        lax.psum_scatter(key_gain_total, (DP, CTX), scatter_dimension=0, tiled=True),
    )
    return (
        output,
        input_grad,
        attn_grads[4],
        attn_grads[0],
        attn_grads[1],
        attn_grads[2],
        attn_grads[5],
        attn_grads[6],
        attn_grads[3],
        mlp_grads[3],
        mlp_grads[0],
        mlp_grads[1],
        mlp_grads[2],
    )


def solution(mesh):
    in_specs = (
        P(DP, CTX, None),
        P(DP, CTX),
        P(DP, CTX),
        P(DP, CTX, None),
        P((DP, CTX)),
        P((DP, CTX), TENSOR),
        P((DP, CTX), TENSOR),
        P((DP, CTX), TENSOR),
        P((DP, CTX)),
        P((DP, CTX)),
        P(TENSOR, (DP, CTX)),
        P((DP, CTX)),
        P((DP, CTX), TENSOR),
        P((DP, CTX), TENSOR),
        P(TENSOR, (DP, CTX)),
    )
    out_specs = (
        P(DP, CTX, None),
        P(DP, CTX, None),
        P((DP, CTX)),
        P((DP, CTX), TENSOR),
        P((DP, CTX), TENSOR),
        P((DP, CTX), TENSOR),
        P((DP, CTX)),
        P((DP, CTX)),
        P(TENSOR, (DP, CTX)),
        P((DP, CTX)),
        P((DP, CTX), TENSOR),
        P((DP, CTX), TENSOR),
        P(TENSOR, (DP, CTX)),
    )

    def step(*args):
        body = on_device_sliced if can_slice(mesh, args[0], args[5], args[6], args[12]) else on_device
        return jax.shard_map(
            body, mesh=mesh, in_specs=in_specs, out_specs=out_specs, check_vma=False
        )(*args)

    return step
```

```python
import math
from types import SimpleNamespace

import jax
import jax.numpy as jnp
from jax import lax
from jax.experimental import pallas as pl
from jax.experimental.pallas import tpu as pltpu
from jax.sharding import PartitionSpec as P


HEAD_DIM = 128
BF16 = jnp.bfloat16
F32 = jnp.float32
MESH = pl.DeviceIdType.MESH
TILE = (8, 128)
DP, CTX, TENSOR = "dp", "ctx", "tensor"

epsilon = 1e-06
rope_base = 1000000.0
masked_value = -1e30


def from_behind(value, axis, steps):
    count = lax.axis_size(axis)
    pairs = [(source, (source + steps) % count) for source in range(count)]
    return lax.ppermute(value, axis, pairs)


def rope_tables(positions, head_size):
    half_dim = head_size // 2
    frequency = rope_base ** (-(jnp.arange(half_dim, dtype=jnp.float32) * 2.0) / head_size)
    angles = positions.astype(jnp.float32)[..., None] * frequency
    return (jnp.cos(angles), jnp.sin(angles))


def rotate(values, cosine_table, sine_table):
    half_dim = values.shape[-1] // 2
    first_half = values[..., :half_dim]
    second_half = values[..., half_dim:]
    return jnp.concatenate(
        [
            first_half * cosine_table - second_half * sine_table,
            second_half * cosine_table + first_half * sine_table,
        ],
        axis=-1,
    )


def head_norm(raw_heads, gain_vector, cosine_table, sine_table):
    scaled = (
        raw_heads
        * lax.rsqrt(jnp.mean(raw_heads * raw_heads, axis=-1, keepdims=True) + epsilon)
        * gain_vector
    )
    return rotate(scaled, cosine_table, sine_table)


def rms_norm(stream, gain_vector):
    return (
        stream
        * lax.rsqrt(jnp.mean(stream * stream, axis=-1, keepdims=True) + epsilon)
        * gain_vector
    )


def silu_product(gate, upward):
    return jax.nn.silu(gate) * upward


def shift(value, axis, steps):
    count = lax.axis_size(axis)
    pairs = [(source, (source + steps) % count) for source in range(count)]
    return lax.ppermute(value, axis, pairs)


def take_ring(blocks, first):
    return lax.dynamic_slice_in_dim(jnp.concatenate([blocks, blocks]), first, blocks.shape[0], 0)


def block_ahead(blocks, steps):
    count = lax.axis_size(CTX)
    place = (lax.axis_index(CTX) + steps) % count
    return lax.dynamic_index_in_dim(blocks, place, 0, keepdims=False)


def scatter_sum(blocks):
    total = block_ahead(blocks, 0).astype(F32)
    for d in range(1, blocks.shape[0]):
        total = total + shift(block_ahead(blocks, d), CTX, d).astype(F32)
    return total


def swap_ahead(blocks):
    count = lax.axis_size(CTX)
    return [block_ahead(blocks, 0)] + [
        shift(block_ahead(blocks, d), CTX, d) for d in range(1, count)
    ]


def rows_of(got):
    count, rank = len(got), lax.axis_index(CTX)
    size = got[0].shape[0]
    whole_rows = jnp.zeros((count * size, got[0].shape[1]), got[0].dtype)
    for d, block in enumerate(got):
        place = (rank - d) % count * size
        whole_rows = lax.dynamic_update_slice_in_dim(whole_rows, block, place, 0)
    return whole_rows


def columns_of(got, widths):
    count, rank = len(got), lax.axis_index(CTX)
    shards, first = [], 0
    for width in widths:
        shard = jnp.zeros((got[0].shape[0], count * width), F32)
        for d, block in enumerate(got):
            part = block[:, first : first + width].astype(F32)
            shard = lax.dynamic_update_slice_in_dim(shard, part, (rank - d) % count * width, 1)
        shards.append(shard)
        first += width
    return shards


def greet(peers):
    barrier = pltpu.get_barrier_semaphore()
    for peer in peers:
        pl.semaphore_signal(barrier, inc=1, device_id=peer, device_id_type=MESH)
    pl.semaphore_wait(barrier, len(peers))


def remote(source, target, send_sem, recv_sem, peer):
    copy = pltpu.make_async_remote_copy(
        src_ref=source,
        dst_ref=target,
        send_sem=send_sem,
        recv_sem=recv_sem,
        device_id=peer,
        device_id_type=MESH,
    )
    copy.start()
    return copy


def to_tile(values):
    return jnp.pad(values, (0, math.prod(TILE) - values.shape[0])).reshape(TILE)


def place():
    pair, rank, half = lax.axis_index(DP), lax.axis_index(CTX), lax.axis_index(TENSOR)
    core = lax.rem(pair, 2)
    return SimpleNamespace(
        pair=pair,
        rank=rank,
        half=half,
        sibling=pair + 1 - 2 * core,
        across=lax.rem(pair + 2, 4),
        twin=1 - half,
    )


class Relay:
    KINDS = 9

    def __init__(self, here, source, view, rows, send_sem, recv_sem):
        self.here, self.source, self.view, self.rows = here, source, view, rows
        self.send_sem, self.recv_sem = send_sem, recv_sem
        self.copies = {}

    def go(self, kind, source, target, peer):
        self.copies[kind] = remote(
            source, target, self.send_sem.at[kind], self.recv_sem.at[kind], peer
        )

    def first(self):
        p = self.here
        target = self.view(p.half, p.pair, 0, self.rows)
        self.go(1, self.source, target, {DP: p.across})
        self.go(2, self.source, target, {TENSOR: p.twin})
        self.go(0, self.source, target, {DP: p.sibling})

    def second(self):
        p, part = self.here, self.rows // 2
        self.copies[1].wait_recv()
        low = self.view(p.half, p.across, 0, part)
        self.go(4, low, low, {TENSOR: p.twin})
        whole = self.view(p.half, p.across, 0, self.rows)
        self.go(3, whole, whole, {DP: p.sibling})
        self.copies[2].wait_recv()
        high = self.view(p.twin, p.pair, part, part)
        self.go(6, high, high, {DP: p.across})
        whole = self.view(p.twin, p.pair, 0, self.rows)
        self.go(5, whole, whole, {DP: p.sibling})

    def third(self):
        p, part = self.here, self.rows // 2
        self.copies[4].wait_recv()
        low = self.view(p.twin, p.across, 0, part)
        self.go(7, low, low, {DP: p.sibling})
        self.copies[6].wait_recv()
        high = self.view(p.twin, p.across, part, part)
        self.go(8, high, high, {DP: p.sibling})

    def last(self):
        for kind in (0, 3, 5, 7, 8):
            self.copies[kind].wait_recv()
        for copy in self.copies.values():
            copy.wait_send()


class Chain:
    def __init__(self, rank, count, source, spot, send_sem, recv_sem):
        self.rank, self.count, self.source, self.spot = rank, count, source, spot
        self.send_sem, self.recv_sem = send_sem, recv_sem

    def copy(self, way, step):
        step_to = self.rank + (1 if way == 0 else -1)
        owner = self.rank - step if way == 0 else self.rank + step
        owner = jnp.clip(owner, 0, self.count - 1)
        return pltpu.make_async_remote_copy(
            src_ref=self.source if step == 0 else self.spot(owner),
            dst_ref=self.spot(owner),
            send_sem=self.send_sem.at[way, step],
            recv_sem=self.recv_sem.at[way, step],
            device_id={CTX: jnp.clip(step_to, 0, self.count - 1)},
            device_id_type=MESH,
        )

    def sends(self, way, step):
        if way == 0:
            return (self.rank >= step) & (self.rank < self.count - 1)
        return (self.rank + step < self.count) & (self.rank > 0)

    def receives(self, way, step):
        return self.rank > step if way == 0 else self.rank + step < self.count - 1

    def start(self, step):
        for way in (0, 1):
            if step > 0:

                @pl.when(self.receives(way, step - 1))
                def _():
                    self.copy(way, step - 1).wait_recv()

            @pl.when(self.sends(way, step))
            def _():
                self.copy(way, step).start()

    def arrive(self):
        last = self.count - 2
        for way in (0, 1):

            @pl.when(self.receives(way, last))
            def _():
                self.copy(way, last).wait_recv()

    def drain(self):
        for way in (0, 1):
            for step in range(self.count - 1):

                @pl.when(self.sends(way, step))
                def _():
                    self.copy(way, step).wait_send()


SEMS = pltpu.SemaphoreType.DMA
ANYWHERE = pl.BlockSpec(memory_space=pl.ANY)
ON_CHIP = pl.BlockSpec(memory_space=pltpu.VMEM)


def enter(gains, marks, block, w_query, w_key, w_value, out_shard):
    count, pairs = lax.axis_size(CTX), lax.axis_size(DP)
    owners = count * pairs
    depth = w_query.shape[0]
    widths = [w.shape[1] // count for w in (w_query, w_key, w_value)]
    width = sum(widths)
    spots = [sum(widths[:i]) for i in range(3)]
    rows = block.shape[0]

    def kernel(
        gain_ref, mark_ref, block_ref, wq_ref, wk_ref, wv_ref, wo_ref,
        gains_ref, marks_ref, rows_ref, weight_ref, out_ref,
        held, held_out, out_send, out_recv, out_relay_send, out_relay_recv, gain_send, gain_recv, mark_send, mark_recv,
        swap_send, swap_recv, chain_send, chain_recv, relay_send, relay_recv, local_sem,
    ):
        here = place()
        rank, pair, half = here.rank, here.pair, here.half
        me = pair * count + rank
        far = [lax.rem(me + k, owners) for k in range(1, owners)]
        far = [{DP: lax.div(t, count), CTX: lax.rem(t, count)} for t in far]
        near = [{CTX: lax.rem(rank + k, count)} for k in range(1, count)]
        greet(far + [{TENSOR: here.twin}])

        def view(owner_rank):
            def at(t, p, start, size):
                first = pl.multiple_of((p * count + owner_rank) * depth + start, 64)
                return weight_ref.at[pl.ds(first, size), pl.ds(pl.multiple_of(t * width, 128), width)]

            return at

        def out_view(owner_rank):
            def at(t, p, start, size):
                first = t * owners * depth + (p * count + owner_rank) * depth + start
                return out_ref.at[pl.ds(pl.multiple_of(first, 64), size)]

            return at

        def columns(ref, i, target):
            return ref.at[:, pl.ds(pl.multiple_of(target * widths[i], 128), widths[i])]

        sources = (wq_ref, wk_ref, wv_ref)
        takes = [
            pltpu.make_async_copy(
                columns(ref, i, rank), held.at[:, pl.ds(spots[i], widths[i])], local_sem.at[i]
            )
            for i, ref in enumerate(sources)
        ]
        takes.append(pltpu.make_async_copy(wo_ref, held_out, local_sem.at[4]))
        for take in takes:
            take.start()
        small = [
            remote(mark_ref, marks_ref.at[rank], mark_send.at[k], mark_recv.at[k], peer)
            for k, peer in enumerate(near)
        ]
        small += [
            remote(gain_ref, gains_ref.at[me], gain_send.at[k], gain_recv.at[k], peer)
            for k, peer in enumerate(far)
        ]
        own_rows = pl.ds(pl.multiple_of(me * depth, depth), depth)
        swaps = []
        for k, peer in enumerate(near):
            swaps.append([])
            for i, ref in enumerate(sources):
                spot = pl.ds(pl.multiple_of(half * width + spots[i], 128), widths[i])
                swaps[k].append(
                    remote(
                        columns(ref, i, peer[CTX]),
                        weight_ref.at[own_rows, spot],
                        swap_send.at[k, i],
                        swap_recv.at[k, i],
                        peer,
                    )
                )
                out_own = out_view(rank)(half, pair, 0, depth)
        out_chain = Chain(
            rank, count, wo_ref, lambda o: out_view(o)(half, pair, 0, depth), out_send, out_recv
        )
        out_chain.start(0)
        chain = Chain(rank, count, block_ref, lambda o: rows_ref.at[o], chain_send, chain_recv)
        gains_ref[me] = gain_ref[...]
        marks_ref[rank] = mark_ref[...]
        for take in takes:
            take.wait()
        keep = pltpu.make_async_copy(held, view(rank)(half, pair, 0, depth), local_sem.at[3])
        keep.start()
        keep_out = pltpu.make_async_copy(held_out, out_own, local_sem.at[5])
        keep_out.start()
        relays = [Relay(here, held, view(rank), depth, relay_send.at[0], relay_recv.at[0])]
        relays[0].first()
        for k in range(1, count):
            owner = lax.rem(rank - k + count, count)
            for swap in swaps[k - 1]:
                swap.wait_recv()
            at = view(owner)
            relays.append(
                Relay(here, at(half, pair, 0, depth), at, depth, relay_send.at[k], relay_recv.at[k])
            )
            relays[k].first()
        out_chain.start(1)
        out_chain.start(2)
        chain.start(0)
        for relay in relays:
            relay.second()
        for relay in relays:
            relay.third()
        keep_out.wait()
        out_chain.arrive()
        at = out_view(0)
        relays.append(
            Relay(
                here, at(half, pair, 0, count * depth), at, count * depth,
                out_relay_send, out_relay_recv,
            )
        )
        relays[-1].first()
        chain.start(1)
        relays[-1].second()
        chain.start(2)
        relays[-1].third()
        for relay in relays:
            relay.last()
        keep.wait()
        chain.arrive()
        chain.drain()
        out_chain.drain()
        for swap in swaps:
            for copy in swap:
                copy.wait_send()
        for copy in small:
            copy.wait()

    return pl.pallas_call(
        kernel,
        out_shape=(
            jax.ShapeDtypeStruct((owners, *TILE), F32),
            jax.ShapeDtypeStruct((count, *TILE), jnp.int32),
            jax.ShapeDtypeStruct((count, rows, block.shape[1]), block.dtype),
            jax.ShapeDtypeStruct((owners * depth, 2 * width), w_query.dtype),
            jax.ShapeDtypeStruct((2 * owners * depth, out_shard.shape[1]), out_shard.dtype),
        ),
        in_specs=[ON_CHIP] * 2 + [ANYWHERE] * 5,
        out_specs=(ON_CHIP, ON_CHIP, ANYWHERE, ANYWHERE, ANYWHERE),
        scratch_shapes=[
            pltpu.VMEM((depth, width), w_query.dtype),
            pltpu.VMEM(out_shard.shape, out_shard.dtype),
            SEMS((2, count - 1)),
            SEMS((2, count - 1)),
            SEMS((Relay.KINDS,)),
            SEMS((Relay.KINDS,)),
            SEMS((owners - 1,)),
            SEMS((owners - 1,)),
            SEMS((count - 1,)),
            SEMS((count - 1,)),
            SEMS((count - 1, 3)),
            SEMS((count - 1, 3)),
            SEMS((2, count - 1)),
            SEMS((2, count - 1)),
            SEMS((count, Relay.KINDS)),
            SEMS((count, Relay.KINDS)),
            SEMS((6,)),
        ],
        compiler_params=pltpu.CompilerParams(collective_id=0, has_side_effects=True),
        name="enter",
    )(gains, marks, block, w_query, w_key, w_value, out_shard)


def spread_mlp(first, second, pieces):
    count, pairs = lax.axis_size(CTX), lax.axis_size(DP)
    kinds, depth, width = pieces[0].shape
    rows, features = first.shape

    def kernel(first_ref, second_ref, *rest):
        piece_refs, rest = rest[:count], rest[count:]
        firsts_ref, seconds_ref = rest[:2]
        weight_refs, rest = rest[2 : 2 + kinds], rest[2 + kinds :]
        held, chain_send, chain_recv, relay_send, relay_recv, take_sem, keep_sem = rest
        here = place()
        rank, pair, half = here.rank, here.pair, here.half
        greet(
            [{CTX: lax.rem(rank + k, count)} for k in range(1, count)]
            + [{DP: here.sibling}, {DP: here.across}, {TENSOR: here.twin}]
        )
        takes = []
        for i in range(kinds):
            for d, ref in enumerate(piece_refs):
                owner = lax.rem(rank - d + count, count)
                take = pltpu.make_async_copy(
                    ref.at[i],
                    held.at[i, pl.ds(pl.multiple_of(owner * depth, depth), depth)],
                    take_sem.at[i, d],
                )
                take.start()
                takes.append(take)
        chains = [
            Chain(rank, count, first_ref, lambda o: firsts_ref.at[o], chain_send.at[0], chain_recv.at[0]),
            Chain(rank, count, second_ref, lambda o: seconds_ref.at[o], chain_send.at[1], chain_recv.at[1]),
        ]
        chains[0].start(0)
        block = count * depth

        def view(i):
            def at(t, p, start, size):
                first = pl.multiple_of(p * block + start, 64)
                return weight_refs[i].at[
                    pl.ds(first, size), pl.ds(pl.multiple_of(t * width, 128), width)
                ]

            return at

        relays, keeps = [], []
        for i in range(kinds):
            for take in takes[i * count : (i + 1) * count]:
                take.wait()
            keeps.append(
                pltpu.make_async_copy(held.at[i], view(i)(half, pair, 0, block), keep_sem.at[i])
            )
            keeps[i].start()
            relays.append(
                Relay(here, held.at[i], view(i), block, relay_send.at[i], relay_recv.at[i])
            )
            relays[i].first()
        chains[0].start(1)
        relays[0].second()
        chains[0].start(2)
        chains[1].start(0)
        relays[0].third()
        relays[1].second()
        chains[1].start(1)
        relays[1].third()
        chains[1].start(2)
        for relay in relays:
            relay.last()
        for keep in keeps:
            keep.wait()
        for chain in chains:
            chain.arrive()
            chain.drain()

    return pl.pallas_call(
        kernel,
        out_shape=(
            jax.ShapeDtypeStruct((count, rows, features), first.dtype),
            jax.ShapeDtypeStruct((count, rows, features), second.dtype),
        )
        + (jax.ShapeDtypeStruct((pairs * count * depth, 2 * width), pieces[0].dtype),) * kinds,
        in_specs=[ANYWHERE] * (2 + count),
        out_specs=(ANYWHERE,) * (2 + kinds),
        scratch_shapes=[
            pltpu.VMEM((kinds, count * depth, width), pieces[0].dtype),
            SEMS((2, 2, count - 1)),
            SEMS((2, 2, count - 1)),
            SEMS((kinds, Relay.KINDS)),
            SEMS((kinds, Relay.KINDS)),
            SEMS((kinds, count)),
            SEMS((kinds,)),
        ],
        compiler_params=pltpu.CompilerParams(
            collective_id=2, has_side_effects=True, vmem_limit_bytes=16 * 1024 * 1024
        ),
        name="spread_mlp",
    )(first, second, *pieces)


def swap_heads(source, gather, collective_id):
    count = lax.axis_size(CTX)
    tensors = lax.axis_size(TENSOR)
    rows, width = source.shape
    own = rows // count if gather else rows
    part = width // tensors if gather else width // (tensors * count)
    shape = (own, tensors * count * part) if gather else (count * own, tensors * part)

    def kernel(source_ref, got_ref, held, send_sem, recv_sem, local_sem):
        rank = lax.axis_index(CTX)
        peers = [lax.rem(rank + k, count) for k in range(1, count)]
        greet([{CTX: peer} for peer in peers])

        def tall(ref, z, t):
            return ref.at[pl.ds(pl.multiple_of(z * own, own), own), pl.ds(t * part, part)]

        def wide(ref, z, t):
            return ref.at[:, pl.ds(pl.multiple_of((t * count + z) * part, part), part)]

        take, put = (tall, wide) if gather else (wide, tall)
        copies = [
            remote(
                take(source_ref, peer, t),
                put(got_ref, rank, t),
                send_sem.at[k, t],
                recv_sem.at[k, t],
                {CTX: peer},
            )
            for k, peer in enumerate(peers)
            for t in range(tensors)
        ]
        local = [
            pltpu.make_async_copy(take(source_ref, rank, t), held.at[t], local_sem.at[t])
            for t in range(tensors)
        ]
        for copy in local:
            copy.start()
        for copy in local:
            copy.wait()
        local = [
            pltpu.make_async_copy(held.at[t], put(got_ref, rank, t), local_sem.at[tensors + t])
            for t in range(tensors)
        ]
        for copy in local:
            copy.start()
        for copy in local + copies:
            copy.wait()

    return pl.pallas_call(
        kernel,
        out_shape=jax.ShapeDtypeStruct(shape, source.dtype),
        in_specs=[ANYWHERE],
        out_specs=ANYWHERE,
        scratch_shapes=[
            pltpu.VMEM((tensors, own, part), source.dtype),
            SEMS((count - 1, tensors)),
            SEMS((count - 1, tensors)),
            SEMS((2 * tensors,)),
        ],
        compiler_params=pltpu.CompilerParams(collective_id=collective_id, has_side_effects=True),
    )(source)


def sum_tail(blocks, partial):
    count = lax.axis_size(CTX)
    tensors, depth, width = partial.shape
    part = depth // 4
    low = part // 2
    own = part // count
    tile = 64

    def kernel(
        blocks_ref, partial_ref, got_ref, owned_ref,
        held, kept, near, mine, far, near_b, far_b, result,
        send_sem, recv_sem, block_send, block_recv, swap_send, swap_recv, local_sem,
    ):
        here = place()
        rank, pair, half = here.rank, here.pair, here.half
        core, side = lax.rem(pair, 2), lax.div(pair, 2)
        peers = [lax.rem(rank + k, count) for k in range(1, count)]
        greet(
            [{CTX: peer} for peer in peers]
            + [{DP: here.sibling}, {DP: here.across}, {TENSOR: here.twin}]
        )

        def rows_of(t, x, c):
            return partial_ref.at[t, pl.ds(pl.multiple_of((x * 2 + c) * part, part), part)]

        copies = {}
        for t in range(tensors):
            for x in range(2):
                copies[0, t, x] = remote(
                    rows_of(t, x, 1 - core),
                    near.at[t, x],
                    send_sem.at[t * 2 + x],
                    recv_sem.at[t * 2 + x],
                    {DP: here.sibling},
                )
        takes = [
            pltpu.make_async_copy(rows_of(t, x, core), kept.at[t, x], local_sem.at[t * 2 + x])
            for t in range(tensors)
            for x in range(2)
        ]
        for take in takes:
            take.start()
        moves = [
            remote(
                blocks_ref.at[peer], got_ref.at[rank], block_send.at[k], block_recv.at[k], {CTX: peer}
            )
            for k, peer in enumerate(peers)
        ]
        take_own = pltpu.make_async_copy(blocks_ref.at[rank], held, local_sem.at[4])
        take_own.start()

        def add(target, left, right, size):
            @pl.loop(0, size // tile)
            def _(i):
                at = pl.ds(pl.multiple_of(i * tile, tile), tile)
                target[at] = (left[at].astype(F32) + right[at].astype(F32)).astype(BF16)

        for t in range(tensors):
            for x in range(2):
                takes[t * 2 + x].wait()
                copies[0, t, x].wait_recv()
                add(mine.at[t, x], kept.at[t, x], near.at[t, x], part)
        first, second = pl.ds(0, low), pl.ds(low, low)
        for i in range(2):
            copies[1, i] = remote(
                mine.at[here.twin, i, first],
                far.at[i],
                send_sem.at[4 + i],
                recv_sem.at[4 + i],
                {TENSOR: here.twin},
            )
            copies[2, i] = remote(
                mine.at[i, 1 - side, second],
                far_b.at[i],
                send_sem.at[6 + i],
                recv_sem.at[6 + i],
                {DP: here.across},
            )
        for i in range(2):
            copies[1, i].wait_recv()
            add(near.at[0, i], mine.at[half, i, first], far.at[i], low)
            copies[2, i].wait_recv()
            add(near.at[1, i], mine.at[i, side, second], far_b.at[i], low)
        copies[3] = remote(
            near.at[0, 1 - side, first],
            near_b.at[0],
            send_sem.at[8],
            recv_sem.at[8],
            {DP: here.across},
        )
        copies[4] = remote(
            near.at[1, here.twin, first],
            near_b.at[1],
            send_sem.at[9],
            recv_sem.at[9],
            {TENSOR: here.twin},
        )
        take_own.wait()
        keep_own = pltpu.make_async_copy(held, got_ref.at[rank], local_sem.at[5])
        keep_own.start()
        copies[3].wait_recv()
        add(result.at[first], near.at[0, side, first], near_b.at[0], low)
        copies[4].wait_recv()
        add(result.at[second], near.at[1, half, first], near_b.at[1], low)

        def rows_for(target):
            return result.at[pl.ds(pl.multiple_of(target * own, own), own)]

        swaps = [
            remote(
                rows_for(peer), owned_ref.at[rank], swap_send.at[k], swap_recv.at[k], {CTX: peer}
            )
            for k, peer in enumerate(peers)
        ]
        keep = pltpu.make_async_copy(rows_for(rank), owned_ref.at[rank], local_sem.at[6])
        keep.start()
        for copy in swaps + moves:
            copy.wait()
        for copy in copies.values():
            copy.wait_send()
        keep.wait()
        keep_own.wait()

    sixteen = 10
    return pl.pallas_call(
        kernel,
        out_shape=(
            jax.ShapeDtypeStruct(blocks.shape, BF16),
            jax.ShapeDtypeStruct((count, own, width), BF16),
        ),
        in_specs=[ANYWHERE, ANYWHERE],
        out_specs=(ANYWHERE, ANYWHERE),
        scratch_shapes=[
            pltpu.VMEM(blocks.shape[1:], BF16),
            pltpu.VMEM((tensors, 2, part, width), BF16),
            pltpu.VMEM((tensors, 2, part, width), BF16),
            pltpu.VMEM((tensors, 2, part, width), BF16),
            pltpu.VMEM((2, low, width), BF16),
            pltpu.VMEM((2, low, width), BF16),
            pltpu.VMEM((2, low, width), BF16),
            pltpu.VMEM((part, width), BF16),
            SEMS((sixteen,)),
            SEMS((sixteen,)),
            SEMS((count - 1,)),
            SEMS((count - 1,)),
            SEMS((count - 1,)),
            SEMS((count - 1,)),
            SEMS((7,)),
        ],
        compiler_params=pltpu.CompilerParams(
            collective_id=5, has_side_effects=True, vmem_limit_bytes=24 * 1024 * 1024
        ),
        name="sum_tail",
    )(blocks, partial)


def owner_sums(tiles):
    count, pairs, tensors = lax.axis_size(CTX), lax.axis_size(DP), lax.axis_size(TENSOR)
    total = count * pairs * tensors

    def kernel(tiles_ref, sum_ref, got, send_sem, recv_sem):
        owner = lax.axis_index(DP) * count + lax.axis_index(CTX)
        half = lax.axis_index(TENSOR)
        me = owner * tensors + half
        targets = [lax.rem(me + k, total) for k in range(1, total)]
        peers = [
            {
                DP: lax.div(t, count * tensors),
                CTX: lax.rem(lax.div(t, tensors), count),
                TENSOR: lax.rem(t, tensors),
            }
            for t in targets
        ]
        greet(peers)
        copies = [
            remote(
                tiles_ref.at[lax.div(t, tensors)], got.at[me], send_sem.at[k], recv_sem.at[k], peer
            )
            for k, (t, peer) in enumerate(zip(targets, peers))
        ]
        got[me] = tiles_ref[owner]
        for copy in copies:
            copy.wait()
        value = got[0]
        for source in range(1, total):
            value = value + got[source]
        sum_ref[...] = value

    return pl.pallas_call(
        kernel,
        out_shape=jax.ShapeDtypeStruct(TILE, F32),
        in_specs=[ON_CHIP],
        out_specs=ON_CHIP,
        scratch_shapes=[
            pltpu.VMEM((total, *TILE), F32),
            SEMS((total - 1,)),
            SEMS((total - 1,)),
        ],
        compiler_params=pltpu.CompilerParams(collective_id=1, has_side_effects=True),
        name="owner_sums",
    )(tiles)


def whole(shape):
    return pl.BlockSpec(shape, lambda *_: (0,) * len(shape))


def turned(values, cosines, sines):
    return values * cosines + pltpu.roll(values, HEAD_DIM // 2, 1) * sines


def unturned(grads, cosines, sines):
    return grads * cosines + pltpu.roll(grads * sines, HEAD_DIM // 2, 1)


def head_scale(raw):
    return lax.rsqrt(jnp.mean(raw * raw, axis=-1, keepdims=True) + epsilon)


def qkv_forward(blocks, scale, weight, cosines, sines, query_gain, key_gain):
    count, rows, width = blocks.shape
    cols = weight.shape[1]

    def kernel(x_ref, s_ref, w_ref, cos_ref, sin_ref, qg_ref, kg_ref, n_ref, raw_ref, q_ref, kv_ref):
        x = x_ref[0].astype(F32)
        normed = x * lax.rsqrt(jnp.mean(x * x, axis=-1, keepdims=True) + epsilon) * s_ref[...]
        normed = normed.astype(BF16)
        n_ref[...] = normed
        raw = jnp.dot(normed, w_ref[...], preferred_element_type=F32)
        cosine, sine = cos_ref[...], sin_ref[...]
        for head in range(8):
            t, part = head // 4, head % 4
            values = raw[:, head * HEAD_DIM : (head + 1) * HEAD_DIM]
            if part < 3:
                at = (2 * t + part if part < 2 else 4 + t) * HEAD_DIM
                raw_ref[:, at : at + HEAD_DIM] = values
                gain = qg_ref[...] if part < 2 else kg_ref[...]
                values = turned(values * head_scale(values) * gain, cosine, sine)
            if part < 2:
                at = (2 * t + part) * HEAD_DIM
                q_ref[:, at : at + HEAD_DIM] = values.astype(BF16)
            else:
                at = (t if part == 2 else 2 + t) * HEAD_DIM
                kv_ref[:, at : at + HEAD_DIM] = values.astype(BF16)

    def rows_of(size):
        return pl.BlockSpec((rows, size), lambda i: (i, 0))

    total = count * rows
    return pl.pallas_call(
        kernel,
        grid=(count,),
        out_shape=(
            jax.ShapeDtypeStruct((total, width), BF16),
            jax.ShapeDtypeStruct((total, 6 * HEAD_DIM), F32),
            jax.ShapeDtypeStruct((total, 4 * HEAD_DIM), BF16),
            jax.ShapeDtypeStruct((total, 4 * HEAD_DIM), BF16),
        ),
        in_specs=[
            pl.BlockSpec((1, rows, width), lambda i: (i, 0, 0)),
            whole((1, width)),
            whole((width, cols)),
            rows_of(HEAD_DIM),
            rows_of(HEAD_DIM),
            whole((1, HEAD_DIM)),
            whole((1, HEAD_DIM)),
        ],
        out_specs=(rows_of(width), rows_of(6 * HEAD_DIM), rows_of(4 * HEAD_DIM), rows_of(4 * HEAD_DIM)),
        cost_estimate=pl.CostEstimate(
            flops=2 * total * width * cols, bytes_accessed=2 * width * (cols + total), transcendentals=0
        ),
        compiler_params=pltpu.CompilerParams(vmem_limit_bytes=24 * 1024 * 1024),
        name="qkv_forward",
    )(blocks, scale, weight, cosines, sines, query_gain, key_gain)


def probabilities(q, keys, marks):
    seg, index, key_seg, key_index = marks
    scores = []
    for i, key in enumerate(keys):
        s = lax.dot_general(q, key, (((1,), (1,)), ((), ())), preferred_element_type=F32)
        ok = (key_index[i : i + 1] <= index) & (key_seg[i : i + 1] == seg)
        scores.append(jnp.where(ok, s * (1.0 / math.sqrt(HEAD_DIM)), masked_value))
    best = jnp.maximum(*[jnp.max(s, axis=-1, keepdims=True) for s in scores])
    weights = [jnp.exp(s - best) for s in scores]
    total = sum(jnp.sum(w, axis=-1, keepdims=True) for w in weights)
    return [w / total for w in weights]


def key_specs(rows):
    tensors = 2
    specs = []
    for place in (0, tensors):
        specs.append(pl.BlockSpec((rows, HEAD_DIM), lambda t, g, p=place: (0, p + t)))
    return specs * 2


def attend(query, kv_own, kv_twin, marks):
    rows = query.shape[0]

    def kernel(q_ref, k0_ref, v0_ref, k1_ref, v1_ref, *rest):
        marks, out_ref = [ref[...] for ref in rest[:4]], rest[4]
        prob = probabilities(q_ref[...], (k0_ref[...], k1_ref[...]), marks)
        out = jnp.dot(prob[0].astype(BF16), v0_ref[...], preferred_element_type=F32)
        out = out + jnp.dot(prob[1].astype(BF16), v1_ref[...], preferred_element_type=F32)
        out_ref[...] = out.astype(BF16)

    head = pl.BlockSpec((rows, HEAD_DIM), lambda t, g: (0, 2 * t + g))
    return pl.pallas_call(
        kernel,
        grid=(2, 2),
        out_shape=jax.ShapeDtypeStruct(query.shape, BF16),
        in_specs=[head] + key_specs(rows) + [whole(m.shape) for m in marks],
        out_specs=head,
        cost_estimate=pl.CostEstimate(
            flops=32 * rows * rows * HEAD_DIM, bytes_accessed=8 * rows * 512, transcendentals=8 * rows * rows
        ),
        compiler_params=pltpu.CompilerParams(vmem_limit_bytes=32 * 1024 * 1024),
        name="attend",
    )(query, kv_own, kv_own, kv_twin, kv_twin, *marks)


def attend_back(query, kv_own, kv_twin, grad, marks):
    rows = query.shape[0]

    def kernel(q_ref, g_ref, k0_ref, v0_ref, k1_ref, v1_ref, *rest):
        marks = [ref[...] for ref in rest[:4]]
        dq_ref, own_ref, twin_ref, held = rest[4:]
        q, g = q_ref[...], g_ref[...]
        keys = (k0_ref[...], k1_ref[...])
        prob = probabilities(q, keys, marks)
        prob_grad = [
            lax.dot_general(g, v[...], (((1,), (1,)), ((), ())), preferred_element_type=F32)
            for v in (v0_ref, v1_ref)
        ]
        delta = sum(jnp.sum(p * d, axis=-1, keepdims=True) for p, d in zip(prob, prob_grad))
        score = [(p * (d - delta)).astype(BF16) for p, d in zip(prob, prob_grad)]
        dq_ref[...] = sum(
            jnp.dot(s, k, preferred_element_type=F32) for s, k in zip(score, keys)
        )

        def back(left, right):
            return lax.dot_general(
                left, right, (((0,), (0,)), ((), ())), preferred_element_type=F32
            )

        parts = [
            back(score[0], q),
            back(prob[0].astype(BF16), g),
            back(score[1], q),
            back(prob[1].astype(BF16), g),
        ]

        @pl.when(pl.program_id(1) == 0)
        def _():
            own_ref[0], own_ref[1] = parts[0], parts[1]
            held[0], held[1] = parts[2], parts[3]

        @pl.when(pl.program_id(1) == 1)
        def _():
            own_ref[0] += parts[0]
            own_ref[1] += parts[1]
            twin_ref[0] = (held[0] + parts[2]).astype(BF16)
            twin_ref[1] = (held[1] + parts[3]).astype(BF16)

    head = pl.BlockSpec((rows, HEAD_DIM), lambda t, g: (0, 2 * t + g))
    pair = pl.BlockSpec((2, rows, HEAD_DIM), lambda t, g: (0, 0, t))
    return pl.pallas_call(
        kernel,
        grid=(2, 2),
        out_shape=(
            jax.ShapeDtypeStruct(query.shape, F32),
            jax.ShapeDtypeStruct((2, rows, 2 * HEAD_DIM), F32),
            jax.ShapeDtypeStruct((2, rows, 2 * HEAD_DIM), BF16),
        ),
        in_specs=[head, head] + key_specs(rows) + [whole(m.shape) for m in marks],
        out_specs=(head, pair, pair),
        scratch_shapes=[pltpu.VMEM((2, rows, HEAD_DIM), F32)],
        cost_estimate=pl.CostEstimate(
            flops=80 * rows * rows * HEAD_DIM, bytes_accessed=20 * rows * 512, transcendentals=8 * rows * rows
        ),
        compiler_params=pltpu.CompilerParams(vmem_limit_bytes=48 * 1024 * 1024),
        name="attend_back",
    )(query, grad, kv_own, kv_own, kv_twin, kv_twin, *marks)


def qkv_back(raw, query_grad, kv_own, kv_back, cosines, sines, query_gain, key_gain):
    rows = 128
    total = raw.shape[0]
    scale = 1.0 / math.sqrt(HEAD_DIM)

    def kernel(raw_ref, dq_ref, own_ref, back_ref, cos_ref, sin_ref, qg_ref, kg_ref, out_ref, gain_ref):
        cosine, sine = cos_ref[...], sin_ref[...]
        sums = [jnp.zeros((1, HEAD_DIM), F32)] * 2
        kv = own_ref[...] + back_ref[...].astype(F32)
        for t in range(2):
            for part in range(3):
                which = 0 if part < 2 else 1
                at = (2 * t + part if part < 2 else 4 + t) * HEAD_DIM
                values = raw_ref[:, at : at + HEAD_DIM]
                if part < 2:
                    grad = dq_ref[:, at : at + HEAD_DIM]
                else:
                    grad = kv[0, :, t * HEAD_DIM : (t + 1) * HEAD_DIM]
                grad = unturned(grad * scale, cosine, sine)
                r = head_scale(values)
                normed = values * r
                sums[which] = sums[which] + jnp.sum(grad * normed, axis=0, keepdims=True)
                grad = grad * (qg_ref[...] if part < 2 else kg_ref[...])
                grad = r * (grad - normed * jnp.mean(grad * normed, axis=-1, keepdims=True))
                at = (4 * t + part) * HEAD_DIM
                out_ref[:, at : at + HEAD_DIM] = grad.astype(BF16)
            at = (4 * t + 3) * HEAD_DIM
            out_ref[:, at : at + HEAD_DIM] = kv[1, :, t * HEAD_DIM : (t + 1) * HEAD_DIM].astype(BF16)

        @pl.when(pl.program_id(0) == 0)
        def _():
            gain_ref[...] = jnp.zeros_like(gain_ref)

        gain_ref[0:1] += sums[0]
        gain_ref[1:2] += sums[1]

    def rows_of(size):
        return pl.BlockSpec((rows, size), lambda i: (i, 0))

    pair = pl.BlockSpec((2, rows, 2 * HEAD_DIM), lambda i: (0, i, 0))
    return pl.pallas_call(
        kernel,
        grid=(total // rows,),
        out_shape=(
            jax.ShapeDtypeStruct((total, 8 * HEAD_DIM), BF16),
            jax.ShapeDtypeStruct(TILE, F32),
        ),
        in_specs=[
            rows_of(6 * HEAD_DIM),
            rows_of(4 * HEAD_DIM),
            pair,
            pair,
            rows_of(HEAD_DIM),
            rows_of(HEAD_DIM),
            whole((1, HEAD_DIM)),
            whole((1, HEAD_DIM)),
        ],
        out_specs=(rows_of(8 * HEAD_DIM), whole(TILE)),
        cost_estimate=pl.CostEstimate(
            flops=40 * total * 768, bytes_accessed=10 * total * 1024, transcendentals=0
        ),
        compiler_params=pltpu.CompilerParams(vmem_limit_bytes=24 * 1024 * 1024),
        name="qkv_back",
    )(raw, query_grad, kv_own, kv_back, cosines, sines, query_gain, key_gain)


def weight_partials(pairs):
    depth = pairs[0][0][0].shape[1]
    tensors = lax.axis_size(TENSOR)
    widths = [rights[0].shape[1] // tensors for _, rights in pairs]
    tokens = sum(block.shape[0] for block in pairs[0][0])
    tile = 512
    sides, in_specs = [], []
    for (lefts, rights), width in zip(pairs, widths):
        for left, right in zip(lefts, rights):
            sides += [left, right]
            in_specs.append(pl.BlockSpec((left.shape[0], tile), lambda t, k: (0, k)))
            in_specs.append(pl.BlockSpec((right.shape[0], width), lambda t, k: (0, t)))

    def kernel(*refs):
        out_ref = refs[-1]
        first, place = 0, 0
        for (lefts, _), width in zip(pairs, widths):
            product = 0.0
            for _ in lefts:
                product = product + lax.dot_general(
                    refs[place][...],
                    refs[place + 1][...],
                    (((0,), (0,)), ((), ())),
                    preferred_element_type=F32,
                )
                place += 2
            out_ref[0, :, first : first + width] = product.astype(BF16)
            first += width

    return pl.pallas_call(
        kernel,
        grid=(tensors, depth // tile),
        out_shape=jax.ShapeDtypeStruct((tensors, depth, sum(widths)), BF16),
        in_specs=in_specs,
        out_specs=pl.BlockSpec((1, tile, sum(widths)), lambda t, k: (t, k, 0)),
        cost_estimate=pl.CostEstimate(
            flops=2 * tokens * depth * sum(widths) * tensors,
            bytes_accessed=2 * depth * tensors * sum(widths) + 4 * tokens * depth,
            transcendentals=0,
        ),
        compiler_params=pltpu.CompilerParams(vmem_limit_bytes=24 * 1024 * 1024),
        name="weight_partials",
    )(*sides)


def scattered(partial):
    count = lax.axis_size(CTX)
    width = partial.shape[2]
    mine = lax.psum_scatter(
        partial.reshape(-1, width), (TENSOR, DP), scatter_dimension=0, tiled=True
    )
    return mine.reshape(count, mine.shape[0] // count, width)


def parts_of(got, widths):
    shards, first = [], 0
    for width in widths:
        part = [got[z, :, first : first + width] for z in range(got.shape[0])]
        shards.append(jnp.concatenate(part, axis=1).astype(F32))
        first += width
    return shards


def with_twin(own):
    other = shift(own, TENSOR, 1)
    first = lax.axis_index(TENSOR) == 0
    return jnp.concatenate([jnp.where(first, own, other), jnp.where(first, other, own)])


def sliced_layer(
    inputs,
    segment_ids,
    positions,
    out_grad,
    attn_gain,
    w_query,
    w_key,
    w_value,
    q_gain,
    k_gain,
    w_out,
    mlp_gain,
    w_gate,
    w_up,
    w_down,
):
    _, tok_count, width = inputs.shape
    count = lax.axis_size(CTX)
    tensors = lax.axis_size(TENSOR)
    rank = lax.axis_index(CTX)
    half = lax.axis_index(TENSOR)
    own_rows = tok_count // tensors
    rows = own_rows * count
    head_rows = w_out.shape[0]
    q_cols = w_query.shape[1] // count
    k_cols = w_key.shape[1] // count
    piece = attn_gain.shape[0]
    small = q_gain.shape[0]

    input_own = lax.dynamic_slice_in_dim(inputs[0], half * own_rows, own_rows, 0)
    grad_own = lax.dynamic_slice_in_dim(out_grad[0], half * own_rows, own_rows, 0)
    own_gains = jnp.concatenate([attn_gain, mlp_gain, q_gain, k_gain]).astype(F32)
    own_marks = jnp.concatenate([segment_ids[0], positions[0]])
    gains, marks, input_all, in_weight, out_weight = enter(
        to_tile(own_gains), to_tile(own_marks), input_own, w_query, w_key, w_value, w_out.T
    )
    out_weight = [out_weight[t * width : (t + 1) * width] for t in range(tensors)]
    gains = gains.reshape(gains.shape[0], -1)
    attn_scale = gains[:, :piece].reshape(-1)
    mlp_scale = gains[:, piece : 2 * piece].reshape(-1)
    query_scale = gains[:, 2 * piece : 2 * piece + small].reshape(-1)
    key_scale = gains[:, 2 * piece + small : 2 * (piece + small)].reshape(-1)

    ff_cols = w_gate.shape[1] // count
    late_gate, late_up, late_down, in_weight = lax.optimization_barrier(
        (w_gate, w_up, w_down, in_weight)
    )
    down_mine = swap_ahead(late_down.T.reshape(-1, count, ff_cols).transpose(1, 0, 2))
    mlp_shards = jnp.stack([late_gate, late_up]).reshape(2, -1, count, ff_cols)
    mlp_pieces = [lax.dynamic_index_in_dim(mlp_shards, rank, 2, keepdims=False)]
    for d in range(1, count):
        piece_ahead = lax.dynamic_index_in_dim(mlp_shards, (rank + d) % count, 2, keepdims=False)
        mlp_pieces.append(shift(piece_ahead, CTX, d))
    down_weight = lax.all_gather(rows_of(down_mine), (TENSOR, DP), axis=0, tiled=True)
    down_weight = [down_weight[t * width : (t + 1) * width] for t in range(tensors)]

    own_segs = lax.dynamic_index_in_dim(marks, half, 1, keepdims=False).reshape(rows)
    twin_segs = lax.dynamic_index_in_dim(marks, 1 - half, 1, keepdims=False).reshape(rows)
    own_positions = lax.dynamic_index_in_dim(marks, 2 + half, 1, keepdims=False).reshape(rows)
    order = jnp.arange(rows, dtype=jnp.int32)
    order = order // own_rows * tok_count + order % own_rows
    own_index, twin_index = order + half * own_rows, order + (1 - half) * own_rows
    token_marks = (
        own_segs[:, None],
        own_index[:, None],
        jnp.stack([own_segs, twin_segs]),
        jnp.stack([own_index, twin_index]),
    )
    cosine_table, sine_table = rope_tables(own_positions, HEAD_DIM)
    cosine_table = jnp.concatenate([cosine_table, cosine_table], axis=1)
    sine_table = jnp.concatenate([-sine_table, sine_table], axis=1)
    head_gains = (query_scale[None], key_scale[None])

    stream = input_own.astype(F32)
    input_all = lax.dynamic_update_index_in_dim(input_all, input_own, rank, 0)
    _, attn_norm_pullback = jax.vjp(rms_norm, stream, attn_scale)
    normed_low, raw, query_low, kv_own = qkv_forward(
        input_all, attn_scale[None], in_weight, cosine_table, sine_table, *head_gains
    )
    kv_twin = shift(kv_own, TENSOR, 1)
    attended_low = attend(query_low, kv_own, kv_twin, token_marks)
    attended_own = swap_heads(attended_low, True, 3)
    attended_ahead = take_ring(attended_low.reshape(count, own_rows, tensors * q_cols), rank)
    attended_ahead = [attended_ahead[d] for d in range(count)]
    middle = stream
    for t in range(tensors):
        middle = middle + jnp.dot(
            attended_own[:, t * head_rows : (t + 1) * head_rows],
            out_weight[t].T,
            preferred_element_type=F32
        )
    normed_mid, mlp_norm_pullback = jax.vjp(rms_norm, middle, mlp_scale)
    mid_own = normed_mid.astype(BF16)
    mid_low, grad_low, gate_weight, up_weight = spread_mlp(mid_own, grad_own, mlp_pieces)
    mid_low = lax.dynamic_update_index_in_dim(mid_low, mid_own, rank, 0).reshape(rows, width)
    grad_low = lax.dynamic_update_index_in_dim(grad_low, grad_own, rank, 0).reshape(rows, width)

    gate = jnp.dot(mid_low, gate_weight, preferred_element_type=F32)
    upward = jnp.dot(mid_low, up_weight, preferred_element_type=F32)
    hidden, silu_pullback = jax.vjp(silu_product, gate, upward)
    hidden_low = hidden.astype(BF16)
    down_part = sum(
        jnp.dot(
            hidden_low[:, t * ff_cols : (t + 1) * ff_cols],
            down_weight[t].T,
            preferred_element_type=F32,
        )
        for t in range(tensors)
    ).astype(BF16)
    down_sum = scatter_sum(down_part.reshape(count, own_rows, width))
    hidden_low, _ = lax.optimization_barrier((hidden_low, down_part))
    down_weight_part = weight_partials([([grad_low], [hidden_low])])
    down_mine = scattered(down_weight_part)
    grad_low, _ = lax.optimization_barrier((grad_low, down_weight_part))
    hidden_grad = [jnp.dot(grad_low, w, preferred_element_type=F32) for w in down_weight]
    hidden_grad = jnp.concatenate(hidden_grad, axis=1)
    gate_grad, upward_grad = silu_pullback(hidden_grad)
    gate_grad_low = gate_grad.astype(BF16)
    upward_grad_low = upward_grad.astype(BF16)
    mid_grad_part = jnp.dot(gate_grad_low, gate_weight.T, preferred_element_type=F32) + jnp.dot(
        upward_grad_low, up_weight.T, preferred_element_type=F32
    )
    mid_grad_part, gate_grad_low, upward_grad_low = lax.optimization_barrier(
        (mid_grad_part.astype(BF16), gate_grad_low, upward_grad_low)
    )
    mid_grad_part = mid_grad_part.reshape(count, own_rows, width)
    mid_grad = scatter_sum(mid_grad_part)
    gate_up_part = weight_partials([([mid_low], [gate_grad_low]), ([mid_low], [upward_grad_low])])
    gate_up_mine = scattered(gate_up_part)

    middle_norm_grad, mlp_gain_grad = mlp_norm_pullback(mid_grad)
    middle_grad = grad_own.astype(F32) + middle_norm_grad
    branch_grad = middle_grad.astype(BF16)
    attended_grad = jnp.concatenate(
        [jnp.dot(branch_grad, w, preferred_element_type=F32).astype(BF16) for w in out_weight],
        axis=1,
    )
    attended_grad = swap_heads(attended_grad, False, 4)
    branch_grad, attended_grad, down_mine = lax.optimization_barrier(
        (branch_grad, attended_grad, down_mine)
    )
    branch_all = [branch_grad] + [shift(branch_grad, CTX, -d) for d in range(1, count)]
    (down_weight_grad,) = columns_of(swap_ahead(down_mine), [ff_cols])
    query_grad, kv_grad, kv_back = attend_back(query_low, kv_own, kv_twin, attended_grad, token_marks)
    kv_back = shift(kv_back, TENSOR, 1)
    raw_grad_low, head_gain_grads = qkv_back(
        raw, query_grad, kv_grad, kv_back, cosine_table, sine_table, *head_gains
    )
    down_weight_grad = down_weight_grad.T
    output, raw_grad_low = lax.optimization_barrier(
        ((middle + down_sum).astype(BF16), raw_grad_low)
    )
    output = with_twin(output)[None]
    gate_up_ahead = [block_ahead(gate_up_mine, d) for d in range(count)]
    gate_up_ahead, raw_grad_low = lax.optimization_barrier((gate_up_ahead, raw_grad_low))
    normed_grad_part = jnp.dot(raw_grad_low, in_weight.T, preferred_element_type=F32)
    attn_part = weight_partials([([normed_low], [raw_grad_low]), (branch_all, attended_ahead)])
    normed_grad, attn_got = sum_tail(
        normed_grad_part.astype(BF16).reshape(count, own_rows, width), attn_part
    )
    gate_up_ahead, attn_got = lax.optimization_barrier((gate_up_ahead, attn_got))
    got = [shift(gate_up_ahead[d], CTX, d) for d in range(1, count)]
    gate_weight_grad, up_weight_grad = columns_of([gate_up_ahead[0]] + got, [ff_cols, ff_cols])
    normed_grad = sum(normed_grad[i].astype(F32) for i in range(count))
    query_weight_grad, key_weight_grad, value_weight_grad, out_weight_grad = parts_of(
        attn_got, [q_cols, k_cols, k_cols, q_cols]
    )
    stream_norm_grad, attn_gain_grad = attn_norm_pullback(normed_grad)
    gain_grads = jnp.concatenate(
        [
            attn_gain_grad.reshape(-1, piece),
            mlp_gain_grad.reshape(-1, piece),
            head_gain_grads[0].reshape(-1, small),
            head_gain_grads[1].reshape(-1, small),
        ],
        axis=1,
    )
    gain_grads = owner_sums(jax.vmap(to_tile)(gain_grads)).reshape(-1)
    input_grad = with_twin((middle_grad + stream_norm_grad).astype(BF16))[None]
    return (
        output,
        input_grad,
        gain_grads[:piece],
        query_weight_grad,
        key_weight_grad,
        value_weight_grad,
        gain_grads[2 * piece : 2 * piece + small],
        gain_grads[2 * piece + small : 2 * (piece + small)],
        out_weight_grad.T,
        gain_grads[piece : 2 * piece],
        gate_weight_grad,
        up_weight_grad,
        down_weight_grad,
    )


def on_device_sliced(*args):
    return sliced_layer(*args)


def can_slice(mesh, inputs, w_query, w_key, w_gate):
    tensors, count = mesh.shape[TENSOR], mesh.shape[CTX]
    return (
        (mesh.shape[DP], count, tensors) == (4, 4, 2)
        and inputs.shape[0] == mesh.shape[DP]
        and inputs.shape[1] == count * tensors * TILE[1]
        and w_key.shape[1] == tensors * count * HEAD_DIM
        and w_query.shape[1] == 2 * w_key.shape[1]
        and w_gate.shape[1] % (tensors * count * 128) == 0
    )


def on_device(
    inputs,
    segment_ids,
    positions,
    out_grad,
    attn_gain,
    w_query,
    w_key,
    w_value,
    q_gain,
    k_gain,
    w_out,
    mlp_gain,
    w_gate,
    w_up,
    w_down,
):
    seq_count, tok_count, width = inputs.shape
    row_count = seq_count * tok_count
    cycle_size = lax.axis_size(CTX)
    cycle_rank = lax.axis_index(CTX)
    gathered_attn = (
        lax.all_gather(w_query, (DP, CTX), axis=0, tiled=True),
        lax.all_gather(w_key, (DP, CTX), axis=0, tiled=True),
        lax.all_gather(w_value, (DP, CTX), axis=0, tiled=True),
        lax.all_gather(w_out, (DP, CTX), axis=1, tiled=True),
        lax.all_gather(attn_gain, (DP, CTX), axis=0, tiled=True),
        lax.all_gather(q_gain, (DP, CTX), axis=0, tiled=True),
        lax.all_gather(k_gain, (DP, CTX), axis=0, tiled=True),
    )
    query_weight, key_weight, value_weight, out_weight, attn_scale, query_scale, key_scale = (
        gathered_attn
    )
    gathered_mlp = (
        lax.all_gather(w_gate, (DP, CTX), axis=0, tiled=True),
        lax.all_gather(w_up, (DP, CTX), axis=0, tiled=True),
        lax.all_gather(w_down, (DP, CTX), axis=1, tiled=True),
        lax.all_gather(mlp_gain, (DP, CTX), axis=0, tiled=True),
    )
    gate_weight, up_weight, down_weight, mlp_scale = gathered_mlp
    segments_all = lax.all_gather(segment_ids, CTX, axis=1, tiled=True)
    local_heads = query_weight.shape[1] // HEAD_DIM
    local_kv = key_weight.shape[1] // HEAD_DIM
    group_size = local_heads // local_kv
    kv_width = local_kv * HEAD_DIM
    score_scale = 1.0 / math.sqrt(HEAD_DIM)
    stream = inputs.astype(jnp.float32).reshape(row_count, width)
    normed_attn, attn_norm_pullback = jax.vjp(rms_norm, stream, attn_scale.astype(jnp.float32))
    normed_low = normed_attn.astype(jnp.bfloat16)
    query_raw = jnp.dot(normed_low, query_weight, preferred_element_type=jnp.float32).reshape(
        seq_count, tok_count, local_heads, HEAD_DIM
    )
    key_raw = jnp.dot(normed_low, key_weight, preferred_element_type=jnp.float32).reshape(
        seq_count, tok_count, local_kv, HEAD_DIM
    )
    value_low = (
        jnp.dot(normed_low, value_weight, preferred_element_type=jnp.float32)
        .astype(jnp.bfloat16)
        .reshape(seq_count, tok_count, kv_width)
    )
    cosine_table, sine_table = rope_tables(positions, HEAD_DIM)
    cosine_table = cosine_table[:, :, None, :]
    sine_table = sine_table[:, :, None, :]

    def norm_rope(raw_heads, gain_vector):
        return head_norm(raw_heads, gain_vector, cosine_table, sine_table)

    query_rot, query_pullback = jax.vjp(norm_rope, query_raw, query_scale.astype(jnp.float32))
    key_rot, key_pullback = jax.vjp(norm_rope, key_raw, key_scale.astype(jnp.float32))
    query_low = query_rot.astype(jnp.bfloat16).reshape(
        seq_count, tok_count, local_kv, group_size, HEAD_DIM
    )
    key_low = key_rot.astype(jnp.bfloat16).reshape(seq_count, tok_count, kv_width)
    query_index = cycle_rank * tok_count + jnp.arange(tok_count, dtype=jnp.int32)

    def block_scores(key_block, first_row):
        key_count = key_block.shape[1]
        key_heads = key_block.reshape(seq_count, key_count, local_kv, HEAD_DIM)
        raw_scores = (
            jnp.einsum(
                "stkgd,snkd->skgtn", query_low, key_heads, preferred_element_type=jnp.float32
            )
            * score_scale
        )
        key_index = first_row + jnp.arange(key_count, dtype=jnp.int32)
        key_segments = lax.dynamic_slice_in_dim(segments_all, first_row, key_count, 1)
        allowed = (key_index[None, None, :] <= query_index[None, :, None]) & (
            key_segments[:, None, :] == segment_ids[:, :, None]
        )
        return (raw_scores, allowed[:, None, None, :, :])

    stat_shape = (seq_count, local_kv, group_size, tok_count)
    pieces = (
        lax.all_gather(key_low, CTX, axis=1, tiled=True),
        lax.all_gather(value_low, CTX, axis=1, tiled=True),
    )
    row_best = jnp.full(stat_shape, masked_value, jnp.float32)
    raw_scores, allowed = block_scores(pieces[0], jnp.int32(0))
    masked = jnp.where(allowed, raw_scores, masked_value)
    new_best = jnp.maximum(row_best, jnp.max(masked, axis=-1))
    weights = jnp.where(allowed, jnp.exp(masked - new_best[..., None]), 0.0)
    value_heads = pieces[1].reshape(seq_count, pieces[1].shape[1], local_kv, HEAD_DIM)
    added = jnp.einsum(
        "skgtn,snkd->skgtd",
        weights.astype(jnp.bfloat16),
        value_heads,
        preferred_element_type=jnp.float32,
    )
    row_total = jnp.sum(weights, axis=-1)
    log_total = new_best + jnp.log(row_total)
    attended = added / row_total[..., None]
    attended_low = (
        jnp.transpose(attended, (0, 3, 1, 2, 4))
        .reshape(row_count, local_heads * HEAD_DIM)
        .astype(jnp.bfloat16)
    )
    attn_part = jnp.dot(attended_low, out_weight, preferred_element_type=jnp.float32)
    middle = stream + lax.psum(attn_part.astype(jnp.bfloat16), TENSOR).astype(jnp.float32)
    normed_mid, mlp_norm_pullback = jax.vjp(rms_norm, middle, mlp_scale.astype(jnp.float32))
    mid_low = normed_mid.astype(jnp.bfloat16)
    gate = jnp.dot(mid_low, gate_weight, preferred_element_type=jnp.float32)
    upward = jnp.dot(mid_low, up_weight, preferred_element_type=jnp.float32)
    hidden, silu_pullback = jax.vjp(silu_product, gate, upward)
    hidden_low = hidden.astype(jnp.bfloat16)
    down_part = jnp.dot(hidden_low, down_weight, preferred_element_type=jnp.float32)
    down_sum = lax.psum(down_part.astype(jnp.bfloat16), TENSOR).astype(jnp.float32)
    output = (middle + down_sum).astype(jnp.bfloat16).reshape(seq_count, tok_count, width)
    grad_low = out_grad.reshape(row_count, width)
    down_weight_grad = jnp.dot(hidden_low.T, grad_low, preferred_element_type=jnp.float32)
    hidden_grad = jnp.dot(grad_low, down_weight.T, preferred_element_type=jnp.float32)
    gate_grad, upward_grad = silu_pullback(hidden_grad)
    gate_grad_low = gate_grad.astype(jnp.bfloat16)
    upward_grad_low = upward_grad.astype(jnp.bfloat16)
    gate_weight_grad = jnp.dot(mid_low.T, gate_grad_low, preferred_element_type=jnp.float32)
    up_weight_grad = jnp.dot(mid_low.T, upward_grad_low, preferred_element_type=jnp.float32)
    mid_grad_part = jnp.dot(
        gate_grad_low, gate_weight.T, preferred_element_type=jnp.float32
    ) + jnp.dot(upward_grad_low, up_weight.T, preferred_element_type=jnp.float32)
    mid_grad = lax.psum(mid_grad_part.astype(jnp.bfloat16), TENSOR).astype(jnp.float32)
    middle_norm_grad, mlp_gain_grad = mlp_norm_pullback(mid_grad)
    middle_grad = grad_low.astype(jnp.float32) + middle_norm_grad
    mlp_grads = (
        lax.psum_scatter(gate_weight_grad, (DP, CTX), scatter_dimension=0, tiled=True),
        lax.psum_scatter(up_weight_grad, (DP, CTX), scatter_dimension=0, tiled=True),
        lax.psum_scatter(down_weight_grad, (DP, CTX), scatter_dimension=1, tiled=True),
        lax.psum_scatter(mlp_gain_grad, (DP, CTX), scatter_dimension=0, tiled=True),
    )
    branch_grad = middle_grad.astype(jnp.bfloat16)
    out_weight_grad = jnp.dot(attended_low.T, branch_grad, preferred_element_type=jnp.float32)
    attended_grad = jnp.dot(branch_grad, out_weight.T, preferred_element_type=jnp.float32).astype(
        jnp.bfloat16
    )
    attended_grad_heads = jnp.transpose(
        attended_grad.reshape(seq_count, tok_count, local_kv, group_size, HEAD_DIM), (0, 2, 3, 1, 4)
    )
    row_delta = jnp.sum(attended_grad_heads.astype(jnp.float32) * attended, axis=-1)

    def key_block_grads(key_block, value_block, first_row):
        raw_scores, allowed = block_scores(key_block, first_row)
        probability = jnp.where(allowed, jnp.exp(raw_scores - log_total[..., None]), 0.0)
        key_count = key_block.shape[1]
        value_heads = value_block.reshape(seq_count, key_count, local_kv, HEAD_DIM)
        key_heads = key_block.reshape(seq_count, key_count, local_kv, HEAD_DIM)
        prob_grad = jnp.einsum(
            "skgtd,snkd->skgtn",
            attended_grad_heads,
            value_heads,
            preferred_element_type=jnp.float32,
        )
        score_grad = (probability * (prob_grad - row_delta[..., None])).astype(jnp.bfloat16)
        query_add = jnp.einsum(
            "skgtn,snkd->skgtd", score_grad, key_heads, preferred_element_type=jnp.float32
        )
        key_add = jnp.einsum(
            "skgtn,stkgd->snkd", score_grad, query_low, preferred_element_type=jnp.float32
        ).reshape(seq_count, key_count, kv_width)
        value_add = jnp.einsum(
            "skgtn,skgtd->snkd",
            probability.astype(jnp.bfloat16),
            attended_grad_heads,
            preferred_element_type=jnp.float32,
        ).reshape(seq_count, key_count, kv_width)
        return (query_add, key_add, value_add)

    query_zero = jnp.zeros(stat_shape + (HEAD_DIM,), jnp.float32)
    kv_zero = jnp.zeros((seq_count, tok_count, kv_width), jnp.float32)

    def cycle_turn(turn_index, state):
        key_block, value_block, key_grad_acc, value_grad_acc, query_grad_acc = state
        owner_rank = (cycle_rank + turn_index) % cycle_size
        query_add, key_add, value_add = key_block_grads(
            key_block, value_block, owner_rank * tok_count
        )
        moved_blocks = from_behind((key_block, value_block), CTX, -1)
        moved_grads = (
            from_behind((key_grad_acc + key_add).astype(jnp.bfloat16), CTX, -1).astype(
                jnp.float32
            ),
            from_behind((value_grad_acc + value_add).astype(jnp.bfloat16), CTX, -1).astype(
                jnp.float32
            ),
        )
        return (
            moved_blocks[0],
            moved_blocks[1],
            moved_grads[0],
            moved_grads[1],
            query_grad_acc + query_add,
        )

    final_state = lax.fori_loop(
        0, cycle_size, cycle_turn, (key_low, value_low, kv_zero, kv_zero, query_zero)
    )
    key_grad_sum = final_state[2]
    value_grad_sum = final_state[3]
    query_grad_sum = final_state[4]
    query_grad = (
        jnp.transpose(query_grad_sum, (0, 3, 1, 2, 4)).reshape(
            seq_count, tok_count, local_heads, HEAD_DIM
        )
        * score_scale
    )
    query_raw_grad, query_gain_grad = query_pullback(query_grad)
    key_raw_grad, key_gain_grad = key_pullback(
        (key_grad_sum * score_scale).reshape(seq_count, tok_count, local_kv, HEAD_DIM)
    )
    query_grad_low = query_raw_grad.reshape(row_count, local_heads * HEAD_DIM).astype(jnp.bfloat16)
    key_grad_low = key_raw_grad.reshape(row_count, kv_width).astype(jnp.bfloat16)
    value_grad_low = value_grad_sum.reshape(row_count, kv_width).astype(jnp.bfloat16)
    query_weight_grad = jnp.dot(normed_low.T, query_grad_low, preferred_element_type=jnp.float32)
    key_weight_grad = jnp.dot(normed_low.T, key_grad_low, preferred_element_type=jnp.float32)
    value_weight_grad = jnp.dot(normed_low.T, value_grad_low, preferred_element_type=jnp.float32)
    normed_grad_part = (
        jnp.dot(query_grad_low, query_weight.T, preferred_element_type=jnp.float32)
        + jnp.dot(key_grad_low, key_weight.T, preferred_element_type=jnp.float32)
        + jnp.dot(value_grad_low, value_weight.T, preferred_element_type=jnp.float32)
    )
    normed_grad, query_gain_total, key_gain_total = (
        lax.psum(normed_grad_part.astype(jnp.bfloat16), TENSOR).astype(jnp.float32),
        lax.psum(query_gain_grad.astype(jnp.bfloat16), TENSOR).astype(jnp.float32),
        lax.psum(key_gain_grad.astype(jnp.bfloat16), TENSOR).astype(jnp.float32),
    )
    stream_norm_grad, attn_gain_grad = attn_norm_pullback(normed_grad)
    input_grad = (
        (middle_grad + stream_norm_grad).astype(jnp.bfloat16).reshape(seq_count, tok_count, width)
    )
    attn_grads = (
        lax.psum_scatter(query_weight_grad, (DP, CTX), scatter_dimension=0, tiled=True),
        lax.psum_scatter(key_weight_grad, (DP, CTX), scatter_dimension=0, tiled=True),
        lax.psum_scatter(value_weight_grad, (DP, CTX), scatter_dimension=0, tiled=True),
        lax.psum_scatter(out_weight_grad, (DP, CTX), scatter_dimension=1, tiled=True),
        lax.psum_scatter(attn_gain_grad, (DP, CTX), scatter_dimension=0, tiled=True),
        lax.psum_scatter(query_gain_total, (DP, CTX), scatter_dimension=0, tiled=True),
        lax.psum_scatter(key_gain_total, (DP, CTX), scatter_dimension=0, tiled=True),
    )
    return (
        output,
        input_grad,
        attn_grads[4],
        attn_grads[0],
        attn_grads[1],
        attn_grads[2],
        attn_grads[5],
        attn_grads[6],
        attn_grads[3],
        mlp_grads[3],
        mlp_grads[0],
        mlp_grads[1],
        mlp_grads[2],
    )


def solution(mesh):
    in_specs = (
        P(DP, CTX, None),
        P(DP, CTX),
        P(DP, CTX),
        P(DP, CTX, None),
        P((DP, CTX)),
        P((DP, CTX), TENSOR),
        P((DP, CTX), TENSOR),
        P((DP, CTX), TENSOR),
        P((DP, CTX)),
        P((DP, CTX)),
        P(TENSOR, (DP, CTX)),
        P((DP, CTX)),
        P((DP, CTX), TENSOR),
        P((DP, CTX), TENSOR),
        P(TENSOR, (DP, CTX)),
    )
    out_specs = (
        P(DP, CTX, None),
        P(DP, CTX, None),
        P((DP, CTX)),
        P((DP, CTX), TENSOR),
        P((DP, CTX), TENSOR),
        P((DP, CTX), TENSOR),
        P((DP, CTX)),
        P((DP, CTX)),
        P(TENSOR, (DP, CTX)),
        P((DP, CTX)),
        P((DP, CTX), TENSOR),
        P((DP, CTX), TENSOR),
        P(TENSOR, (DP, CTX)),
    )

    def step(*args):
        body = on_device_sliced if can_slice(mesh, args[0], args[5], args[6], args[12]) else on_device
        return jax.shard_map(
            body, mesh=mesh, in_specs=in_specs, out_specs=out_specs, check_vma=False
        )(*args)

    return step
```

```python
import math
from types import SimpleNamespace

import jax
import jax.numpy as jnp
from jax import lax
from jax.experimental import pallas as pl
from jax.experimental.pallas import tpu as pltpu
from jax.sharding import PartitionSpec as P


HEAD_DIM = 128
BF16 = jnp.bfloat16
F32 = jnp.float32
MESH = pl.DeviceIdType.MESH
TILE = (8, 128)
DP, CTX, TENSOR = "dp", "ctx", "tensor"

epsilon = 1e-06
rope_base = 1000000.0
masked_value = -1e30


def from_behind(value, axis, steps):
    count = lax.axis_size(axis)
    pairs = [(source, (source + steps) % count) for source in range(count)]
    return lax.ppermute(value, axis, pairs)


def rope_tables(positions, head_size):
    half_dim = head_size // 2
    frequency = rope_base ** (-(jnp.arange(half_dim, dtype=jnp.float32) * 2.0) / head_size)
    angles = positions.astype(jnp.float32)[..., None] * frequency
    return (jnp.cos(angles), jnp.sin(angles))


def rotate(values, cosine_table, sine_table):
    half_dim = values.shape[-1] // 2
    first_half = values[..., :half_dim]
    second_half = values[..., half_dim:]
    return jnp.concatenate(
        [
            first_half * cosine_table - second_half * sine_table,
            second_half * cosine_table + first_half * sine_table,
        ],
        axis=-1,
    )


def head_norm(raw_heads, gain_vector, cosine_table, sine_table):
    scaled = (
        raw_heads
        * lax.rsqrt(jnp.mean(raw_heads * raw_heads, axis=-1, keepdims=True) + epsilon)
        * gain_vector
    )
    return rotate(scaled, cosine_table, sine_table)


def rms_norm(stream, gain_vector):
    return (
        stream
        * lax.rsqrt(jnp.mean(stream * stream, axis=-1, keepdims=True) + epsilon)
        * gain_vector
    )


def silu_product(gate, upward):
    return jax.nn.silu(gate) * upward


def shift(value, axis, steps):
    count = lax.axis_size(axis)
    pairs = [(source, (source + steps) % count) for source in range(count)]
    return lax.ppermute(value, axis, pairs)


def take_ring(blocks, first):
    return lax.dynamic_slice_in_dim(jnp.concatenate([blocks, blocks]), first, blocks.shape[0], 0)


def block_ahead(blocks, steps):
    count = lax.axis_size(CTX)
    place = (lax.axis_index(CTX) + steps) % count
    return lax.dynamic_index_in_dim(blocks, place, 0, keepdims=False)


def scatter_sum(blocks):
    total = block_ahead(blocks, 0).astype(F32)
    for d in range(1, blocks.shape[0]):
        total = total + shift(block_ahead(blocks, d), CTX, d).astype(F32)
    return total


def swap_ahead(blocks):
    count = lax.axis_size(CTX)
    return [block_ahead(blocks, 0)] + [
        shift(block_ahead(blocks, d), CTX, d) for d in range(1, count)
    ]


def rows_of(got):
    count, rank = len(got), lax.axis_index(CTX)
    size = got[0].shape[0]
    whole_rows = jnp.zeros((count * size, got[0].shape[1]), got[0].dtype)
    for d, block in enumerate(got):
        place = (rank - d) % count * size
        whole_rows = lax.dynamic_update_slice_in_dim(whole_rows, block, place, 0)
    return whole_rows


def assemble(blocks, widths, turned, behind):
    count, rows = len(blocks), blocks[0].shape[0]
    shapes = [(count * w, rows) if t else (rows, count * w) for w, t in zip(widths, turned)]

    def kernel(*refs):
        rank = lax.axis_index(CTX)
        for d in range(count):
            place = lax.rem(rank - d + count, count) if behind else d
            first = 0
            for out_ref, width, turn in zip(refs[count:], widths, turned):
                part = refs[d][:, first : first + width].astype(F32)
                spot = pl.ds(pl.multiple_of(place * width, 128), width)
                if turn:
                    out_ref[spot, :] = part.T
                else:
                    out_ref[:, spot] = part
                first += width

    size = sum(rows * count * w for w in widths)
    return pl.pallas_call(
        kernel,
        out_shape=[jax.ShapeDtypeStruct(shape, F32) for shape in shapes],
        in_specs=[ON_CHIP] * count,
        out_specs=[ON_CHIP] * len(widths),
        cost_estimate=pl.CostEstimate(flops=size, bytes_accessed=6 * size, transcendentals=0),
        compiler_params=pltpu.CompilerParams(vmem_limit_bytes=24 * 1024 * 1024),
        name="assemble",
    )(*blocks)


def greet(peers):
    barrier = pltpu.get_barrier_semaphore()
    for peer in peers:
        pl.semaphore_signal(barrier, inc=1, device_id=peer, device_id_type=MESH)
    pl.semaphore_wait(barrier, len(peers))


def remote(source, target, send_sem, recv_sem, peer):
    copy = pltpu.make_async_remote_copy(
        src_ref=source,
        dst_ref=target,
        send_sem=send_sem,
        recv_sem=recv_sem,
        device_id=peer,
        device_id_type=MESH,
    )
    copy.start()
    return copy


def to_tile(values):
    return jnp.pad(values, (0, math.prod(TILE) - values.shape[0])).reshape(TILE)


def place():
    pair, rank, half = lax.axis_index(DP), lax.axis_index(CTX), lax.axis_index(TENSOR)
    core = lax.rem(pair, 2)
    return SimpleNamespace(
        pair=pair,
        rank=rank,
        half=half,
        sibling=pair + 1 - 2 * core,
        across=lax.rem(pair + 2, 4),
        twin=1 - half,
    )


class Relay:
    KINDS = 9

    def __init__(self, here, source, view, rows, send_sem, recv_sem):
        self.here, self.source, self.view, self.rows = here, source, view, rows
        self.send_sem, self.recv_sem = send_sem, recv_sem
        self.copies = {}

    def go(self, kind, source, target, peer):
        self.copies[kind] = remote(
            source, target, self.send_sem.at[kind], self.recv_sem.at[kind], peer
        )

    def first(self):
        p = self.here
        target = self.view(p.half, p.pair, 0, self.rows)
        self.go(1, self.source, target, {DP: p.across})
        self.go(2, self.source, target, {TENSOR: p.twin})
        self.go(0, self.source, target, {DP: p.sibling})

    def second(self):
        p, part = self.here, self.rows // 2
        self.copies[1].wait_recv()
        low = self.view(p.half, p.across, 0, part)
        self.go(4, low, low, {TENSOR: p.twin})
        whole = self.view(p.half, p.across, 0, self.rows)
        self.go(3, whole, whole, {DP: p.sibling})
        self.copies[2].wait_recv()
        high = self.view(p.twin, p.pair, part, part)
        self.go(6, high, high, {DP: p.across})
        whole = self.view(p.twin, p.pair, 0, self.rows)
        self.go(5, whole, whole, {DP: p.sibling})

    def third(self):
        p, part = self.here, self.rows // 2
        self.copies[4].wait_recv()
        low = self.view(p.twin, p.across, 0, part)
        self.go(7, low, low, {DP: p.sibling})
        self.copies[6].wait_recv()
        high = self.view(p.twin, p.across, part, part)
        self.go(8, high, high, {DP: p.sibling})

    def last(self):
        for kind in (0, 3, 5, 7, 8):
            self.copies[kind].wait_recv()
        for copy in self.copies.values():
            copy.wait_send()


class Chain:
    def __init__(self, rank, count, source, spot, send_sem, recv_sem):
        self.rank, self.count, self.source, self.spot = rank, count, source, spot
        self.send_sem, self.recv_sem = send_sem, recv_sem

    def copy(self, way, step):
        step_to = self.rank + (1 if way == 0 else -1)
        owner = self.rank - step if way == 0 else self.rank + step
        owner = jnp.clip(owner, 0, self.count - 1)
        return pltpu.make_async_remote_copy(
            src_ref=self.source if step == 0 else self.spot(owner),
            dst_ref=self.spot(owner),
            send_sem=self.send_sem.at[way, step],
            recv_sem=self.recv_sem.at[way, step],
            device_id={CTX: jnp.clip(step_to, 0, self.count - 1)},
            device_id_type=MESH,
        )

    def sends(self, way, step):
        if way == 0:
            return (self.rank >= step) & (self.rank < self.count - 1)
        return (self.rank + step < self.count) & (self.rank > 0)

    def receives(self, way, step):
        return self.rank > step if way == 0 else self.rank + step < self.count - 1

    def start(self, step):
        for way in (0, 1):
            if step > 0:

                @pl.when(self.receives(way, step - 1))
                def _():
                    self.copy(way, step - 1).wait_recv()

            @pl.when(self.sends(way, step))
            def _():
                self.copy(way, step).start()

    def arrive(self):
        last = self.count - 2
        for way in (0, 1):

            @pl.when(self.receives(way, last))
            def _():
                self.copy(way, last).wait_recv()

    def drain(self):
        for way in (0, 1):
            for step in range(self.count - 1):

                @pl.when(self.sends(way, step))
                def _():
                    self.copy(way, step).wait_send()


SEMS = pltpu.SemaphoreType.DMA
ANYWHERE = pl.BlockSpec(memory_space=pl.ANY)
ON_CHIP = pl.BlockSpec(memory_space=pltpu.VMEM)


def enter(gains, marks, block, w_query, w_key, w_value, out_shard):
    count, pairs = lax.axis_size(CTX), lax.axis_size(DP)
    owners = count * pairs
    depth = w_query.shape[0]
    widths = [w.shape[1] // count for w in (w_query, w_key, w_value)]
    width = sum(widths)
    spots = [sum(widths[:i]) for i in range(3)]
    rows = block.shape[0]

    def kernel(
        gain_ref, mark_ref, block_ref, wq_ref, wk_ref, wv_ref, wo_ref,
        gains_ref, marks_ref, rows_ref, weight_ref, out_ref,
        held, held_out, out_send, out_recv, out_relay_send, out_relay_recv, gain_send, gain_recv, mark_send, mark_recv,
        swap_send, swap_recv, chain_send, chain_recv, relay_send, relay_recv, local_sem,
    ):
        here = place()
        rank, pair, half = here.rank, here.pair, here.half
        me = pair * count + rank
        far = [lax.rem(me + k, owners) for k in range(1, owners)]
        far = [{DP: lax.div(t, count), CTX: lax.rem(t, count)} for t in far]
        near = [{CTX: lax.rem(rank + k, count)} for k in range(1, count)]
        greet(far + [{TENSOR: here.twin}])

        def view(owner_rank):
            def at(t, p, start, size):
                first = pl.multiple_of((p * count + owner_rank) * depth + start, 64)
                return weight_ref.at[pl.ds(first, size), pl.ds(pl.multiple_of(t * width, 128), width)]

            return at

        def out_view(owner_rank):
            def at(t, p, start, size):
                first = t * owners * depth + (p * count + owner_rank) * depth + start
                return out_ref.at[pl.ds(pl.multiple_of(first, 64), size)]

            return at

        def columns(ref, i, target):
            return ref.at[:, pl.ds(pl.multiple_of(target * widths[i], 128), widths[i])]

        sources = (wq_ref, wk_ref, wv_ref)
        takes = [
            pltpu.make_async_copy(
                columns(ref, i, rank), held.at[:, pl.ds(spots[i], widths[i])], local_sem.at[i]
            )
            for i, ref in enumerate(sources)
        ]
        takes.append(pltpu.make_async_copy(wo_ref, held_out, local_sem.at[4]))
        for take in takes:
            take.start()
        small = [
            remote(mark_ref, marks_ref.at[rank], mark_send.at[k], mark_recv.at[k], peer)
            for k, peer in enumerate(near)
        ]
        small += [
            remote(gain_ref, gains_ref.at[me], gain_send.at[k], gain_recv.at[k], peer)
            for k, peer in enumerate(far)
        ]
        own_rows = pl.ds(pl.multiple_of(me * depth, depth), depth)
        swaps = []
        for k, peer in enumerate(near):
            swaps.append([])
            for i, ref in enumerate(sources):
                spot = pl.ds(pl.multiple_of(half * width + spots[i], 128), widths[i])
                swaps[k].append(
                    remote(
                        columns(ref, i, peer[CTX]),
                        weight_ref.at[own_rows, spot],
                        swap_send.at[k, i],
                        swap_recv.at[k, i],
                        peer,
                    )
                )
                out_own = out_view(rank)(half, pair, 0, depth)
        out_chain = Chain(
            rank, count, wo_ref, lambda o: out_view(o)(half, pair, 0, depth), out_send, out_recv
        )
        out_chain.start(0)
        chain = Chain(rank, count, block_ref, lambda o: rows_ref.at[o], chain_send, chain_recv)
        gains_ref[me] = gain_ref[...]
        marks_ref[rank] = mark_ref[...]
        for take in takes:
            take.wait()
        keep = pltpu.make_async_copy(held, view(rank)(half, pair, 0, depth), local_sem.at[3])
        keep.start()
        keep_out = pltpu.make_async_copy(held_out, out_own, local_sem.at[5])
        keep_out.start()
        relays = [Relay(here, held, view(rank), depth, relay_send.at[0], relay_recv.at[0])]
        relays[0].first()
        for k in range(1, count):
            owner = lax.rem(rank - k + count, count)
            for swap in swaps[k - 1]:
                swap.wait_recv()
            at = view(owner)
            relays.append(
                Relay(here, at(half, pair, 0, depth), at, depth, relay_send.at[k], relay_recv.at[k])
            )
            relays[k].first()
        out_chain.start(1)
        out_chain.start(2)
        chain.start(0)
        for relay in relays:
            relay.second()
        for relay in relays:
            relay.third()
        keep_out.wait()
        out_chain.arrive()
        at = out_view(0)
        relays.append(
            Relay(
                here, at(half, pair, 0, count * depth), at, count * depth,
                out_relay_send, out_relay_recv,
            )
        )
        relays[-1].first()
        chain.start(1)
        relays[-1].second()
        chain.start(2)
        relays[-1].third()
        for relay in relays:
            relay.last()
        keep.wait()
        chain.arrive()
        chain.drain()
        out_chain.drain()
        for swap in swaps:
            for copy in swap:
                copy.wait_send()
        for copy in small:
            copy.wait()

    return pl.pallas_call(
        kernel,
        out_shape=(
            jax.ShapeDtypeStruct((owners, *TILE), F32),
            jax.ShapeDtypeStruct((count, *TILE), jnp.int32),
            jax.ShapeDtypeStruct((count, rows, block.shape[1]), block.dtype),
            jax.ShapeDtypeStruct((owners * depth, 2 * width), w_query.dtype),
            jax.ShapeDtypeStruct((2 * owners * depth, out_shard.shape[1]), out_shard.dtype),
        ),
        in_specs=[ON_CHIP] * 2 + [ANYWHERE] * 5,
        out_specs=(ON_CHIP, ON_CHIP, ANYWHERE, ANYWHERE, ANYWHERE),
        scratch_shapes=[
            pltpu.VMEM((depth, width), w_query.dtype),
            pltpu.VMEM(out_shard.shape, out_shard.dtype),
            SEMS((2, count - 1)),
            SEMS((2, count - 1)),
            SEMS((Relay.KINDS,)),
            SEMS((Relay.KINDS,)),
            SEMS((owners - 1,)),
            SEMS((owners - 1,)),
            SEMS((count - 1,)),
            SEMS((count - 1,)),
            SEMS((count - 1, 3)),
            SEMS((count - 1, 3)),
            SEMS((2, count - 1)),
            SEMS((2, count - 1)),
            SEMS((count, Relay.KINDS)),
            SEMS((count, Relay.KINDS)),
            SEMS((6,)),
        ],
        compiler_params=pltpu.CompilerParams(collective_id=0, has_side_effects=True),
        name="enter",
    )(gains, marks, block, w_query, w_key, w_value, out_shard)


def spread_mlp(first, second, pieces):
    count, pairs = lax.axis_size(CTX), lax.axis_size(DP)
    kinds, depth, width = pieces[0].shape
    rows, features = first.shape

    def kernel(first_ref, second_ref, *rest):
        piece_refs, rest = rest[:count], rest[count:]
        firsts_ref, seconds_ref = rest[:2]
        weight_refs, rest = rest[2 : 2 + kinds], rest[2 + kinds :]
        held, chain_send, chain_recv, relay_send, relay_recv, take_sem, keep_sem = rest
        here = place()
        rank, pair, half = here.rank, here.pair, here.half
        greet(
            [{CTX: lax.rem(rank + k, count)} for k in range(1, count)]
            + [{DP: here.sibling}, {DP: here.across}, {TENSOR: here.twin}]
        )
        takes = []
        for i in range(kinds):
            for d, ref in enumerate(piece_refs):
                owner = lax.rem(rank - d + count, count)
                take = pltpu.make_async_copy(
                    ref.at[i],
                    held.at[i, pl.ds(pl.multiple_of(owner * depth, depth), depth)],
                    take_sem.at[i, d],
                )
                take.start()
                takes.append(take)
        chains = [
            Chain(rank, count, first_ref, lambda o: firsts_ref.at[o], chain_send.at[0], chain_recv.at[0]),
            Chain(rank, count, second_ref, lambda o: seconds_ref.at[o], chain_send.at[1], chain_recv.at[1]),
        ]
        chains[0].start(0)
        block = count * depth

        def view(i):
            def at(t, p, start, size):
                first = pl.multiple_of(p * block + start, 64)
                return weight_refs[i].at[
                    pl.ds(first, size), pl.ds(pl.multiple_of(t * width, 128), width)
                ]

            return at

        relays, keeps = [], []
        for i in range(kinds):
            for take in takes[i * count : (i + 1) * count]:
                take.wait()
            keeps.append(
                pltpu.make_async_copy(held.at[i], view(i)(half, pair, 0, block), keep_sem.at[i])
            )
            keeps[i].start()
            relays.append(
                Relay(here, held.at[i], view(i), block, relay_send.at[i], relay_recv.at[i])
            )
            relays[i].first()
        chains[0].start(1)
        relays[0].second()
        chains[0].start(2)
        chains[1].start(0)
        relays[0].third()
        relays[1].second()
        chains[1].start(1)
        relays[1].third()
        chains[1].start(2)
        for relay in relays:
            relay.last()
        for keep in keeps:
            keep.wait()
        for chain in chains:
            chain.arrive()
            chain.drain()

    return pl.pallas_call(
        kernel,
        out_shape=(
            jax.ShapeDtypeStruct((count, rows, features), first.dtype),
            jax.ShapeDtypeStruct((count, rows, features), second.dtype),
        )
        + (jax.ShapeDtypeStruct((pairs * count * depth, 2 * width), pieces[0].dtype),) * kinds,
        in_specs=[ANYWHERE] * (2 + count),
        out_specs=(ANYWHERE,) * (2 + kinds),
        scratch_shapes=[
            pltpu.VMEM((kinds, count * depth, width), pieces[0].dtype),
            SEMS((2, 2, count - 1)),
            SEMS((2, 2, count - 1)),
            SEMS((kinds, Relay.KINDS)),
            SEMS((kinds, Relay.KINDS)),
            SEMS((kinds, count)),
            SEMS((kinds,)),
        ],
        compiler_params=pltpu.CompilerParams(
            collective_id=2, has_side_effects=True, vmem_limit_bytes=16 * 1024 * 1024
        ),
        name="spread_mlp",
    )(first, second, *pieces)


def swap_heads(source, gather, collective_id):
    count = lax.axis_size(CTX)
    tensors = lax.axis_size(TENSOR)
    rows, width = source.shape
    own = rows // count if gather else rows
    part = width // tensors if gather else width // (tensors * count)
    shape = (own, tensors * count * part) if gather else (count * own, tensors * part)

    def kernel(source_ref, got_ref, held, send_sem, recv_sem, local_sem):
        rank = lax.axis_index(CTX)
        peers = [lax.rem(rank + k, count) for k in range(1, count)]
        greet([{CTX: peer} for peer in peers])

        def tall(ref, z, t):
            return ref.at[pl.ds(pl.multiple_of(z * own, own), own), pl.ds(t * part, part)]

        def wide(ref, z, t):
            return ref.at[:, pl.ds(pl.multiple_of((t * count + z) * part, part), part)]

        take, put = (tall, wide) if gather else (wide, tall)
        copies = [
            remote(
                take(source_ref, peer, t),
                put(got_ref, rank, t),
                send_sem.at[k, t],
                recv_sem.at[k, t],
                {CTX: peer},
            )
            for k, peer in enumerate(peers)
            for t in range(tensors)
        ]
        local = [
            pltpu.make_async_copy(take(source_ref, rank, t), held.at[t], local_sem.at[t])
            for t in range(tensors)
        ]
        for copy in local:
            copy.start()
        for copy in local:
            copy.wait()
        local = [
            pltpu.make_async_copy(held.at[t], put(got_ref, rank, t), local_sem.at[tensors + t])
            for t in range(tensors)
        ]
        for copy in local:
            copy.start()
        for copy in local + copies:
            copy.wait()

    return pl.pallas_call(
        kernel,
        out_shape=jax.ShapeDtypeStruct(shape, source.dtype),
        in_specs=[ANYWHERE],
        out_specs=ANYWHERE,
        scratch_shapes=[
            pltpu.VMEM((tensors, own, part), source.dtype),
            SEMS((count - 1, tensors)),
            SEMS((count - 1, tensors)),
            SEMS((2 * tensors,)),
        ],
        compiler_params=pltpu.CompilerParams(collective_id=collective_id, has_side_effects=True),
    )(source)


def sum_tail(blocks, partial):
    count = lax.axis_size(CTX)
    tensors, depth, width = partial.shape
    part = depth // 4
    low = part // 2
    own = part // count
    tile = 64

    def kernel(
        blocks_ref, partial_ref, got_ref, owned_ref,
        held, kept, near, mine, far, near_b, far_b, result,
        send_sem, recv_sem, block_send, block_recv, swap_send, swap_recv, local_sem,
    ):
        here = place()
        rank, pair, half = here.rank, here.pair, here.half
        core, side = lax.rem(pair, 2), lax.div(pair, 2)
        peers = [lax.rem(rank + k, count) for k in range(1, count)]
        greet(
            [{CTX: peer} for peer in peers]
            + [{DP: here.sibling}, {DP: here.across}, {TENSOR: here.twin}]
        )

        def rows_of(t, x, c):
            return partial_ref.at[t, pl.ds(pl.multiple_of((x * 2 + c) * part, part), part)]

        copies = {}
        for t in range(tensors):
            for x in range(2):
                copies[0, t, x] = remote(
                    rows_of(t, x, 1 - core),
                    near.at[t, x],
                    send_sem.at[t * 2 + x],
                    recv_sem.at[t * 2 + x],
                    {DP: here.sibling},
                )
        takes = [
            pltpu.make_async_copy(rows_of(t, x, core), kept.at[t, x], local_sem.at[t * 2 + x])
            for t in range(tensors)
            for x in range(2)
        ]
        for take in takes:
            take.start()
        moves = [
            remote(
                blocks_ref.at[peer], got_ref.at[rank], block_send.at[k], block_recv.at[k], {CTX: peer}
            )
            for k, peer in enumerate(peers)
        ]
        take_own = pltpu.make_async_copy(blocks_ref.at[rank], held, local_sem.at[4])
        take_own.start()

        def add(target, left, right, size):
            @pl.loop(0, size // tile)
            def _(i):
                at = pl.ds(pl.multiple_of(i * tile, tile), tile)
                target[at] = (left[at].astype(F32) + right[at].astype(F32)).astype(BF16)

        for t in range(tensors):
            for x in range(2):
                takes[t * 2 + x].wait()
                copies[0, t, x].wait_recv()
                add(mine.at[t, x], kept.at[t, x], near.at[t, x], part)
        first, second = pl.ds(0, low), pl.ds(low, low)
        for i in range(2):
            copies[1, i] = remote(
                mine.at[here.twin, i, first],
                far.at[i],
                send_sem.at[4 + i],
                recv_sem.at[4 + i],
                {TENSOR: here.twin},
            )
            copies[2, i] = remote(
                mine.at[i, 1 - side, second],
                far_b.at[i],
                send_sem.at[6 + i],
                recv_sem.at[6 + i],
                {DP: here.across},
            )
        for i in range(2):
            copies[1, i].wait_recv()
            add(near.at[0, i], mine.at[half, i, first], far.at[i], low)
            copies[2, i].wait_recv()
            add(near.at[1, i], mine.at[i, side, second], far_b.at[i], low)
        copies[3] = remote(
            near.at[0, 1 - side, first],
            near_b.at[0],
            send_sem.at[8],
            recv_sem.at[8],
            {DP: here.across},
        )
        copies[4] = remote(
            near.at[1, here.twin, first],
            near_b.at[1],
            send_sem.at[9],
            recv_sem.at[9],
            {TENSOR: here.twin},
        )
        take_own.wait()
        keep_own = pltpu.make_async_copy(held, got_ref.at[rank], local_sem.at[5])
        keep_own.start()
        copies[3].wait_recv()
        add(result.at[first], near.at[0, side, first], near_b.at[0], low)
        copies[4].wait_recv()
        add(result.at[second], near.at[1, half, first], near_b.at[1], low)

        def rows_for(target):
            return result.at[pl.ds(pl.multiple_of(target * own, own), own)]

        swaps = [
            remote(
                rows_for(peer), owned_ref.at[rank], swap_send.at[k], swap_recv.at[k], {CTX: peer}
            )
            for k, peer in enumerate(peers)
        ]
        keep = pltpu.make_async_copy(rows_for(rank), owned_ref.at[rank], local_sem.at[6])
        keep.start()
        for copy in swaps + moves:
            copy.wait()
        for copy in copies.values():
            copy.wait_send()
        keep.wait()
        keep_own.wait()

    sixteen = 10
    return pl.pallas_call(
        kernel,
        out_shape=(
            jax.ShapeDtypeStruct(blocks.shape, BF16),
            jax.ShapeDtypeStruct((count, own, width), BF16),
        ),
        in_specs=[ANYWHERE, ANYWHERE],
        out_specs=(ANYWHERE, ANYWHERE),
        scratch_shapes=[
            pltpu.VMEM(blocks.shape[1:], BF16),
            pltpu.VMEM((tensors, 2, part, width), BF16),
            pltpu.VMEM((tensors, 2, part, width), BF16),
            pltpu.VMEM((tensors, 2, part, width), BF16),
            pltpu.VMEM((2, low, width), BF16),
            pltpu.VMEM((2, low, width), BF16),
            pltpu.VMEM((2, low, width), BF16),
            pltpu.VMEM((part, width), BF16),
            SEMS((sixteen,)),
            SEMS((sixteen,)),
            SEMS((count - 1,)),
            SEMS((count - 1,)),
            SEMS((count - 1,)),
            SEMS((count - 1,)),
            SEMS((7,)),
        ],
        compiler_params=pltpu.CompilerParams(
            collective_id=5, has_side_effects=True, vmem_limit_bytes=24 * 1024 * 1024
        ),
        name="sum_tail",
    )(blocks, partial)


def owner_sums(tiles):
    count, pairs, tensors = lax.axis_size(CTX), lax.axis_size(DP), lax.axis_size(TENSOR)
    total = count * pairs * tensors

    def kernel(tiles_ref, sum_ref, got, send_sem, recv_sem):
        owner = lax.axis_index(DP) * count + lax.axis_index(CTX)
        half = lax.axis_index(TENSOR)
        me = owner * tensors + half
        targets = [lax.rem(me + k, total) for k in range(1, total)]
        peers = [
            {
                DP: lax.div(t, count * tensors),
                CTX: lax.rem(lax.div(t, tensors), count),
                TENSOR: lax.rem(t, tensors),
            }
            for t in targets
        ]
        greet(peers)
        copies = [
            remote(
                tiles_ref.at[lax.div(t, tensors)], got.at[me], send_sem.at[k], recv_sem.at[k], peer
            )
            for k, (t, peer) in enumerate(zip(targets, peers))
        ]
        got[me] = tiles_ref[owner]
        for copy in copies:
            copy.wait()
        value = got[0]
        for source in range(1, total):
            value = value + got[source]
        sum_ref[...] = value

    return pl.pallas_call(
        kernel,
        out_shape=jax.ShapeDtypeStruct(TILE, F32),
        in_specs=[ON_CHIP],
        out_specs=ON_CHIP,
        scratch_shapes=[
            pltpu.VMEM((total, *TILE), F32),
            SEMS((total - 1,)),
            SEMS((total - 1,)),
        ],
        compiler_params=pltpu.CompilerParams(collective_id=1, has_side_effects=True),
        name="owner_sums",
    )(tiles)


def whole(shape):
    return pl.BlockSpec(shape, lambda *_: (0,) * len(shape))


def turned(values, cosines, sines):
    return values * cosines + pltpu.roll(values, HEAD_DIM // 2, 1) * sines


def unturned(grads, cosines, sines):
    return grads * cosines + pltpu.roll(grads * sines, HEAD_DIM // 2, 1)


def head_scale(raw):
    return lax.rsqrt(jnp.mean(raw * raw, axis=-1, keepdims=True) + epsilon)


def qkv_forward(blocks, scale, weight, cosines, sines, query_gain, key_gain):
    count, rows, width = blocks.shape
    cols = weight.shape[1]

    def kernel(x_ref, s_ref, w_ref, cos_ref, sin_ref, qg_ref, kg_ref, n_ref, raw_ref, q_ref, kv_ref):
        x = x_ref[0].astype(F32)
        normed = x * lax.rsqrt(jnp.mean(x * x, axis=-1, keepdims=True) + epsilon) * s_ref[...]
        normed = normed.astype(BF16)
        n_ref[...] = normed
        raw = jnp.dot(normed, w_ref[...], preferred_element_type=F32)
        cosine, sine = cos_ref[...], sin_ref[...]
        for head in range(8):
            t, part = head // 4, head % 4
            values = raw[:, head * HEAD_DIM : (head + 1) * HEAD_DIM]
            if part < 3:
                at = (2 * t + part if part < 2 else 4 + t) * HEAD_DIM
                raw_ref[:, at : at + HEAD_DIM] = values
                gain = qg_ref[...] if part < 2 else kg_ref[...]
                values = turned(values * head_scale(values) * gain, cosine, sine)
            if part < 2:
                at = (2 * t + part) * HEAD_DIM
                q_ref[:, at : at + HEAD_DIM] = values.astype(BF16)
            else:
                at = (t if part == 2 else 2 + t) * HEAD_DIM
                kv_ref[:, at : at + HEAD_DIM] = values.astype(BF16)

    def rows_of(size):
        return pl.BlockSpec((rows, size), lambda i: (i, 0))

    total = count * rows
    return pl.pallas_call(
        kernel,
        grid=(count,),
        out_shape=(
            jax.ShapeDtypeStruct((total, width), BF16),
            jax.ShapeDtypeStruct((total, 6 * HEAD_DIM), F32),
            jax.ShapeDtypeStruct((total, 4 * HEAD_DIM), BF16),
            jax.ShapeDtypeStruct((total, 4 * HEAD_DIM), BF16),
        ),
        in_specs=[
            pl.BlockSpec((1, rows, width), lambda i: (i, 0, 0)),
            whole((1, width)),
            whole((width, cols)),
            rows_of(HEAD_DIM),
            rows_of(HEAD_DIM),
            whole((1, HEAD_DIM)),
            whole((1, HEAD_DIM)),
        ],
        out_specs=(rows_of(width), rows_of(6 * HEAD_DIM), rows_of(4 * HEAD_DIM), rows_of(4 * HEAD_DIM)),
        cost_estimate=pl.CostEstimate(
            flops=2 * total * width * cols, bytes_accessed=2 * width * (cols + total), transcendentals=0
        ),
        compiler_params=pltpu.CompilerParams(vmem_limit_bytes=24 * 1024 * 1024),
        name="qkv_forward",
    )(blocks, scale, weight, cosines, sines, query_gain, key_gain)


def probabilities(q, keys, marks):
    seg, index, key_seg, key_index = marks
    scores = []
    for i, key in enumerate(keys):
        s = lax.dot_general(q, key, (((1,), (1,)), ((), ())), preferred_element_type=F32)
        ok = (key_index[i : i + 1] <= index) & (key_seg[i : i + 1] == seg)
        scores.append(jnp.where(ok, s * (1.0 / math.sqrt(HEAD_DIM)), masked_value))
    best = jnp.maximum(*[jnp.max(s, axis=-1, keepdims=True) for s in scores])
    weights = [jnp.exp(s - best) for s in scores]
    total = sum(jnp.sum(w, axis=-1, keepdims=True) for w in weights)
    return [w / total for w in weights]


def key_specs(rows):
    tensors = 2
    specs = []
    for place in (0, tensors):
        specs.append(pl.BlockSpec((rows, HEAD_DIM), lambda t, g, p=place: (0, p + t)))
    return specs * 2


def attend(query, kv_own, kv_twin, marks):
    rows = query.shape[0]

    def kernel(q_ref, k0_ref, v0_ref, k1_ref, v1_ref, *rest):
        marks, out_ref = [ref[...] for ref in rest[:4]], rest[4]
        prob = probabilities(q_ref[...], (k0_ref[...], k1_ref[...]), marks)
        out = jnp.dot(prob[0].astype(BF16), v0_ref[...], preferred_element_type=F32)
        out = out + jnp.dot(prob[1].astype(BF16), v1_ref[...], preferred_element_type=F32)
        out_ref[...] = out.astype(BF16)

    head = pl.BlockSpec((rows, HEAD_DIM), lambda t, g: (0, 2 * t + g))
    return pl.pallas_call(
        kernel,
        grid=(2, 2),
        out_shape=jax.ShapeDtypeStruct(query.shape, BF16),
        in_specs=[head] + key_specs(rows) + [whole(m.shape) for m in marks],
        out_specs=head,
        cost_estimate=pl.CostEstimate(
            flops=32 * rows * rows * HEAD_DIM, bytes_accessed=8 * rows * 512, transcendentals=8 * rows * rows
        ),
        compiler_params=pltpu.CompilerParams(vmem_limit_bytes=32 * 1024 * 1024),
        name="attend",
    )(query, kv_own, kv_own, kv_twin, kv_twin, *marks)


def attend_back(query, kv_own, kv_twin, grad, marks):
    rows = query.shape[0]

    def kernel(q_ref, g_ref, k0_ref, v0_ref, k1_ref, v1_ref, *rest):
        marks = [ref[...] for ref in rest[:4]]
        dq_ref, own_ref, twin_ref, held = rest[4:]
        q, g = q_ref[...], g_ref[...]
        keys = (k0_ref[...], k1_ref[...])
        prob = probabilities(q, keys, marks)
        prob_grad = [
            lax.dot_general(g, v[...], (((1,), (1,)), ((), ())), preferred_element_type=F32)
            for v in (v0_ref, v1_ref)
        ]
        delta = sum(jnp.sum(p * d, axis=-1, keepdims=True) for p, d in zip(prob, prob_grad))
        score = [(p * (d - delta)).astype(BF16) for p, d in zip(prob, prob_grad)]
        dq_ref[...] = sum(
            jnp.dot(s, k, preferred_element_type=F32) for s, k in zip(score, keys)
        )

        def back(left, right):
            return lax.dot_general(
                left, right, (((0,), (0,)), ((), ())), preferred_element_type=F32
            )

        parts = [
            back(score[0], q),
            back(prob[0].astype(BF16), g),
            back(score[1], q),
            back(prob[1].astype(BF16), g),
        ]

        @pl.when(pl.program_id(1) == 0)
        def _():
            own_ref[0], own_ref[1] = parts[0], parts[1]
            held[0], held[1] = parts[2], parts[3]

        @pl.when(pl.program_id(1) == 1)
        def _():
            own_ref[0] += parts[0]
            own_ref[1] += parts[1]
            twin_ref[0] = (held[0] + parts[2]).astype(BF16)
            twin_ref[1] = (held[1] + parts[3]).astype(BF16)

    head = pl.BlockSpec((rows, HEAD_DIM), lambda t, g: (0, 2 * t + g))
    pair = pl.BlockSpec((2, rows, HEAD_DIM), lambda t, g: (0, 0, t))
    return pl.pallas_call(
        kernel,
        grid=(2, 2),
        out_shape=(
            jax.ShapeDtypeStruct(query.shape, F32),
            jax.ShapeDtypeStruct((2, rows, 2 * HEAD_DIM), F32),
            jax.ShapeDtypeStruct((2, rows, 2 * HEAD_DIM), BF16),
        ),
        in_specs=[head, head] + key_specs(rows) + [whole(m.shape) for m in marks],
        out_specs=(head, pair, pair),
        scratch_shapes=[pltpu.VMEM((2, rows, HEAD_DIM), F32)],
        cost_estimate=pl.CostEstimate(
            flops=80 * rows * rows * HEAD_DIM, bytes_accessed=20 * rows * 512, transcendentals=8 * rows * rows
        ),
        compiler_params=pltpu.CompilerParams(vmem_limit_bytes=48 * 1024 * 1024),
        name="attend_back",
    )(query, grad, kv_own, kv_own, kv_twin, kv_twin, *marks)


def qkv_back(raw, query_grad, kv_own, kv_back, cosines, sines, query_gain, key_gain):
    rows = 128
    total = raw.shape[0]
    scale = 1.0 / math.sqrt(HEAD_DIM)

    def kernel(raw_ref, dq_ref, own_ref, back_ref, cos_ref, sin_ref, qg_ref, kg_ref, out_ref, gain_ref):
        cosine, sine = cos_ref[...], sin_ref[...]
        sums = [jnp.zeros((1, HEAD_DIM), F32)] * 2
        kv = own_ref[...] + back_ref[...].astype(F32)
        for t in range(2):
            for part in range(3):
                which = 0 if part < 2 else 1
                at = (2 * t + part if part < 2 else 4 + t) * HEAD_DIM
                values = raw_ref[:, at : at + HEAD_DIM]
                if part < 2:
                    grad = dq_ref[:, at : at + HEAD_DIM]
                else:
                    grad = kv[0, :, t * HEAD_DIM : (t + 1) * HEAD_DIM]
                grad = unturned(grad * scale, cosine, sine)
                r = head_scale(values)
                normed = values * r
                sums[which] = sums[which] + jnp.sum(grad * normed, axis=0, keepdims=True)
                grad = grad * (qg_ref[...] if part < 2 else kg_ref[...])
                grad = r * (grad - normed * jnp.mean(grad * normed, axis=-1, keepdims=True))
                at = (4 * t + part) * HEAD_DIM
                out_ref[:, at : at + HEAD_DIM] = grad.astype(BF16)
            at = (4 * t + 3) * HEAD_DIM
            out_ref[:, at : at + HEAD_DIM] = kv[1, :, t * HEAD_DIM : (t + 1) * HEAD_DIM].astype(BF16)

        @pl.when(pl.program_id(0) == 0)
        def _():
            gain_ref[...] = jnp.zeros_like(gain_ref)

        gain_ref[0:1] += sums[0]
        gain_ref[1:2] += sums[1]

    def rows_of(size):
        return pl.BlockSpec((rows, size), lambda i: (i, 0))

    pair = pl.BlockSpec((2, rows, 2 * HEAD_DIM), lambda i: (0, i, 0))
    return pl.pallas_call(
        kernel,
        grid=(total // rows,),
        out_shape=(
            jax.ShapeDtypeStruct((total, 8 * HEAD_DIM), BF16),
            jax.ShapeDtypeStruct(TILE, F32),
        ),
        in_specs=[
            rows_of(6 * HEAD_DIM),
            rows_of(4 * HEAD_DIM),
            pair,
            pair,
            rows_of(HEAD_DIM),
            rows_of(HEAD_DIM),
            whole((1, HEAD_DIM)),
            whole((1, HEAD_DIM)),
        ],
        out_specs=(rows_of(8 * HEAD_DIM), whole(TILE)),
        cost_estimate=pl.CostEstimate(
            flops=40 * total * 768, bytes_accessed=10 * total * 1024, transcendentals=0
        ),
        compiler_params=pltpu.CompilerParams(vmem_limit_bytes=24 * 1024 * 1024),
        name="qkv_back",
    )(raw, query_grad, kv_own, kv_back, cosines, sines, query_gain, key_gain)


def weight_partials(pairs):
    depth = pairs[0][0][0].shape[1]
    tensors = lax.axis_size(TENSOR)
    widths = [rights[0].shape[1] // tensors for _, rights in pairs]
    tokens = sum(block.shape[0] for block in pairs[0][0])
    tile = 512
    sides, in_specs = [], []
    for (lefts, rights), width in zip(pairs, widths):
        for left, right in zip(lefts, rights):
            sides += [left, right]
            in_specs.append(pl.BlockSpec((left.shape[0], tile), lambda t, k: (0, k)))
            in_specs.append(pl.BlockSpec((right.shape[0], width), lambda t, k: (0, t)))

    def kernel(*refs):
        out_ref = refs[-1]
        first, place = 0, 0
        for (lefts, _), width in zip(pairs, widths):
            product = 0.0
            for _ in lefts:
                product = product + lax.dot_general(
                    refs[place][...],
                    refs[place + 1][...],
                    (((0,), (0,)), ((), ())),
                    preferred_element_type=F32,
                )
                place += 2
            out_ref[0, :, first : first + width] = product.astype(BF16)
            first += width

    return pl.pallas_call(
        kernel,
        grid=(tensors, depth // tile),
        out_shape=jax.ShapeDtypeStruct((tensors, depth, sum(widths)), BF16),
        in_specs=in_specs,
        out_specs=pl.BlockSpec((1, tile, sum(widths)), lambda t, k: (t, k, 0)),
        cost_estimate=pl.CostEstimate(
            flops=2 * tokens * depth * sum(widths) * tensors,
            bytes_accessed=2 * depth * tensors * sum(widths) + 4 * tokens * depth,
            transcendentals=0,
        ),
        compiler_params=pltpu.CompilerParams(vmem_limit_bytes=24 * 1024 * 1024),
        name="weight_partials",
    )(*sides)


def scattered(partial):
    count = lax.axis_size(CTX)
    width = partial.shape[2]
    mine = lax.psum_scatter(
        partial.reshape(-1, width), (TENSOR, DP), scatter_dimension=0, tiled=True
    )
    return mine.reshape(count, mine.shape[0] // count, width)


def with_twin(own):
    other = shift(own, TENSOR, 1)
    first = lax.axis_index(TENSOR) == 0
    return jnp.concatenate([jnp.where(first, own, other), jnp.where(first, other, own)])


def sliced_layer(
    inputs,
    segment_ids,
    positions,
    out_grad,
    attn_gain,
    w_query,
    w_key,
    w_value,
    q_gain,
    k_gain,
    w_out,
    mlp_gain,
    w_gate,
    w_up,
    w_down,
):
    _, tok_count, width = inputs.shape
    count = lax.axis_size(CTX)
    tensors = lax.axis_size(TENSOR)
    rank = lax.axis_index(CTX)
    half = lax.axis_index(TENSOR)
    own_rows = tok_count // tensors
    rows = own_rows * count
    head_rows = w_out.shape[0]
    q_cols = w_query.shape[1] // count
    k_cols = w_key.shape[1] // count
    piece = attn_gain.shape[0]
    small = q_gain.shape[0]

    input_own = lax.dynamic_slice_in_dim(inputs[0], half * own_rows, own_rows, 0)
    grad_own = lax.dynamic_slice_in_dim(out_grad[0], half * own_rows, own_rows, 0)
    own_gains = jnp.concatenate([attn_gain, mlp_gain, q_gain, k_gain]).astype(F32)
    own_marks = jnp.concatenate([segment_ids[0], positions[0]])
    gains, marks, input_all, in_weight, out_weight = enter(
        to_tile(own_gains), to_tile(own_marks), input_own, w_query, w_key, w_value, w_out.T
    )
    out_weight = [out_weight[t * width : (t + 1) * width] for t in range(tensors)]
    gains = gains.reshape(gains.shape[0], -1)
    attn_scale = gains[:, :piece].reshape(-1)
    mlp_scale = gains[:, piece : 2 * piece].reshape(-1)
    query_scale = gains[:, 2 * piece : 2 * piece + small].reshape(-1)
    key_scale = gains[:, 2 * piece + small : 2 * (piece + small)].reshape(-1)

    ff_cols = w_gate.shape[1] // count
    late_gate, late_up, late_down, in_weight = lax.optimization_barrier(
        (w_gate, w_up, w_down, in_weight)
    )
    down_mine = swap_ahead(late_down.T.reshape(-1, count, ff_cols).transpose(1, 0, 2))
    mlp_shards = jnp.stack([late_gate, late_up]).reshape(2, -1, count, ff_cols)
    mlp_pieces = [lax.dynamic_index_in_dim(mlp_shards, rank, 2, keepdims=False)]
    for d in range(1, count):
        piece_ahead = lax.dynamic_index_in_dim(mlp_shards, (rank + d) % count, 2, keepdims=False)
        mlp_pieces.append(shift(piece_ahead, CTX, d))
    down_weight = lax.all_gather(rows_of(down_mine), (TENSOR, DP), axis=0, tiled=True)
    down_weight = [down_weight[t * width : (t + 1) * width] for t in range(tensors)]

    own_segs = lax.dynamic_index_in_dim(marks, half, 1, keepdims=False).reshape(rows)
    twin_segs = lax.dynamic_index_in_dim(marks, 1 - half, 1, keepdims=False).reshape(rows)
    own_positions = lax.dynamic_index_in_dim(marks, 2 + half, 1, keepdims=False).reshape(rows)
    order = jnp.arange(rows, dtype=jnp.int32)
    order = order // own_rows * tok_count + order % own_rows
    own_index, twin_index = order + half * own_rows, order + (1 - half) * own_rows
    token_marks = (
        own_segs[:, None],
        own_index[:, None],
        jnp.stack([own_segs, twin_segs]),
        jnp.stack([own_index, twin_index]),
    )
    cosine_table, sine_table = rope_tables(own_positions, HEAD_DIM)
    cosine_table = jnp.concatenate([cosine_table, cosine_table], axis=1)
    sine_table = jnp.concatenate([-sine_table, sine_table], axis=1)
    head_gains = (query_scale[None], key_scale[None])

    input_own, in_weight = lax.optimization_barrier((input_own, in_weight))
    stream = input_own.astype(F32)
    input_all = lax.dynamic_update_index_in_dim(input_all, input_own, rank, 0)
    _, attn_norm_pullback = jax.vjp(rms_norm, stream, attn_scale)
    normed_low, raw, query_low, kv_own = qkv_forward(
        input_all, attn_scale[None], in_weight, cosine_table, sine_table, *head_gains
    )
    kv_twin = shift(kv_own, TENSOR, 1)
    attended_low = attend(query_low, kv_own, kv_twin, token_marks)
    attended_own = swap_heads(attended_low, True, 3)
    attended_ahead = take_ring(attended_low.reshape(count, own_rows, tensors * q_cols), rank)
    attended_ahead = [attended_ahead[d] for d in range(count)]
    middle = stream
    for t in range(tensors):
        middle = middle + jnp.dot(
            attended_own[:, t * head_rows : (t + 1) * head_rows],
            out_weight[t].T,
            preferred_element_type=F32
        )
    normed_mid, mlp_norm_pullback = jax.vjp(rms_norm, middle, mlp_scale)
    mid_own = normed_mid.astype(BF16)
    mid_low, grad_low, gate_weight, up_weight = spread_mlp(mid_own, grad_own, mlp_pieces)
    mid_low = lax.dynamic_update_index_in_dim(mid_low, mid_own, rank, 0).reshape(rows, width)
    grad_low = lax.dynamic_update_index_in_dim(grad_low, grad_own, rank, 0).reshape(rows, width)

    gate = jnp.dot(mid_low, gate_weight, preferred_element_type=F32)
    upward = jnp.dot(mid_low, up_weight, preferred_element_type=F32)
    hidden, silu_pullback = jax.vjp(silu_product, gate, upward)
    hidden_low = hidden.astype(BF16)
    down_part = sum(
        jnp.dot(
            hidden_low[:, t * ff_cols : (t + 1) * ff_cols],
            down_weight[t].T,
            preferred_element_type=F32,
        )
        for t in range(tensors)
    ).astype(BF16)
    down_sum = scatter_sum(down_part.reshape(count, own_rows, width))
    hidden_low, _ = lax.optimization_barrier((hidden_low, down_part))
    down_weight_part = weight_partials([([grad_low], [hidden_low])])
    down_mine = scattered(down_weight_part)
    grad_low, _ = lax.optimization_barrier((grad_low, down_weight_part))
    hidden_grad = [jnp.dot(grad_low, w, preferred_element_type=F32) for w in down_weight]
    hidden_grad = jnp.concatenate(hidden_grad, axis=1)
    gate_grad, upward_grad = silu_pullback(hidden_grad)
    gate_grad_low = gate_grad.astype(BF16)
    upward_grad_low = upward_grad.astype(BF16)
    mid_grad_part = jnp.dot(gate_grad_low, gate_weight.T, preferred_element_type=F32) + jnp.dot(
        upward_grad_low, up_weight.T, preferred_element_type=F32
    )
    mid_grad_part, gate_grad_low, upward_grad_low = lax.optimization_barrier(
        (mid_grad_part.astype(BF16), gate_grad_low, upward_grad_low)
    )
    mid_grad_part = mid_grad_part.reshape(count, own_rows, width)
    mid_grad = scatter_sum(mid_grad_part)
    gate_up_part = weight_partials([([mid_low], [gate_grad_low]), ([mid_low], [upward_grad_low])])
    gate_up_mine = scattered(gate_up_part)

    middle_norm_grad, mlp_gain_grad = mlp_norm_pullback(mid_grad)
    middle_grad = grad_own.astype(F32) + middle_norm_grad
    branch_grad = middle_grad.astype(BF16)
    attended_grad = jnp.concatenate(
        [jnp.dot(branch_grad, w, preferred_element_type=F32).astype(BF16) for w in out_weight],
        axis=1,
    )
    attended_grad = swap_heads(attended_grad, False, 4)
    branch_grad, attended_grad = lax.optimization_barrier((branch_grad, attended_grad))
    branch_all = [branch_grad] + [shift(branch_grad, CTX, -d) for d in range(1, count)]
    query_grad, kv_grad, kv_back = attend_back(query_low, kv_own, kv_twin, attended_grad, token_marks)
    kv_arrived = shift(kv_back, TENSOR, 1)
    down_mine, _ = lax.optimization_barrier((down_mine, kv_back))
    down_got = swap_ahead(down_mine)
    kv_back = kv_arrived
    raw_grad_low, head_gain_grads = qkv_back(
        raw, query_grad, kv_grad, kv_back, cosine_table, sine_table, *head_gains
    )
    output, raw_grad_low = lax.optimization_barrier(
        ((middle + down_sum).astype(BF16), raw_grad_low)
    )
    output = with_twin(output)[None]
    normed_grad_part = jnp.dot(raw_grad_low, in_weight.T, preferred_element_type=F32)
    attn_part = weight_partials([([normed_low], [raw_grad_low]), (branch_all, attended_ahead)])
    normed_grad, attn_got = sum_tail(
        normed_grad_part.astype(BF16).reshape(count, own_rows, width), attn_part
    )
    gate_up_mine, attn_got = lax.optimization_barrier((gate_up_mine, attn_got))
    gate_up_got = swap_ahead(gate_up_mine)
    gate_weight_grad, up_weight_grad = assemble(
        gate_up_got, [ff_cols] * 2, [False] * 2, True
    )
    normed_grad = sum(normed_grad[i].astype(F32) for i in range(count))
    attn_grads = assemble(
        [attn_got[z] for z in range(count)],
        [q_cols, k_cols, k_cols, q_cols],
        [False, False, False, True],
        False,
    )
    (down_weight_grad,) = assemble(down_got, [ff_cols], [True], True)
    stream_norm_grad, attn_gain_grad = attn_norm_pullback(normed_grad)
    gain_grads = jnp.concatenate(
        [
            attn_gain_grad.reshape(-1, piece),
            mlp_gain_grad.reshape(-1, piece),
            head_gain_grads[0].reshape(-1, small),
            head_gain_grads[1].reshape(-1, small),
        ],
        axis=1,
    )
    gain_grads, attn_grads = lax.optimization_barrier((gain_grads, attn_grads))
    query_weight_grad, key_weight_grad, value_weight_grad, out_weight_grad = attn_grads
    gain_grads = owner_sums(jax.vmap(to_tile)(gain_grads)).reshape(-1)
    input_grad = with_twin((middle_grad + stream_norm_grad).astype(BF16))[None]
    return (
        output,
        input_grad,
        gain_grads[:piece],
        query_weight_grad,
        key_weight_grad,
        value_weight_grad,
        gain_grads[2 * piece : 2 * piece + small],
        gain_grads[2 * piece + small : 2 * (piece + small)],
        out_weight_grad,
        gain_grads[piece : 2 * piece],
        gate_weight_grad,
        up_weight_grad,
        down_weight_grad,
    )


def on_device_sliced(*args):
    return sliced_layer(*args)


def can_slice(mesh, inputs, w_query, w_key, w_gate):
    tensors, count = mesh.shape[TENSOR], mesh.shape[CTX]
    return (
        (mesh.shape[DP], count, tensors) == (4, 4, 2)
        and inputs.shape[0] == mesh.shape[DP]
        and inputs.shape[1] == count * tensors * TILE[1]
        and w_key.shape[1] == tensors * count * HEAD_DIM
        and w_query.shape[1] == 2 * w_key.shape[1]
        and w_gate.shape[1] % (tensors * count * 128) == 0
    )


def on_device(
    inputs,
    segment_ids,
    positions,
    out_grad,
    attn_gain,
    w_query,
    w_key,
    w_value,
    q_gain,
    k_gain,
    w_out,
    mlp_gain,
    w_gate,
    w_up,
    w_down,
):
    seq_count, tok_count, width = inputs.shape
    row_count = seq_count * tok_count
    cycle_size = lax.axis_size(CTX)
    cycle_rank = lax.axis_index(CTX)
    gathered_attn = (
        lax.all_gather(w_query, (DP, CTX), axis=0, tiled=True),
        lax.all_gather(w_key, (DP, CTX), axis=0, tiled=True),
        lax.all_gather(w_value, (DP, CTX), axis=0, tiled=True),
        lax.all_gather(w_out, (DP, CTX), axis=1, tiled=True),
        lax.all_gather(attn_gain, (DP, CTX), axis=0, tiled=True),
        lax.all_gather(q_gain, (DP, CTX), axis=0, tiled=True),
        lax.all_gather(k_gain, (DP, CTX), axis=0, tiled=True),
    )
    query_weight, key_weight, value_weight, out_weight, attn_scale, query_scale, key_scale = (
        gathered_attn
    )
    gathered_mlp = (
        lax.all_gather(w_gate, (DP, CTX), axis=0, tiled=True),
        lax.all_gather(w_up, (DP, CTX), axis=0, tiled=True),
        lax.all_gather(w_down, (DP, CTX), axis=1, tiled=True),
        lax.all_gather(mlp_gain, (DP, CTX), axis=0, tiled=True),
    )
    gate_weight, up_weight, down_weight, mlp_scale = gathered_mlp
    segments_all = lax.all_gather(segment_ids, CTX, axis=1, tiled=True)
    local_heads = query_weight.shape[1] // HEAD_DIM
    local_kv = key_weight.shape[1] // HEAD_DIM
    group_size = local_heads // local_kv
    kv_width = local_kv * HEAD_DIM
    score_scale = 1.0 / math.sqrt(HEAD_DIM)
    stream = inputs.astype(jnp.float32).reshape(row_count, width)
    normed_attn, attn_norm_pullback = jax.vjp(rms_norm, stream, attn_scale.astype(jnp.float32))
    normed_low = normed_attn.astype(jnp.bfloat16)
    query_raw = jnp.dot(normed_low, query_weight, preferred_element_type=jnp.float32).reshape(
        seq_count, tok_count, local_heads, HEAD_DIM
    )
    key_raw = jnp.dot(normed_low, key_weight, preferred_element_type=jnp.float32).reshape(
        seq_count, tok_count, local_kv, HEAD_DIM
    )
    value_low = (
        jnp.dot(normed_low, value_weight, preferred_element_type=jnp.float32)
        .astype(jnp.bfloat16)
        .reshape(seq_count, tok_count, kv_width)
    )
    cosine_table, sine_table = rope_tables(positions, HEAD_DIM)
    cosine_table = cosine_table[:, :, None, :]
    sine_table = sine_table[:, :, None, :]

    def norm_rope(raw_heads, gain_vector):
        return head_norm(raw_heads, gain_vector, cosine_table, sine_table)

    query_rot, query_pullback = jax.vjp(norm_rope, query_raw, query_scale.astype(jnp.float32))
    key_rot, key_pullback = jax.vjp(norm_rope, key_raw, key_scale.astype(jnp.float32))
    query_low = query_rot.astype(jnp.bfloat16).reshape(
        seq_count, tok_count, local_kv, group_size, HEAD_DIM
    )
    key_low = key_rot.astype(jnp.bfloat16).reshape(seq_count, tok_count, kv_width)
    query_index = cycle_rank * tok_count + jnp.arange(tok_count, dtype=jnp.int32)

    def block_scores(key_block, first_row):
        key_count = key_block.shape[1]
        key_heads = key_block.reshape(seq_count, key_count, local_kv, HEAD_DIM)
        raw_scores = (
            jnp.einsum(
                "stkgd,snkd->skgtn", query_low, key_heads, preferred_element_type=jnp.float32
            )
            * score_scale
        )
        key_index = first_row + jnp.arange(key_count, dtype=jnp.int32)
        key_segments = lax.dynamic_slice_in_dim(segments_all, first_row, key_count, 1)
        allowed = (key_index[None, None, :] <= query_index[None, :, None]) & (
            key_segments[:, None, :] == segment_ids[:, :, None]
        )
        return (raw_scores, allowed[:, None, None, :, :])

    stat_shape = (seq_count, local_kv, group_size, tok_count)
    pieces = (
        lax.all_gather(key_low, CTX, axis=1, tiled=True),
        lax.all_gather(value_low, CTX, axis=1, tiled=True),
    )
    row_best = jnp.full(stat_shape, masked_value, jnp.float32)
    raw_scores, allowed = block_scores(pieces[0], jnp.int32(0))
    masked = jnp.where(allowed, raw_scores, masked_value)
    new_best = jnp.maximum(row_best, jnp.max(masked, axis=-1))
    weights = jnp.where(allowed, jnp.exp(masked - new_best[..., None]), 0.0)
    value_heads = pieces[1].reshape(seq_count, pieces[1].shape[1], local_kv, HEAD_DIM)
    added = jnp.einsum(
        "skgtn,snkd->skgtd",
        weights.astype(jnp.bfloat16),
        value_heads,
        preferred_element_type=jnp.float32,
    )
    row_total = jnp.sum(weights, axis=-1)
    log_total = new_best + jnp.log(row_total)
    attended = added / row_total[..., None]
    attended_low = (
        jnp.transpose(attended, (0, 3, 1, 2, 4))
        .reshape(row_count, local_heads * HEAD_DIM)
        .astype(jnp.bfloat16)
    )
    attn_part = jnp.dot(attended_low, out_weight, preferred_element_type=jnp.float32)
    middle = stream + lax.psum(attn_part.astype(jnp.bfloat16), TENSOR).astype(jnp.float32)
    normed_mid, mlp_norm_pullback = jax.vjp(rms_norm, middle, mlp_scale.astype(jnp.float32))
    mid_low = normed_mid.astype(jnp.bfloat16)
    gate = jnp.dot(mid_low, gate_weight, preferred_element_type=jnp.float32)
    upward = jnp.dot(mid_low, up_weight, preferred_element_type=jnp.float32)
    hidden, silu_pullback = jax.vjp(silu_product, gate, upward)
    hidden_low = hidden.astype(jnp.bfloat16)
    down_part = jnp.dot(hidden_low, down_weight, preferred_element_type=jnp.float32)
    down_sum = lax.psum(down_part.astype(jnp.bfloat16), TENSOR).astype(jnp.float32)
    output = (middle + down_sum).astype(jnp.bfloat16).reshape(seq_count, tok_count, width)
    grad_low = out_grad.reshape(row_count, width)
    down_weight_grad = jnp.dot(hidden_low.T, grad_low, preferred_element_type=jnp.float32)
    hidden_grad = jnp.dot(grad_low, down_weight.T, preferred_element_type=jnp.float32)
    gate_grad, upward_grad = silu_pullback(hidden_grad)
    gate_grad_low = gate_grad.astype(jnp.bfloat16)
    upward_grad_low = upward_grad.astype(jnp.bfloat16)
    gate_weight_grad = jnp.dot(mid_low.T, gate_grad_low, preferred_element_type=jnp.float32)
    up_weight_grad = jnp.dot(mid_low.T, upward_grad_low, preferred_element_type=jnp.float32)
    mid_grad_part = jnp.dot(
        gate_grad_low, gate_weight.T, preferred_element_type=jnp.float32
    ) + jnp.dot(upward_grad_low, up_weight.T, preferred_element_type=jnp.float32)
    mid_grad = lax.psum(mid_grad_part.astype(jnp.bfloat16), TENSOR).astype(jnp.float32)
    middle_norm_grad, mlp_gain_grad = mlp_norm_pullback(mid_grad)
    middle_grad = grad_low.astype(jnp.float32) + middle_norm_grad
    mlp_grads = (
        lax.psum_scatter(gate_weight_grad, (DP, CTX), scatter_dimension=0, tiled=True),
        lax.psum_scatter(up_weight_grad, (DP, CTX), scatter_dimension=0, tiled=True),
        lax.psum_scatter(down_weight_grad, (DP, CTX), scatter_dimension=1, tiled=True),
        lax.psum_scatter(mlp_gain_grad, (DP, CTX), scatter_dimension=0, tiled=True),
    )
    branch_grad = middle_grad.astype(jnp.bfloat16)
    out_weight_grad = jnp.dot(attended_low.T, branch_grad, preferred_element_type=jnp.float32)
    attended_grad = jnp.dot(branch_grad, out_weight.T, preferred_element_type=jnp.float32).astype(
        jnp.bfloat16
    )
    attended_grad_heads = jnp.transpose(
        attended_grad.reshape(seq_count, tok_count, local_kv, group_size, HEAD_DIM), (0, 2, 3, 1, 4)
    )
    row_delta = jnp.sum(attended_grad_heads.astype(jnp.float32) * attended, axis=-1)

    def key_block_grads(key_block, value_block, first_row):
        raw_scores, allowed = block_scores(key_block, first_row)
        probability = jnp.where(allowed, jnp.exp(raw_scores - log_total[..., None]), 0.0)
        key_count = key_block.shape[1]
        value_heads = value_block.reshape(seq_count, key_count, local_kv, HEAD_DIM)
        key_heads = key_block.reshape(seq_count, key_count, local_kv, HEAD_DIM)
        prob_grad = jnp.einsum(
            "skgtd,snkd->skgtn",
            attended_grad_heads,
            value_heads,
            preferred_element_type=jnp.float32,
        )
        score_grad = (probability * (prob_grad - row_delta[..., None])).astype(jnp.bfloat16)
        query_add = jnp.einsum(
            "skgtn,snkd->skgtd", score_grad, key_heads, preferred_element_type=jnp.float32
        )
        key_add = jnp.einsum(
            "skgtn,stkgd->snkd", score_grad, query_low, preferred_element_type=jnp.float32
        ).reshape(seq_count, key_count, kv_width)
        value_add = jnp.einsum(
            "skgtn,skgtd->snkd",
            probability.astype(jnp.bfloat16),
            attended_grad_heads,
            preferred_element_type=jnp.float32,
        ).reshape(seq_count, key_count, kv_width)
        return (query_add, key_add, value_add)

    query_zero = jnp.zeros(stat_shape + (HEAD_DIM,), jnp.float32)
    kv_zero = jnp.zeros((seq_count, tok_count, kv_width), jnp.float32)

    def cycle_turn(turn_index, state):
        key_block, value_block, key_grad_acc, value_grad_acc, query_grad_acc = state
        owner_rank = (cycle_rank + turn_index) % cycle_size
        query_add, key_add, value_add = key_block_grads(
            key_block, value_block, owner_rank * tok_count
        )
        moved_blocks = from_behind((key_block, value_block), CTX, -1)
        moved_grads = (
            from_behind((key_grad_acc + key_add).astype(jnp.bfloat16), CTX, -1).astype(
                jnp.float32
            ),
            from_behind((value_grad_acc + value_add).astype(jnp.bfloat16), CTX, -1).astype(
                jnp.float32
            ),
        )
        return (
            moved_blocks[0],
            moved_blocks[1],
            moved_grads[0],
            moved_grads[1],
            query_grad_acc + query_add,
        )

    final_state = lax.fori_loop(
        0, cycle_size, cycle_turn, (key_low, value_low, kv_zero, kv_zero, query_zero)
    )
    key_grad_sum = final_state[2]
    value_grad_sum = final_state[3]
    query_grad_sum = final_state[4]
    query_grad = (
        jnp.transpose(query_grad_sum, (0, 3, 1, 2, 4)).reshape(
            seq_count, tok_count, local_heads, HEAD_DIM
        )
        * score_scale
    )
    query_raw_grad, query_gain_grad = query_pullback(query_grad)
    key_raw_grad, key_gain_grad = key_pullback(
        (key_grad_sum * score_scale).reshape(seq_count, tok_count, local_kv, HEAD_DIM)
    )
    query_grad_low = query_raw_grad.reshape(row_count, local_heads * HEAD_DIM).astype(jnp.bfloat16)
    key_grad_low = key_raw_grad.reshape(row_count, kv_width).astype(jnp.bfloat16)
    value_grad_low = value_grad_sum.reshape(row_count, kv_width).astype(jnp.bfloat16)
    query_weight_grad = jnp.dot(normed_low.T, query_grad_low, preferred_element_type=jnp.float32)
    key_weight_grad = jnp.dot(normed_low.T, key_grad_low, preferred_element_type=jnp.float32)
    value_weight_grad = jnp.dot(normed_low.T, value_grad_low, preferred_element_type=jnp.float32)
    normed_grad_part = (
        jnp.dot(query_grad_low, query_weight.T, preferred_element_type=jnp.float32)
        + jnp.dot(key_grad_low, key_weight.T, preferred_element_type=jnp.float32)
        + jnp.dot(value_grad_low, value_weight.T, preferred_element_type=jnp.float32)
    )
    normed_grad, query_gain_total, key_gain_total = (
        lax.psum(normed_grad_part.astype(jnp.bfloat16), TENSOR).astype(jnp.float32),
        lax.psum(query_gain_grad.astype(jnp.bfloat16), TENSOR).astype(jnp.float32),
        lax.psum(key_gain_grad.astype(jnp.bfloat16), TENSOR).astype(jnp.float32),
    )
    stream_norm_grad, attn_gain_grad = attn_norm_pullback(normed_grad)
    input_grad = (
        (middle_grad + stream_norm_grad).astype(jnp.bfloat16).reshape(seq_count, tok_count, width)
    )
    attn_grads = (
        lax.psum_scatter(query_weight_grad, (DP, CTX), scatter_dimension=0, tiled=True),
        lax.psum_scatter(key_weight_grad, (DP, CTX), scatter_dimension=0, tiled=True),
        lax.psum_scatter(value_weight_grad, (DP, CTX), scatter_dimension=0, tiled=True),
        lax.psum_scatter(out_weight_grad, (DP, CTX), scatter_dimension=1, tiled=True),
        lax.psum_scatter(attn_gain_grad, (DP, CTX), scatter_dimension=0, tiled=True),
        lax.psum_scatter(query_gain_total, (DP, CTX), scatter_dimension=0, tiled=True),
        lax.psum_scatter(key_gain_total, (DP, CTX), scatter_dimension=0, tiled=True),
    )
    return (
        output,
        input_grad,
        attn_grads[4],
        attn_grads[0],
        attn_grads[1],
        attn_grads[2],
        attn_grads[5],
        attn_grads[6],
        attn_grads[3],
        mlp_grads[3],
        mlp_grads[0],
        mlp_grads[1],
        mlp_grads[2],
    )


def solution(mesh):
    in_specs = (
        P(DP, CTX, None),
        P(DP, CTX),
        P(DP, CTX),
        P(DP, CTX, None),
        P((DP, CTX)),
        P((DP, CTX), TENSOR),
        P((DP, CTX), TENSOR),
        P((DP, CTX), TENSOR),
        P((DP, CTX)),
        P((DP, CTX)),
        P(TENSOR, (DP, CTX)),
        P((DP, CTX)),
        P((DP, CTX), TENSOR),
        P((DP, CTX), TENSOR),
        P(TENSOR, (DP, CTX)),
    )
    out_specs = (
        P(DP, CTX, None),
        P(DP, CTX, None),
        P((DP, CTX)),
        P((DP, CTX), TENSOR),
        P((DP, CTX), TENSOR),
        P((DP, CTX), TENSOR),
        P((DP, CTX)),
        P((DP, CTX)),
        P(TENSOR, (DP, CTX)),
        P((DP, CTX)),
        P((DP, CTX), TENSOR),
        P((DP, CTX), TENSOR),
        P(TENSOR, (DP, CTX)),
    )

    def step(*args):
        body = on_device_sliced if can_slice(mesh, args[0], args[5], args[6], args[12]) else on_device
        return jax.shard_map(
            body, mesh=mesh, in_specs=in_specs, out_specs=out_specs, check_vma=False
        )(*args)

    return step
```
